256 devices in a mesh: seq: 32 (over z, y_hi, core), batch: 8 (over x, y_lo).
Axes of the slice: x: 4, y: 4 (y_hi: 2, y_lo: 2; y = y_hi * 2 + y_lo), z: 8, core: 2. Of those that a mesh axis runs over, the one named last changes fastest.
Arguments:
- queries: bfloat16 [32768, 1792], P(('batch', 'seq')), parts along dimension 0, may hold values from -128 to 128
- keys: bfloat16 [32768, 256], P(('batch', 'seq')), parts along dimension 0, may hold values from -4 to 4
- values: bfloat16 [32768, 256], P(('batch', 'seq')), parts along dimension 0, may hold values from -4 to 4
- out_grad: bfloat16 [32768, 1792], P(('batch', 'seq')), parts along dimension 0, may hold values from -24 to 24
- row_delta: float32 [32768, 14], P(('batch', 'seq')), parts along dimension 0, may hold values from -6 to 6
- layer_input: bfloat16 [32768, 3584], P(('batch', 'seq')), parts along dimension 0, may hold values from -6 to 6
- norm_gain: float32 [3584], replicated, may hold values from 0.25 to 1.75
- qkv_weight: bfloat16 [3584, 2304], P('seq'), may hold values from -0.5 to 0.5
- block_order: int32 [512], P('batch'), parts along dimension 0, may hold values from 0 to 63, as said below
- block_mask: int32 [512, 64], P('batch'), parts along dimension 0, may hold values from 0 to 1, as said below
- frame_owner: int32 [256], P('batch'), parts along dimension 0, may hold values from 0 to 31, as said below
- vision_features: bfloat16 [256, 128, 1152], P(('batch', 'seq')), parts along dimension 0, may hold values from -6 to 6
- post_gain: float32 [1152], replicated, may hold values from 0.25 to 1.75
- projector: bfloat16 [1152, 3584], replicated, may hold values from -0.1875 to 0.1875
Outputs:
- token_grad: bfloat16 [32768, 3584], P(('batch', 'seq')), parts along dimension 0
- encoder_grad: bfloat16 [256, 128, 1152], P(('batch', 'seq')), parts along dimension 0
The draws below stay inside these ranges and needn't reach their ends.
There are 8 independent parts, one for each index of `batch`. The reference program is written for one: setup_inputs(seed, part) draws one part's arguments, and reference() takes and returns one part's arrays. A program takes and returns all parts, laid end to end along the dimension named above; an argument that names none is the same for every part. Nothing has to cross between parts.
Inputs may be any that keep to these rules, and one draw needn't show every extreme that they name: `block_order`: entries 2i and 2i + 1 are the blocks of device i of seq; all entries together are a permutation; each device's two blocks sum to 63; for every frame f, blocks 2f and 2f + 1 lie on devices 2j and 2j + 1 for some j. `block_mask`: 1 on the diagonal, 0 above it. `frame_owner`: every device of seq owns exactly one frame, and the owner of frame f holds block 2f or block 2f + 1.
All inputs are finite; a program needn't handle non-finite values.
Results may differ from the reference program's by a relative error of at most 0.012.
Values may be sent and summed in bfloat16 or wider, within the bound.
No kernel may reach another device: no remote copies, remote signals or barrier semaphores. Data moves between devices by JAX's collectives and lax.ppermute only.
A program may use at most 128 MiB of HBM per device.

```python
import jax
import jax.numpy as jnp
from jax import lax

D = 3584
HQ = 14
KVH = 2
HD = 128
C_ENC = 1152
TOK_DEV = 128
QKV = 2304
SEQ_LEN = 4096
FRAMES = 32
N_SEQ = 32


def frame_layout(key):
    count = N_SEQ
    groups = count // 2
    slot = jax.random.permutation(jax.random.fold_in(key, 11), groups).astype(jnp.int32)
    flip = jax.random.randint(jax.random.fold_in(key, 12), (groups,), 0, 2).astype(jnp.int32)
    order_first = jax.random.randint(jax.random.fold_in(key, 13), (groups,), 0, 2).astype(jnp.int32)
    order_second = jax.random.randint(jax.random.fold_in(key, 14), (groups,), 0, 2).astype(jnp.int32)
    owner_bit = jax.random.randint(jax.random.fold_in(key, 15), (groups,), 0, 2).astype(jnp.int32)
    group_ids = jnp.arange(groups, dtype=jnp.int32)
    device_first = (2 * slot + flip).astype(jnp.int32)
    device_second = (2 * slot + 1 - flip).astype(jnp.int32)
    first_lead = jnp.where(order_first == 1, 2 * count - 1 - 2 * group_ids, 2 * group_ids).astype(jnp.int32)
    second_lead = jnp.where(order_second == 1, 2 * count - 2 - 2 * group_ids, 2 * group_ids + 1).astype(jnp.int32)
    order = jnp.zeros((2 * count,), jnp.int32)
    order = order.at[2 * device_first].set(first_lead).at[2 * device_first + 1].set(2 * count - 1 - first_lead)
    order = order.at[2 * device_second].set(second_lead).at[2 * device_second + 1].set(2 * count - 1 - second_lead)
    owner = jnp.zeros((count,), jnp.int32)
    owner = owner.at[group_ids].set(jnp.where(owner_bit == 1, device_second, device_first))
    owner = owner.at[count - 1 - group_ids].set(jnp.where(owner_bit == 1, device_first, device_second))
    return (order.astype(jnp.int32), owner.astype(jnp.int32))


def draw_block_order(key, part):
    return frame_layout(key)[0]


def draw_frame_owner(key, part):
    return frame_layout(key)[1]


def draw_block_mask(key, part):
    count_blocks = 2 * N_SEQ
    random_bits = jax.random.randint(jax.random.fold_in(key, 21), (count_blocks, count_blocks), 0, 2).astype(jnp.int32)
    row_index = jnp.arange(count_blocks, dtype=jnp.int32)[:, None]
    column_index = jnp.arange(count_blocks, dtype=jnp.int32)[None, :]
    return jnp.where(row_index > column_index, random_bits, jnp.where(row_index == column_index, 1, 0)).astype(jnp.int32)


def attention_inputs(key):
    total_rows = TOK_DEV * N_SEQ
    half_len = TOK_DEV // 2
    group_size = HQ // KVH
    count_blocks = 2 * N_SEQ
    ranking = jnp.stack([jax.random.permutation(jax.random.fold_in(key, 40 + head), HD) for head in range(KVH)]).astype(jnp.int32)
    dim_scale = jnp.where(ranking < HD // 2, 1.5, 0.5).astype(jnp.float32)
    block_scale = jnp.exp(jax.random.uniform(jax.random.fold_in(key, 41), (count_blocks, 1, KVH, HD), jnp.float32, jnp.log(0.7), jnp.log(1.4)))
    key_scale = dim_scale[None, None, :, :] * block_scale
    limit = 4.0 / key_scale
    key_base = jax.random.truncated_normal(jax.random.fold_in(key, 31), -limit, limit, (count_blocks, half_len, KVH, HD), jnp.float32)
    keys_drawn = (key_base * key_scale).reshape(total_rows, KVH, HD)
    query_base = jax.random.truncated_normal(jax.random.fold_in(key, 32), -4.0, 4.0, (total_rows, KVH, group_size, HD), jnp.float32)
    queries_drawn = query_base * dim_scale[None, :, None, :]
    return (queries_drawn.reshape(total_rows, HQ * HD), keys_drawn.reshape(total_rows, KVH * HD))


def draw_queries(key, part):
    return attention_inputs(key)[0].astype(jnp.bfloat16)


def draw_keys(key, part):
    return attention_inputs(key)[1].astype(jnp.bfloat16)


def level_of(key, extent, cuts, smallest, largest):
    factor_of, own = 1.0, jax.random.fold_in(key, 6)
    for dim, shards_of in cuts:
        heights = jnp.exp(jax.random.uniform(jax.random.fold_in(own, dim), (shards_of,), jnp.float32, smallest / len(cuts), largest / len(cuts)))
        factor_of = factor_of * jnp.repeat(heights, extent[dim] // shards_of).reshape([-1 if axis == dim else 1 for axis in range(len(extent))])
    return factor_of


def gaussian(key, dims, scale, most, cuts=(), held_as=jnp.bfloat16):
    values = jax.random.normal(key, dims, jnp.float32) * scale
    if len(cuts) > 0:
        values = level_of(key, dims, cuts, -0.22, 0.18) * values
    return jnp.clip(values, min=-most, max=most).astype(held_as)


def setup_inputs(seed: int = 0, part: int = 0) -> dict:
    key_of = jax.random.split(jax.random.key(seed), 15)
    part_splits = jax.random.split(jax.random.fold_in(key_of[14], part), 15)
    return {
        "queries": draw_queries(jax.random.fold_in(jax.random.fold_in(key_of[14], part), 71), part),
        "keys": draw_keys(jax.random.fold_in(jax.random.fold_in(key_of[14], part), 71), part),
        "values": gaussian(part_splits[2], (SEQ_LEN, KVH * HD), 1.0, 4.0, ((0, 32),)),
        "out_grad": gaussian(part_splits[3], (SEQ_LEN, HQ * HD), 4.0, 24.0, ((0, 32),)),
        "row_delta": gaussian(part_splits[4], (SEQ_LEN, HQ), 1.0, 6.0, ((0, 32),), jnp.float32),
        "layer_input": gaussian(part_splits[5], (SEQ_LEN, D), 1.0, 6.0, ((0, 32),)),
        "norm_gain": jnp.clip(1.0 + 0.15 * jax.random.normal(key_of[6], (D,), jnp.float32), 0.25, 1.75),
        "qkv_weight": gaussian(key_of[7], (D, QKV), HD ** -0.5, 0.5, ((0, 32),)),
        "block_order": draw_block_order(jax.random.fold_in(jax.random.fold_in(key_of[14], part), 71), part),
        "block_mask": draw_block_mask(jax.random.fold_in(jax.random.fold_in(key_of[14], part), 71), part),
        "frame_owner": draw_frame_owner(jax.random.fold_in(jax.random.fold_in(key_of[14], part), 71), part),
        "vision_features": gaussian(part_splits[11], (FRAMES, TOK_DEV, C_ENC), 1.0, 6.0, ((0, 32),)),
        "post_gain": jnp.clip(1.0 + 0.15 * jax.random.normal(key_of[12], (C_ENC,), jnp.float32), 0.25, 1.75),
        "projector": gaussian(key_of[13], (C_ENC, D), C_ENC ** -0.5, 0.1875),
    }


EPSILON = 1e-06
NEGATIVE = -1e+30

def reference(queries, keys, values, out_grad, row_delta, layer_input, norm_gain, qkv_weight, block_order, block_mask, frame_owner, vision_features, post_gain, projector):
    half_len = TOK_DEV // 2
    total_rows = TOK_DEV * N_SEQ
    group_size = HQ // KVH
    scaling = HD ** (-0.5)
    row_ids = jnp.arange(total_rows, dtype=jnp.int32)
    position = (block_order[row_ids // half_len] * half_len + row_ids % half_len).astype(jnp.int32)
    blocks = (position // half_len).astype(jnp.int32)
    query_heads = queries.reshape(total_rows, HQ, HD)
    grad_heads = out_grad.reshape(total_rows, HQ, HD)
    key_heads = keys.reshape(total_rows, KVH, HD)
    value_heads = values.reshape(total_rows, KVH, HD)

    def one_head(head_index):
        kv_index = (head_index // group_size).astype(jnp.int32)
        query_rows = lax.dynamic_index_in_dim(query_heads, head_index, 1, keepdims=False)
        grad_rows = lax.dynamic_index_in_dim(grad_heads, head_index, 1, keepdims=False)
        key_rows = lax.dynamic_index_in_dim(key_heads, kv_index, 1, keepdims=False)
        value_rows = lax.dynamic_index_in_dim(value_heads, kv_index, 1, keepdims=False)
        delta_rows = lax.dynamic_index_in_dim(row_delta, head_index, 1, keepdims=False)

        def per_block(running, block_start):
            key_acc, value_acc = running
            query_block = lax.dynamic_slice_in_dim(query_rows, block_start, TOK_DEV, 0)
            grad_block = lax.dynamic_slice_in_dim(grad_rows, block_start, TOK_DEV, 0)
            delta_block = lax.dynamic_slice_in_dim(delta_rows, block_start, TOK_DEV, 0)
            pos_block = lax.dynamic_slice_in_dim(position, block_start, TOK_DEV, 0)
            block_ids = lax.dynamic_slice_in_dim(blocks, block_start, TOK_DEV, 0)
            allowed = (block_mask[block_ids][:, blocks] == 1) & (position[None, :] <= pos_block[:, None])
            score = jnp.dot(query_block, key_rows.T, preferred_element_type=jnp.float32) * scaling
            top_score = lax.optimization_barrier(jnp.max(jnp.where(allowed, score, NEGATIVE), axis=1))
            total_exp = lax.optimization_barrier(jnp.sum(jnp.where(allowed, jnp.exp(score - top_score[:, None]), 0.0), axis=1))
            lse = top_score + jnp.log(total_exp)
            prob = jnp.where(allowed, jnp.exp(score - lse[:, None]), 0.0)
            prob_low = prob.astype(jnp.bfloat16)
            value_acc = value_acc + jnp.dot(prob_low.T, grad_block, preferred_element_type=jnp.float32)
            prob_grad = jnp.dot(grad_block, value_rows.T, preferred_element_type=jnp.float32)
            score_grad = (prob * (prob_grad - delta_block[:, None])).astype(jnp.bfloat16)
            query_out = jnp.dot(score_grad, key_rows, preferred_element_type=jnp.float32) * scaling
            key_acc = key_acc + jnp.dot(score_grad.T, query_block, preferred_element_type=jnp.float32)
            return ((key_acc, value_acc), query_out)
        starting = (jnp.zeros((total_rows, HD), jnp.float32), jnp.zeros((total_rows, HD), jnp.float32))
        starts = (jnp.arange(N_SEQ, dtype=jnp.int32) * TOK_DEV).astype(jnp.int32)
        finals, query_parts = lax.scan(per_block, starting, starts)
        return (query_parts.reshape(total_rows, HD), finals[0] * scaling, finals[1])
    query_all, key_all, value_all = lax.map(one_head, jnp.arange(HQ, dtype=jnp.int32))
    query_grad = jnp.transpose(query_all, (1, 0, 2)).reshape(total_rows, HQ * HD)
    key_grad = jnp.transpose(lax.optimization_barrier(jnp.sum(key_all.reshape(KVH, group_size, total_rows, HD), axis=1)), (1, 0, 2)).reshape(total_rows, KVH * HD)
    value_grad = jnp.transpose(lax.optimization_barrier(jnp.sum(value_all.reshape(KVH, group_size, total_rows, HD), axis=1)), (1, 0, 2)).reshape(total_rows, KVH * HD)
    head_grads = jnp.concatenate([query_grad, key_grad, value_grad], axis=1).astype(jnp.bfloat16)
    norm_grad = jnp.dot(head_grads, qkv_weight.T, preferred_element_type=jnp.float32).astype(jnp.bfloat16)
    inputs = layer_input.astype(jnp.float32)
    inverse = lax.rsqrt(lax.optimization_barrier(jnp.mean(inputs * inputs, axis=1, keepdims=True)) + EPSILON)
    scaled = norm_grad.astype(jnp.float32) * norm_gain
    token_grad = (inverse * scaled - inputs * inverse ** 3 * lax.optimization_barrier(jnp.mean(scaled * inputs, axis=1, keepdims=True))).astype(jnp.bfloat16)
    row_of_position = jnp.zeros((total_rows,), jnp.int32).at[position].set(row_ids)
    device_ids = jnp.arange(N_SEQ, dtype=jnp.int32)
    frame_of_device = jnp.zeros((N_SEQ,), jnp.int32).at[frame_owner].set(device_ids)
    spatial = jnp.arange(TOK_DEV, dtype=jnp.int32)
    frame_rows = row_of_position[(frame_of_device[:, None] * TOK_DEV + spatial[None, :]).astype(jnp.int32)]
    frame_grad = token_grad[frame_rows]
    post_grad = jnp.dot(frame_grad.reshape(N_SEQ * TOK_DEV, D), projector.T, preferred_element_type=jnp.float32).reshape(N_SEQ, TOK_DEV, C_ENC)
    features = vision_features.astype(jnp.float32)
    centered = features - lax.optimization_barrier(jnp.mean(features, axis=2, keepdims=True))
    deviation = lax.rsqrt(lax.optimization_barrier(jnp.mean(centered * centered, axis=2, keepdims=True)) + EPSILON)
    normed = centered * deviation
    weighted = post_grad * post_gain
    encoder_grad = (deviation * (weighted - lax.optimization_barrier(jnp.mean(weighted, axis=2, keepdims=True)) - normed * lax.optimization_barrier(jnp.mean(weighted * normed, axis=2, keepdims=True)))).astype(jnp.bfloat16)
    return (token_grad, encoder_grad)
```

```python
import jax
import jax.numpy as jnp
from jax import lax
from jax.experimental import pallas as pl
from jax.experimental.pallas import tpu as pltpu
from jax.sharding import Mesh, PartitionSpec as P

HQ = 14
KVH = 2
HD = 128
GROUP = HQ // KVH
EPSILON = 1e-06
NEGATIVE = -1e30
BLOCK = 64
LANES = GROUP * BLOCK
STEP = 4


def dot_nt(a, b):
    return lax.dot_general(a, b, (((1,), (1,)), ((), ())), preferred_element_type=jnp.float32)


def dot_nn(a, b):
    return lax.dot_general(a, b, (((1,), (0,)), ((), ())), preferred_element_type=jnp.float32)


def dot_tn(a, b):
    return lax.dot_general(a, b, (((0,), (0,)), ((), ())), preferred_element_type=jnp.float32)


def attention_kernel(pieces, *refs):
    slot_ref, dest_ref, kind_ref, turns_ref, q_own, q_got, g_own, g_got, delta_ref = refs[:9]
    kv_parts = refs[9 : 9 + pieces]
    dq_ref, dkv_ref = refs[9 + pieces : 11 + pieces]
    qs, gs, kv, bias, acc, dqt = refs[11 + pieces :]
    scaling = HD ** (-0.5)
    to_log2 = scaling * 1.4426950408889634
    rows = kv_parts[0].shape[0]
    for i, part in enumerate(kv_parts):
        kv[i * rows : (i + 1) * rows, :] = part[...]
    for a in range(4):
        q_ref, g_ref = (q_own, g_own) if a < 2 else (q_got, g_got)
        first = (a % 2) * BLOCK
        for h in range(GROUP):
            qs[a, h * BLOCK : (h + 1) * BLOCK, :] = q_ref[first : first + BLOCK, h * HD : (h + 1) * HD]
            gs[a, h * BLOCK : (h + 1) * BLOCK, :] = g_ref[first : first + BLOCK, h * HD : (h + 1) * HD]
    key_row = lax.broadcasted_iota(jnp.int32, (BLOCK, LANES), 0)
    query_row = lax.broadcasted_iota(jnp.int32, (BLOCK, LANES), 1) % BLOCK
    bias[0] = jnp.zeros((BLOCK, LANES), jnp.float32)
    bias[1] = jnp.where(key_row <= query_row, 0.0, NEGATIVE)
    bias[2] = jnp.full((BLOCK, LANES), NEGATIVE, jnp.float32)
    acc[...] = jnp.zeros(acc.shape, jnp.float32)

    def gathered(a, turn, first):
        parts = []
        for i in range(STEP):
            row = pl.multiple_of(slot_ref[a, turn * STEP + i], BLOCK)
            parts.append(kv[pl.ds(row, BLOCK), first : first + HD])
        return jnp.concatenate(parts, axis=0)

    def scores(a, turn, keys):
        mask = jnp.concatenate([bias[kind_ref[a, turn * STEP + i]] for i in range(STEP)], axis=0)
        return dot_nt(keys, qs[a]) * to_log2 + mask

    for a in range(4):

        def total(turn, state):
            top, summed = state
            score = scores(a, turn, gathered(a, turn, 0)).reshape(STEP * BLOCK // 8, 8, LANES)
            top_next = jnp.maximum(top, jnp.max(score, axis=0))
            summed = summed * jnp.exp2(top - top_next) + jnp.sum(jnp.exp2(score - top_next), axis=0)
            return top_next, summed

        top, summed = lax.fori_loop(
            0,
            turns_ref[a],
            total,
            (jnp.full((8, LANES), NEGATIVE, jnp.float32), jnp.zeros((8, LANES), jnp.float32)),
        )
        peak = jnp.max(top, axis=0, keepdims=True)
        whole = jnp.sum(summed * jnp.exp2(top - peak), axis=0, keepdims=True)
        lse = peak + jnp.log2(whole)
        delta = delta_ref[a]
        dqt[...] = jnp.zeros(dqt.shape, jnp.float32)

        def grads(turn, unused):
            keys = gathered(a, turn, 0)
            values = gathered(a, turn, HD)
            prob = jnp.exp2(scores(a, turn, keys) - lse)
            prob_grad = dot_nt(values, gs[a])
            score_grad = (prob * (prob_grad - delta)).astype(jnp.bfloat16)
            value_add = dot_nn(prob.astype(jnp.bfloat16), gs[a])
            key_add = dot_nn(score_grad, qs[a])
            dqt[...] += dot_tn(keys, score_grad)
            for i in range(STEP):
                row = pl.multiple_of(dest_ref[a, turn * STEP + i], BLOCK)
                acc[pl.ds(row, BLOCK), 0:HD] += key_add[i * BLOCK : (i + 1) * BLOCK, :]
                acc[pl.ds(row, BLOCK), HD : 2 * HD] += value_add[i * BLOCK : (i + 1) * BLOCK, :]
            return unused

        lax.fori_loop(0, turns_ref[a], grads, 0)
        dq = (dqt[...].T * scaling).astype(jnp.bfloat16)
        for h in range(GROUP):
            dq_ref[a * BLOCK : (a + 1) * BLOCK, h * HD : (h + 1) * HD] = dq[h * BLOCK : (h + 1) * BLOCK, :]
    dkv_ref[:, 0:HD] = (acc[:, 0:HD] * scaling).astype(jnp.bfloat16)
    dkv_ref[:, HD : 2 * HD] = acc[:, HD : 2 * HD].astype(jnp.bfloat16)


def attention(slots, dests, kinds, turns, q_own, q_got, g_own, g_got, delta, kv_parts):
    pieces = len(kv_parts)
    rows = pieces * kv_parts[0].shape[0]
    smem = pl.BlockSpec(memory_space=pltpu.SMEM)
    vmem = pl.BlockSpec(memory_space=pltpu.VMEM)
    return pl.pallas_call(
        lambda *refs: attention_kernel(pieces, *refs),
        out_shape=(
            jax.ShapeDtypeStruct((4 * BLOCK, GROUP * HD), jnp.bfloat16),
            jax.ShapeDtypeStruct((rows, 2 * HD), jnp.bfloat16),
        ),
        in_specs=[smem] * 4 + [vmem] * (5 + pieces),
        out_specs=(vmem, vmem),
        scratch_shapes=[
            pltpu.VMEM((4, LANES, HD), jnp.bfloat16),
            pltpu.VMEM((4, LANES, HD), jnp.bfloat16),
            pltpu.VMEM((rows, 2 * HD), jnp.bfloat16),
            pltpu.VMEM((3, BLOCK, LANES), jnp.float32),
            pltpu.VMEM((rows, 2 * HD), jnp.float32),
            pltpu.VMEM((HD, LANES), jnp.float32),
        ],
        name="attention_grads",
    )(slots, dests, kinds, turns, q_own, q_got, g_own, g_got, delta, *kv_parts)


def looked_up(table, index):
    return jnp.sum(jnp.where(index[..., None] == jnp.arange(table.shape[0]), table, 0), axis=-1)


def work_lists(block_order, block_mask, z, yh, c, nz):
    slot = jnp.arange(4 * 2 * nz, dtype=jnp.int32)
    core = c ^ ((slot // 2) % 2)
    chip = ((z - slot // 8) % nz) * 2 + (yh ^ ((slot // 4) % 2))
    key_block = looked_up(block_order, 2 * (2 * chip + core) + slot % 2)
    dest = chip * 256 + (slot % 4) * BLOCK
    mine = slot[:4]
    query_block = looked_up(block_order, 2 * (2 * (2 * z + yh) + (c ^ (mine // 2))) + mine % 2)
    table = jnp.arange(block_mask.shape[0], dtype=jnp.int32)
    query_hot = query_block[:, None] == table
    key_hot = key_block[:, None] == table
    mask_rows = jnp.sum(jnp.where(query_hot[:, :, None], block_mask[None], 0), axis=1)
    live = jnp.sum(jnp.where(key_hot[None], mask_rows[:, None, :], 0), axis=-1) > 0
    place = jnp.sum(jnp.where(live[:, None, :] & (slot[None, :] < slot[:, None]), 1, 0), axis=-1)
    count = jnp.sum(live.astype(jnp.int32), axis=1)
    chosen = live[:, None, :] & (place[:, None, :] == slot[None, :, None])
    diagonal = key_block[None, :] == query_block[:, None]

    def packed(values):
        return jnp.sum(jnp.where(chosen, values, 0), axis=-1)

    slots = packed(jnp.broadcast_to(slot * BLOCK, chosen.shape))
    dests = packed(jnp.broadcast_to(dest, chosen.shape))
    kinds = jnp.where(slot[None, :] < count[:, None], packed(diagonal[:, None, :].astype(jnp.int32)), 2)
    return slots, dests, kinds, (count + STEP - 1) // STEP


def swap_core(value):
    return lax.ppermute(value, "c", [(0, 1), (1, 0)])


def delta_rows(delta):
    return jnp.transpose(delta.reshape(2, BLOCK, GROUP), (0, 2, 1)).reshape(2, 1, LANES)


def body(
    queries,
    keys,
    values,
    out_grad,
    row_delta,
    layer_input,
    norm_gain,
    qkv_weight,
    block_order,
    block_mask,
    frame_owner,
    vision_features,
    post_gain,
    projector,
):
    nz, nx = lax.axis_size("z"), lax.axis_size("x")
    z, yh, c, x, yl = (lax.axis_index(name) for name in ("z", "yh", "c", "x", "yl"))
    wide = GROUP * HD
    tok_rows = queries.shape[0]

    def group_of(array, which, width):
        return lax.dynamic_slice_in_dim(array, which * width, width, 1)

    def kv_of(which):
        return jnp.concatenate([group_of(keys, which, HD), group_of(values, which, HD)], axis=1)

    kv_chip = jnp.concatenate([kv_of(c), swap_core(kv_of(1 - c))], axis=0)
    kv_other = lax.ppermute(kv_chip, "yh", [(0, 1), (1, 0)])

    forward = [(i, (i + 1) % nz) for i in range(nz)]
    backward = [(i, (i - 1) % nz) for i in range(nz)]
    parts = {}
    for y, start in enumerate((kv_chip, kv_other)):
        parts[0, y] = up = down = start
        for k in range(1, nz // 2 + 1):
            parts[k, y] = up = lax.ppermute(up, "z", forward)
            if k < nz // 2:
                parts[nz - k, y] = down = lax.ppermute(down, "z", backward)
    kv_parts = [parts[k, y] for k in range(nz) for y in range(2)]

    q_own, g_own = group_of(queries, c, wide), group_of(out_grad, c, wide)
    q_got = swap_core(group_of(queries, 1 - c, wide))
    g_got = swap_core(group_of(out_grad, 1 - c, wide))
    delta_got = swap_core(delta_rows(group_of(row_delta, 1 - c, GROUP)))
    delta = jnp.concatenate([delta_rows(group_of(row_delta, c, GROUP)), delta_got], axis=0)

    slots, dests, kinds, turns = work_lists(block_order, block_mask, z, yh, c, nz)
    dq, dkv = attention(slots, dests, kinds, turns, q_own, q_got, g_own, g_got, delta, kv_parts)
    spread = lax.all_to_all(dkv, ("z", "yh"), 0, 0, tiled=True)
    dkv_own = jnp.sum(
        spread.reshape(2 * nz, 2 * tok_rows, 2 * HD).astype(jnp.float32), axis=0
    ).astype(jnp.bfloat16)

    def columns_of(which):
        return jnp.concatenate(
            [
                group_of(qkv_weight[:, : HQ * HD], which, wide),
                group_of(qkv_weight[:, HQ * HD :], which, HD),
                group_of(qkv_weight[:, HQ * HD :], KVH + which, HD),
            ],
            axis=1,
        )

    def index(yh_, c_, x_, yl_):
        return ((yh_ * 2 + c_) * nx + x_) * 2 + yl_

    across = [
        (index(x_ >> 1, x_ & 1, x_, yl_), index(1 - (x_ >> 1), x_ & 1, x_, 1 - yl_))
        for x_ in range(nx)
        for yl_ in range(2)
    ]
    from_y = lax.ppermute(qkv_weight, ("yh", "c", "x", "yl"), across)
    qkv_weight = jnp.where(yh == x >> 1, qkv_weight, from_y)
    mine, theirs = columns_of(c), columns_of(1 - c)
    handed = lax.ppermute(
        theirs, ("c", "x"), [((x_ & 1) * nx + x_, (1 - (x_ & 1)) * nx + x_) for x_ in range(nx)]
    )
    quarter = jnp.where(c == x & 1, mine, handed)
    gathered = lax.all_gather(quarter, "z", axis=0, tiled=True)
    gathered = lax.all_gather(gathered, "x", axis=0, tiled=True)
    rows = quarter.shape[0]
    weight = jnp.transpose(
        gathered.reshape(nx, nz, rows, quarter.shape[1]), (1, 0, 2, 3)
    ).reshape(nx * nz * rows, quarter.shape[1])

    partial = dot_nt(dq, weight[:, :wide]) + dot_nt(dkv_own, weight[:, wide:])
    from_core = swap_core(partial[tok_rows:].astype(jnp.bfloat16))
    norm_grad = (partial[:tok_rows] + from_core.astype(jnp.float32)).astype(jnp.bfloat16)

    inputs = layer_input.astype(jnp.float32)
    inverse = lax.rsqrt(jnp.mean(inputs * inputs, axis=1, keepdims=True) + EPSILON)
    scaled = norm_grad.astype(jnp.float32) * norm_gain
    token_grad = (
        inverse * scaled - inputs * inverse**3 * jnp.mean(scaled * inputs, axis=1, keepdims=True)
    ).astype(jnp.bfloat16)

    my_index = (z * 2 + yh) * 2 + c
    frame_table = jnp.arange(frame_owner.shape[0], dtype=jnp.int32)
    my_frame = jnp.sum(jnp.where(frame_owner == my_index, frame_table, 0))
    my_blocks = lax.dynamic_slice_in_dim(block_order, 2 * my_index, 2, 0)
    keep_first = my_blocks[0] // 2 == my_frame
    kept_block = jnp.where(keep_first, my_blocks[0], my_blocks[1])
    leading = kept_block % 2 == 0
    kept = jnp.where(keep_first, token_grad[:BLOCK], token_grad[BLOCK:])
    received = swap_core(jnp.where(keep_first, token_grad[BLOCK:], token_grad[:BLOCK]))
    frame_rows = jnp.where(
        leading,
        jnp.concatenate([kept, received], axis=0),
        jnp.concatenate([received, kept], axis=0),
    )
    post_grad = dot_nt(frame_rows, projector)
    features = vision_features[0].astype(jnp.float32)
    centered = features - jnp.mean(features, axis=1, keepdims=True)
    deviation = lax.rsqrt(jnp.mean(centered * centered, axis=1, keepdims=True) + EPSILON)
    normed = centered * deviation
    weighted = post_grad * post_gain
    encoder_grad = (
        deviation
        * (
            weighted
            - jnp.mean(weighted, axis=1, keepdims=True)
            - normed * jnp.mean(weighted * normed, axis=1, keepdims=True)
        )
    ).astype(jnp.bfloat16)
    return (token_grad, encoder_grad[None])


def solution(mesh):
    grid = Mesh(mesh.devices.reshape(8, 2, 2, 4, 2), ("z", "yh", "c", "x", "yl"))
    both = ("x", "yl", "z", "yh", "c")
    placed = (
        P(both, None),
        P(both, None),
        P(both, None),
        P(both, None),
        P(both, None),
        P(both, None),
        P(),
        P(("z", "yh", "c"), None),
        P(("x", "yl")),
        P(("x", "yl"), None),
        P(("x", "yl")),
        P(both, None, None),
        P(),
        P(),
    )
    return jax.shard_map(
        body,
        mesh=grid,
        in_specs=placed,
        out_specs=(P(both, None), P(both, None, None)),
        check_vma=False,
    )
```

```python
import jax
import jax.numpy as jnp
from jax import lax
from jax.experimental import pallas as pl
from jax.experimental.pallas import tpu as pltpu
from jax.sharding import Mesh, PartitionSpec as P

HQ = 14
KVH = 2
HD = 128
GROUP = HQ // KVH
EPSILON = 1e-06
NEGATIVE = -1e30
BLOCK = 64
LANES = GROUP * BLOCK
STEP = 4


def dot_nt(a, b):
    return lax.dot_general(a, b, (((1,), (1,)), ((), ())), preferred_element_type=jnp.float32)


def dot_nn(a, b):
    return lax.dot_general(a, b, (((1,), (0,)), ((), ())), preferred_element_type=jnp.float32)


def dot_tn(a, b):
    return lax.dot_general(a, b, (((0,), (0,)), ((), ())), preferred_element_type=jnp.float32)


def attention_kernel(pieces, *refs):
    slot_ref, kind_ref, query_ref, start_ref, turns_ref, q_own, q_got, g_own, g_got, delta_ref = refs[:10]
    kv_parts = refs[10 : 10 + pieces]
    dq_ref, dkv_ref = refs[10 + pieces : 12 + pieces]
    qs, gs, kv, bias, acc, dqt, tops, sums, lses = refs[12 + pieces :]
    scaling = HD ** (-0.5)
    to_log2 = scaling * 1.4426950408889634
    rows = kv_parts[0].shape[0]
    for i, part in enumerate(kv_parts):
        kv[i * rows : (i + 1) * rows, :] = part[...]
    for a in range(4):
        q_ref, g_ref = (q_own, g_own) if a < 2 else (q_got, g_got)
        first = (a % 2) * BLOCK
        for h in range(GROUP):
            qs[a, h * BLOCK : (h + 1) * BLOCK, :] = q_ref[first : first + BLOCK, h * HD : (h + 1) * HD]
            gs[a, h * BLOCK : (h + 1) * BLOCK, :] = g_ref[first : first + BLOCK, h * HD : (h + 1) * HD]
    key_row = lax.broadcasted_iota(jnp.int32, (BLOCK, LANES), 0)
    query_row = lax.broadcasted_iota(jnp.int32, (BLOCK, LANES), 1) % BLOCK
    bias[0] = jnp.zeros((BLOCK, LANES), jnp.float32)
    bias[1] = jnp.where(key_row <= query_row, 0.0, NEGATIVE)
    bias[2] = jnp.full((BLOCK, LANES), NEGATIVE, jnp.float32)
    acc[...] = jnp.zeros(acc.shape, jnp.float32)
    dqt[...] = jnp.zeros(dqt.shape, jnp.float32)
    tops[...] = jnp.full(tops.shape, NEGATIVE, jnp.float32)
    sums[...] = jnp.zeros(sums.shape, jnp.float32)

    def slots_of(item):
        first = start_ref[item]
        return [pl.multiple_of(slot_ref[first + i], BLOCK) for i in range(STEP)]

    def gathered(slots, first):
        return jnp.concatenate([kv[pl.ds(row, BLOCK), first : first + HD] for row in slots], axis=0)

    def scores(item, a, keys):
        first = start_ref[item]
        mask = jnp.concatenate([bias[kind_ref[first + i]] for i in range(STEP)], axis=0)
        return dot_nt(keys, qs[a]) * to_log2 + mask

    def total(turn, unused):
        for item in (2 * turn, 2 * turn + 1):
            a = query_ref[item]
            score = scores(item, a, gathered(slots_of(item), 0)).reshape(STEP * BLOCK // 8, 8, LANES)
            top = tops[a]
            top_next = jnp.maximum(top, jnp.max(score, axis=0))
            sums[a] = sums[a] * jnp.exp2(top - top_next) + jnp.sum(jnp.exp2(score - top_next), axis=0)
            tops[a] = top_next
        return unused

    lax.fori_loop(0, turns_ref[0], total, 0)
    for a in range(4):
        top = tops[a]
        peak = jnp.max(top, axis=0, keepdims=True)
        whole = jnp.sum(sums[a] * jnp.exp2(top - peak), axis=0, keepdims=True)
        lses[a] = peak + jnp.log2(whole)

    def grads(turn, unused):
        for item in (2 * turn, 2 * turn + 1):
            a = query_ref[item]
            slots = slots_of(item)
            keys = gathered(slots, 0)
            values = gathered(slots, HD)
            prob = jnp.exp2(scores(item, a, keys) - lses[a])
            prob_grad = dot_nt(values, gs[a])
            score_grad = (prob * (prob_grad - delta_ref[a])).astype(jnp.bfloat16)
            value_add = dot_nn(prob.astype(jnp.bfloat16), gs[a])
            key_add = dot_nn(score_grad, qs[a])
            dqt[a] += dot_tn(keys, score_grad)
            for i, row in enumerate(slots):
                acc[pl.ds(row, BLOCK), 0:HD] += key_add[i * BLOCK : (i + 1) * BLOCK, :]
                acc[pl.ds(row, BLOCK), HD : 2 * HD] += value_add[i * BLOCK : (i + 1) * BLOCK, :]
        return unused

    lax.fori_loop(0, turns_ref[0], grads, 0)
    for a in range(4):
        dq = (dqt[a].T * scaling).astype(jnp.bfloat16)
        for h in range(GROUP):
            dq_ref[a * BLOCK : (a + 1) * BLOCK, h * HD : (h + 1) * HD] = dq[h * BLOCK : (h + 1) * BLOCK, :]
    dkv_ref[:, 0:HD] = (acc[:, 0:HD] * scaling).astype(jnp.bfloat16)
    dkv_ref[:, HD : 2 * HD] = acc[:, HD : 2 * HD].astype(jnp.bfloat16)


SMEM = pl.BlockSpec(memory_space=pltpu.SMEM)
VMEM = pl.BlockSpec(memory_space=pltpu.VMEM)
ANY = pl.BlockSpec(memory_space=pl.ANY)


def attention(lists, q_own, q_got, g_own, g_got, delta, kv_parts):
    pieces = len(kv_parts)
    rows = pieces * kv_parts[0].shape[0]
    return pl.pallas_call(
        lambda *refs: attention_kernel(pieces, *refs),
        out_shape=(
            jax.ShapeDtypeStruct((4 * BLOCK, GROUP * HD), jnp.bfloat16),
            jax.ShapeDtypeStruct((rows, 2 * HD), jnp.bfloat16),
        ),
        in_specs=[SMEM] * 5 + [VMEM] * (5 + pieces),
        out_specs=(VMEM, VMEM),
        scratch_shapes=[
            pltpu.VMEM((4, LANES, HD), jnp.bfloat16),
            pltpu.VMEM((4, LANES, HD), jnp.bfloat16),
            pltpu.VMEM((rows, 2 * HD), jnp.bfloat16),
            pltpu.VMEM((3, BLOCK, LANES), jnp.float32),
            pltpu.VMEM((rows, 2 * HD), jnp.float32),
            pltpu.VMEM((4, HD, LANES), jnp.float32),
            pltpu.VMEM((4, 8, LANES), jnp.float32),
            pltpu.VMEM((4, 8, LANES), jnp.float32),
            pltpu.VMEM((4, 1, LANES), jnp.float32),
        ],
        compiler_params=pltpu.CompilerParams(vmem_limit_bytes=32 * 1024 * 1024),
        name="attention_grads",
    )(*lists, q_own, q_got, g_own, g_got, delta, *kv_parts)


def looked_up(table, index):
    return jnp.sum(jnp.where(index[..., None] == jnp.arange(table.shape[0]), table, 0), axis=-1)


def work_lists(block_order, block_mask, z, yh, c, nz):
    slot = jnp.arange(4 * 2 * nz, dtype=jnp.int32)
    core = c ^ ((slot // 2) % 2)
    chip = ((z - slot // 8) % nz) * 2 + (yh ^ ((slot // 4) % 2))
    key_block = looked_up(block_order, 2 * (2 * chip + core) + slot % 2)
    mine = slot[:4]
    query_block = looked_up(block_order, 2 * (2 * (2 * z + yh) + (c ^ (mine // 2))) + mine % 2)
    table = jnp.arange(block_mask.shape[0], dtype=jnp.int32)
    query_hot = query_block[:, None] == table
    key_hot = key_block[:, None] == table
    mask_rows = jnp.sum(jnp.where(query_hot[:, :, None], block_mask[None], 0), axis=1)
    live = jnp.sum(jnp.where(key_hot[None], mask_rows[:, None, :], 0), axis=-1) > 0
    place = jnp.sum(jnp.where(live[:, None, :] & (slot[None, :] < slot[:, None]), 1, 0), axis=-1)
    count = jnp.sum(live.astype(jnp.int32), axis=1)
    chosen = live[:, None, :] & (place[:, None, :] == slot[None, :, None])
    diagonal = key_block[None, :] == query_block[:, None]

    def packed(values):
        return jnp.sum(jnp.where(chosen, values, 0), axis=-1)

    slots = packed(jnp.broadcast_to(slot * BLOCK, chosen.shape)).reshape(-1)
    kinds = jnp.where(slot[None, :] < count[:, None], packed(diagonal[:, None, :].astype(jnp.int32)), 2).reshape(-1)
    slots = jnp.concatenate([slots, jnp.zeros((STEP,), jnp.int32)])
    kinds = jnp.concatenate([kinds, jnp.full((STEP,), 2, jnp.int32)])
    turns = (count + STEP - 1) // STEP
    upto = jnp.sum(jnp.where(mine[None, :] <= mine[:, None], turns[None, :], 0), axis=1)
    item = jnp.arange(4 * slot.shape[0] // STEP + 1, dtype=jnp.int32)
    query = jnp.sum((item[:, None] >= upto[None, :]).astype(jnp.int32), axis=1)
    before = jnp.sum(jnp.where(query[:, None] == mine[None, :] + 1, upto[None, :], 0), axis=1)
    start = jnp.where(query < 4, query * slot.shape[0] + STEP * (item - before), 4 * slot.shape[0])
    return slots, kinds, jnp.minimum(query, 3), start, ((upto[3] + 1) // 2)[None]


def query_part_kernel(z_ref, dq_ref, *refs):
    pieces, (part_ref, kv_ref, weight, sems) = refs[:-4], refs[-4:]
    z = z_ref[0]
    rows = 112
    copies = []
    for kind, parts in enumerate(PLACES):
        ref = pieces[kind]
        for i, (quarter, back) in enumerate(parts):
            shard = lax.rem(z + 8 - back, 8) * 4 + z_ref[1 + quarter]
            copies.append(
                pltpu.make_async_copy(
                    ref.at[pl.ds(i * rows, rows), :],
                    weight.at[pl.ds(pl.multiple_of(shard * rows, 16), rows), :],
                    sems.at[len(copies)],
                )
            )
    for copy in copies:
        copy.start()
    for copy in copies:
        copy.wait()
    wide = dq_ref.shape[1]
    dq = dq_ref[...]
    step = 512

    def columns(i, unused):
        cols = pl.ds(pl.multiple_of(i * step, step), step)
        part_ref[:, cols] = dot_nt(dq, weight[cols, 0:wide])
        kv_ref[cols, :] = weight[cols, wide:]
        return unused

    lax.fori_loop(0, part_ref.shape[1] // step, columns, 0)


ORDER = (0, 1, 7, 2, 6, 3, 5, 4)
PLACES = tuple(
    [[(0, back)] for back in ORDER]
    + [[(1, back) for back in ORDER[:4]], [(1, back) for back in ORDER[4:]]]
    + [[(2, back) for back in ORDER[:4]], [(2, back) for back in ORDER[4:]]]
    + [[(3, back) for back in ORDER[2 * i : 2 * i + 2]] for i in range(4)]
)


def query_part(where, dq, pieces):
    total = 4 * 8 * 112
    wide = dq.shape[1]
    return pl.pallas_call(
        query_part_kernel,
        out_shape=(
            jax.ShapeDtypeStruct((dq.shape[0], total), jnp.float32),
            jax.ShapeDtypeStruct((total, 2 * HD), jnp.bfloat16),
        ),
        in_specs=[SMEM, VMEM] + [ANY] * len(pieces),
        out_specs=(VMEM, VMEM),
        scratch_shapes=[
            pltpu.VMEM((total, wide + 2 * HD), jnp.bfloat16),
            pltpu.SemaphoreType.DMA((sum(len(p) for p in PLACES),)),
        ],
        compiler_params=pltpu.CompilerParams(vmem_limit_bytes=24 * 1024 * 1024),
        name="query_part",
    )(where, dq, *pieces)


def partial_kernel(rows_ref, dkv_ref, kv_ref, part_ref, keep_ref, send_ref, whole):
    tok = dkv_ref.shape[0] // 2
    step = 512
    dkv = dkv_ref[...]

    def columns(i, unused):
        cols = pl.ds(pl.multiple_of(i * step, step), step)
        whole[...] = part_ref[:, cols] + dot_nt(dkv, kv_ref[cols, :])
        keep_ref[0:tok, cols] = whole[0:tok, :]
        send_ref[0:tok, cols] = whole[tok:, :].astype(jnp.bfloat16)
        need = pl.ds(pl.multiple_of(tok + rows_ref[0], BLOCK), BLOCK)
        sent = pl.ds(pl.multiple_of(rows_ref[1], BLOCK), BLOCK)
        keep_ref[tok:, cols] = whole[need, :]
        send_ref[tok:, cols] = whole[sent, :].astype(jnp.bfloat16)
        return unused

    lax.fori_loop(0, part_ref.shape[1] // step, columns, 0)


def partial_sums(rows, dkv, kv_weight, part):
    out = 2 * BLOCK + BLOCK
    return pl.pallas_call(
        partial_kernel,
        out_shape=(
            jax.ShapeDtypeStruct((out, part.shape[1]), jnp.float32),
            jax.ShapeDtypeStruct((out, part.shape[1]), jnp.bfloat16),
        ),
        in_specs=[SMEM, VMEM, VMEM, VMEM],
        out_specs=(VMEM, VMEM),
        scratch_shapes=[pltpu.VMEM((part.shape[0], 512), jnp.float32)],
        compiler_params=pltpu.CompilerParams(vmem_limit_bytes=24 * 1024 * 1024),
        name="partial_sums",
    )(rows, dkv, kv_weight, part)


def final_kernel(
    rows_ref, keep_ref, got_ref, in_own, in_got, gain_ref, feature_ref, post_ref, projector_hbm,
    token_ref, encoder_ref, projector, frame, post, sem,
):
    load = pltpu.make_async_copy(projector_hbm, projector, sem)
    load.start()
    tok = in_own.shape[0]
    height = 16

    def token_rows(first, inputs):
        norm_grad = keep_ref[pl.ds(first, height), :] + got_ref[pl.ds(first, height), :].astype(jnp.float32)
        norm_grad = norm_grad.astype(jnp.bfloat16).astype(jnp.float32)
        inputs = inputs.astype(jnp.float32)
        inverse = lax.rsqrt(jnp.mean(inputs * inputs, axis=1, keepdims=True) + EPSILON)
        scaled = norm_grad * gain_ref[...]
        lean = inverse * inverse * inverse * jnp.mean(scaled * inputs, axis=1, keepdims=True)
        return (inverse * scaled - inputs * lean).astype(jnp.bfloat16)

    def own(i, unused):
        first = pl.multiple_of(i * height, height)
        token_ref[pl.ds(first, height), :] = token_rows(first, in_own[pl.ds(first, height), :])
        return unused

    def got(i, unused):
        first = pl.multiple_of(i * height, height)
        frame[pl.ds(pl.multiple_of(rows_ref[4] + first, height), height), :] = token_rows(
            tok + first, in_got[pl.ds(first, height), :]
        )
        return unused

    lax.fori_loop(0, tok // height, own, 0)
    lax.fori_loop(0, BLOCK // height, got, 0)
    frame[pl.ds(pl.multiple_of(rows_ref[3], BLOCK), BLOCK), :] = token_ref[
        pl.ds(pl.multiple_of(rows_ref[2], BLOCK), BLOCK), :
    ]
    features = feature_ref[...].astype(jnp.float32)
    centered = features - jnp.mean(features, axis=1, keepdims=True)
    deviation = lax.rsqrt(jnp.mean(centered * centered, axis=1, keepdims=True) + EPSILON)
    normed = centered * deviation
    load.wait()
    step = 384

    def columns(i, unused):
        cols = pl.ds(pl.multiple_of(i * step, 128), step)
        post[:, cols] = dot_nt(frame[...], projector[cols, :])
        return unused

    lax.fori_loop(0, post.shape[1] // step, columns, 0)
    weighted = post[...] * post_ref[...]
    encoder_ref[...] = (
        deviation
        * (
            weighted
            - jnp.mean(weighted, axis=1, keepdims=True)
            - normed * jnp.mean(weighted * normed, axis=1, keepdims=True)
        )
    ).astype(jnp.bfloat16)


def finished(rows, keep, got, in_own, in_got, gain, features, post_gain, projector):
    return pl.pallas_call(
        final_kernel,
        out_shape=(
            jax.ShapeDtypeStruct(in_own.shape, jnp.bfloat16),
            jax.ShapeDtypeStruct(features.shape, jnp.bfloat16),
        ),
        in_specs=[SMEM] + [VMEM] * 7 + [ANY],
        out_specs=(VMEM, VMEM),
        scratch_shapes=[
            pltpu.VMEM(projector.shape, jnp.bfloat16),
            pltpu.VMEM((2 * BLOCK, in_own.shape[1]), jnp.bfloat16),
            pltpu.VMEM((2 * BLOCK, projector.shape[0]), jnp.float32),
            pltpu.SemaphoreType.DMA,
        ],
        compiler_params=pltpu.CompilerParams(vmem_limit_bytes=32 * 1024 * 1024),
        name="finished",
    )(rows, keep, got, in_own, in_got, gain, features, post_gain, projector)


def swap_core(value):
    return lax.ppermute(value, "c", [(0, 1), (1, 0)])


def delta_rows(delta):
    return jnp.transpose(delta.reshape(2, BLOCK, GROUP), (0, 2, 1)).reshape(2, 1, LANES)


def body(
    queries,
    keys,
    values,
    out_grad,
    row_delta,
    layer_input,
    norm_gain,
    qkv_weight,
    block_order,
    block_mask,
    frame_owner,
    vision_features,
    post_gain,
    projector,
):
    nz, nx = lax.axis_size("z"), lax.axis_size("x")
    z, yh, c, x, yl = (lax.axis_index(name) for name in ("z", "yh", "c", "x", "yl"))
    wide = GROUP * HD
    tok_rows = queries.shape[0]

    def group_of(array, which, width):
        return lax.dynamic_slice_in_dim(array, which * width, width, 1)

    def kv_of(which):
        return jnp.concatenate([group_of(keys, which, HD), group_of(values, which, HD)], axis=1)

    def columns_of(which):
        return jnp.concatenate(
            [
                group_of(qkv_weight[:, : HQ * HD], which, wide),
                group_of(qkv_weight[:, HQ * HD :], which, HD),
                group_of(qkv_weight[:, HQ * HD :], KVH + which, HD),
            ],
            axis=1,
        )

    forward = [(i, (i + 1) % nz) for i in range(nz)]
    backward = [(i, (i - 1) % nz) for i in range(nz)]

    kv_chip = jnp.concatenate([kv_of(c), swap_core(kv_of(1 - c))], axis=0)
    kv_other = lax.ppermute(kv_chip, "yh", [(0, 1), (1, 0)])

    def index(yh_, c_, x_, yl_):
        return ((yh_ * 2 + c_) * nx + x_) * 2 + yl_

    across = [
        (index(x_ & 1, yl_, x_, 1 - yl_), index(1 - (x_ & 1), yl_, x_, yl_))
        for x_ in range(nx)
        for yl_ in range(2)
    ]
    from_y = lax.ppermute(qkv_weight, ("yh", "c", "x", "yl"), across)
    from_y, _ = lax.optimization_barrier((from_y, kv_other))
    qkv_weight = jnp.where(yh == x & 1, qkv_weight, from_y)
    mine, theirs = columns_of(c), columns_of(1 - c)
    handed = lax.ppermute(theirs, ("c", "yl"), [(0, 2), (3, 1)])
    quarter = jnp.where(c == yl, mine, handed)

    parts = {(0, 0): kv_chip, (0, 1): kv_other}
    ups, downs = [kv_chip, kv_other], [kv_chip, kv_other]
    weights = {0: quarter}
    weight_up = weight_down = quarter
    for k in range(1, nz // 2 + 1):
        for y in range(2):
            parts[k, y] = ups[y] = lax.ppermute(ups[y], "z", forward)
            if k < nz // 2:
                parts[nz - k, y] = downs[y] = lax.ppermute(downs[y], "z", backward)
        weight_up, weight_down, _ = lax.optimization_barrier((weight_up, weight_down, parts[k, 0]))
        weights[k] = weight_up = lax.ppermute(weight_up, "z", forward)
        if k < nz // 2:
            weights[nz - k] = weight_down = lax.ppermute(weight_down, "z", backward)
    kv_parts = [parts[k, y] for k in range(nz) for y in range(2)]

    def shift_x(value, by):
        return lax.ppermute(value, "x", [(i, (i + by) % nx) for i in range(nx)])

    def shift_y(value, by):
        return lax.ppermute(value, ("yh", "yl"), [(i, (i + by) % 4) for i in range(4)])

    near = jnp.concatenate([weights[k] for k in ORDER[:4]], axis=0)
    far = jnp.concatenate([weights[k] for k in ORDER[4:]], axis=0)
    x_near, x_far = shift_x(near, 1), shift_x(far, -1)
    y_near, y_far = shift_y(near, 1), shift_y(far, -1)

    q_own, g_own = group_of(queries, c, wide), group_of(out_grad, c, wide)
    q_got = swap_core(group_of(queries, 1 - c, wide))
    g_got = swap_core(group_of(out_grad, 1 - c, wide))
    delta_got = swap_core(delta_rows(group_of(row_delta, 1 - c, GROUP)))
    delta = jnp.concatenate([delta_rows(group_of(row_delta, c, GROUP)), delta_got], axis=0)

    my_index = (z * 2 + yh) * 2 + c
    frame_table = jnp.arange(frame_owner.shape[0], dtype=jnp.int32)
    my_frame = jnp.sum(jnp.where(frame_owner == my_index, frame_table, 0))
    my_block = looked_up(block_order, 2 * my_index)
    other_block = looked_up(block_order, 2 * (my_index ^ 1))
    keep_first = my_block // 2 == my_frame
    need_first = other_block // 2 == my_frame
    kept_block = jnp.where(keep_first, my_block, 2 * block_order.shape[0] // 2 - 1 - my_block)
    half = jnp.int32(BLOCK)
    kept_row = jnp.where(keep_first, 0, half)
    sent_row = half - kept_row
    need_row = jnp.where(need_first, 0, half)
    lead_row = jnp.where(kept_block % 2 == 0, 0, half)
    frame_rows = jnp.stack([need_row, sent_row, kept_row, lead_row, half - lead_row]).astype(jnp.int32)
    in_got = swap_core(lax.dynamic_slice_in_dim(layer_input, sent_row, BLOCK, 0))

    lists = work_lists(block_order, block_mask, z, yh, c, nz)
    dq, dkv = attention(lists, q_own, q_got, g_own, g_got, delta, kv_parts)

    chunks = dkv.reshape(nz, 2, 2 * tok_rows, 2 * HD)

    def added(a, b):
        return (a.astype(jnp.float32) + b.astype(jnp.float32)).astype(jnp.bfloat16)

    sums = {}
    ups = {y: chunks[nz // 2, y] for y in (1, 0)}
    downs = {y: chunks[nz // 2 - 1, y] for y in (1, 0)}
    for k in range(nz // 2 - 1, -1, -1):
        for y in (1, 0):
            ups[y] = lax.ppermute(ups[y], "z", forward)
            if k > 0:
                ups[y] = added(ups[y], chunks[nz - k, y])
                downs[y] = lax.ppermute(downs[y], "z", backward)
                if k > 1:
                    downs[y] = added(downs[y], chunks[k - 1, y])
        if k == nz // 2 - 1:
            first_turn = ups[0]
        if k == 1:
            late_turn = ups[1]
    for y in (1, 0):
        sums[y] = (
            ups[y].astype(jnp.float32) + downs[y].astype(jnp.float32) + chunks[0, y].astype(jnp.float32)
        )
    from_other = lax.ppermute(sums[1].astype(jnp.bfloat16), "yh", [(0, 1), (1, 0)])
    dkv_own = (sums[0] + from_other.astype(jnp.float32)).astype(jnp.bfloat16)

    (x_near, x_far, y_near, y_far), _ = lax.optimization_barrier(((x_near, x_far, y_near, y_far), first_turn))
    two = near.shape[0] // 2
    diagonals = [
        shift_x(y_near[:two], 1),
        shift_y(x_near[two:], 1),
        shift_x(y_far[:two], -1),
        shift_y(x_far[two:], -1),
    ]
    quarters = [(x & 1) * 2 + yl, (1 - (x & 1)) * 2 + yl, (x & 1) * 2 + 1 - yl, (1 - (x & 1)) * 2 + 1 - yl]
    where = jnp.stack([z] + quarters).astype(jnp.int32)
    late, _ = lax.optimization_barrier((dq, late_turn))
    part, kv_weight = query_part(
        where, late, [weights[k] for k in ORDER] + [x_near, x_far, y_near, y_far] + diagonals
    )
    keep, send = partial_sums(frame_rows, dkv_own, kv_weight, part)
    token_grad, encoder_grad = finished(
        frame_rows,
        keep,
        swap_core(send),
        layer_input,
        in_got,
        norm_gain[None],
        vision_features[0],
        post_gain[None],
        projector,
    )
    return (token_grad, encoder_grad[None])


def solution(mesh):
    grid = Mesh(mesh.devices.reshape(8, 2, 2, 4, 2), ("z", "yh", "c", "x", "yl"))
    both = ("x", "yl", "z", "yh", "c")
    placed = (
        P(both, None),
        P(both, None),
        P(both, None),
        P(both, None),
        P(both, None),
        P(both, None),
        P(),
        P(("z", "yh", "c"), None),
        P(("x", "yl")),
        P(("x", "yl"), None),
        P(("x", "yl")),
        P(both, None, None),
        P(),
        P(),
    )
    return jax.shard_map(
        body,
        mesh=grid,
        in_specs=placed,
        out_specs=(P(both, None), P(both, None, None)),
        check_vma=False,
    )
```

```python
import jax
import jax.numpy as jnp
from jax import lax
from jax.experimental import pallas as pl
from jax.experimental.pallas import tpu as pltpu
from jax.sharding import Mesh, PartitionSpec as P

HQ = 14
KVH = 2
HD = 128
GROUP = HQ // KVH
EPSILON = 1e-06
NEGATIVE = -1e30
BLOCK = 64
LANES = GROUP * BLOCK
STEP = 4


def dot_nt(a, b):
    return lax.dot_general(a, b, (((1,), (1,)), ((), ())), preferred_element_type=jnp.float32)


def dot_nn(a, b):
    return lax.dot_general(a, b, (((1,), (0,)), ((), ())), preferred_element_type=jnp.float32)


def dot_tn(a, b):
    return lax.dot_general(a, b, (((0,), (0,)), ((), ())), preferred_element_type=jnp.float32)


def attention_kernel(pieces, *refs):
    slot_ref, kind_ref, query_ref, start_ref, turns_ref, place_ref, own_ref, got_ref, delta_ref = refs[:9]
    kv_parts = refs[9 : 9 + pieces]
    dq_ref, dkv_ref = refs[9 + pieces : 11 + pieces]
    qs, gs, kv, bias, acc, dqt, tops, sums, lses = refs[11 + pieces :]
    wide = GROUP * HD
    scaling = HD ** (-0.5)
    to_log2 = scaling * 1.4426950408889634
    height = kv_parts[0].shape[0]
    rows = height * pieces
    for i, part in enumerate(kv_parts):
        kv[i * height : (i + 1) * height, :] = part[...]
    for a in range(4):
        ref = own_ref if a < 2 else got_ref
        first = (a % 2) * BLOCK
        for h in range(GROUP):
            into, cols = slice(h * BLOCK, (h + 1) * BLOCK), h * HD
            qs[a, into, :] = ref[first : first + BLOCK, cols : cols + HD]
            gs[a, into, :] = ref[first : first + BLOCK, wide + cols : wide + cols + HD]
    key_row = lax.broadcasted_iota(jnp.int32, (BLOCK, LANES), 0)
    query_row = lax.broadcasted_iota(jnp.int32, (BLOCK, LANES), 1) % BLOCK
    bias[0] = jnp.zeros((BLOCK, LANES), jnp.float32)
    bias[1] = jnp.where(key_row <= query_row, 0.0, NEGATIVE)
    bias[2] = jnp.full((BLOCK, LANES), NEGATIVE, jnp.float32)
    acc[...] = jnp.zeros(acc.shape, jnp.float32)
    dqt[...] = jnp.zeros(dqt.shape, jnp.float32)
    tops[...] = jnp.full(tops.shape, NEGATIVE, jnp.float32)
    sums[...] = jnp.zeros(sums.shape, jnp.float32)

    def slots_of(item):
        first = start_ref[item]
        return [pl.multiple_of(slot_ref[first + i], BLOCK) for i in range(STEP)]

    def gathered(slots, first):
        return jnp.concatenate([kv[pl.ds(row, BLOCK), first : first + HD] for row in slots], axis=0)

    def scores(item, a, keys):
        first = start_ref[item]
        mask = jnp.concatenate([bias[kind_ref[first + i]] for i in range(STEP)], axis=0)
        return dot_nt(keys, qs[a]) * to_log2 + mask

    def total(turn, unused):
        for item in (2 * turn, 2 * turn + 1):
            a = query_ref[item]
            score = scores(item, a, gathered(slots_of(item), 0)).reshape(STEP * BLOCK // 8, 8, LANES)
            top = tops[a]
            top_next = jnp.maximum(top, jnp.max(score, axis=0))
            sums[a] = sums[a] * jnp.exp2(top - top_next) + jnp.sum(jnp.exp2(score - top_next), axis=0)
            tops[a] = top_next
        return unused

    lax.fori_loop(0, turns_ref[0], total, 0)
    for a in range(4):
        top = tops[a]
        peak = jnp.max(top, axis=0, keepdims=True)
        whole = jnp.sum(sums[a] * jnp.exp2(top - peak), axis=0, keepdims=True)
        lses[a] = peak + jnp.log2(whole)

    def grads(turn, unused):
        for item in (2 * turn, 2 * turn + 1):
            a = query_ref[item]
            slots = slots_of(item)
            keys = gathered(slots, 0)
            values = gathered(slots, HD)
            prob = jnp.exp2(scores(item, a, keys) - lses[a])
            prob_grad = dot_nt(values, gs[a])
            score_grad = (prob * (prob_grad - delta_ref[a])).astype(jnp.bfloat16)
            value_add = dot_nn(prob.astype(jnp.bfloat16), gs[a])
            key_add = dot_nn(score_grad, qs[a])
            dqt[a] += dot_tn(keys, score_grad)
            for i, row in enumerate(slots):
                acc[pl.ds(row, BLOCK), 0:HD] += key_add[i * BLOCK : (i + 1) * BLOCK, :]
                acc[pl.ds(row, BLOCK), HD : 2 * HD] += value_add[i * BLOCK : (i + 1) * BLOCK, :]
        return unused

    lax.fori_loop(0, turns_ref[0], grads, 0)
    for a in range(4):
        dq = (dqt[a].T * scaling).astype(jnp.bfloat16)
        for h in range(GROUP):
            dq_ref[a * BLOCK : (a + 1) * BLOCK, h * HD : (h + 1) * HD] = dq[h * BLOCK : (h + 1) * BLOCK, :]
    scale = jnp.where(lax.broadcasted_iota(jnp.int32, (1, 2 * HD), 1) < HD, scaling, 1.0)
    chip = 4 * BLOCK

    def write(i, unused):
        source = pl.ds(pl.multiple_of(i * chip, chip), chip)
        target = pl.ds(pl.multiple_of(place_ref[i], chip), chip)
        dkv_ref[target, :] = (acc[source, :] * scale).astype(jnp.bfloat16)
        return unused

    lax.fori_loop(0, rows // chip, write, 0)


SMEM = pl.BlockSpec(memory_space=pltpu.SMEM)
VMEM = pl.BlockSpec(memory_space=pltpu.VMEM)
ANY = pl.BlockSpec(memory_space=pl.ANY)


def attention(lists, own, got, delta, kv_parts):
    pieces = len(kv_parts)
    rows = pieces * kv_parts[0].shape[0]
    return pl.pallas_call(
        lambda *refs: attention_kernel(pieces, *refs),
        out_shape=(
            jax.ShapeDtypeStruct((4 * BLOCK, GROUP * HD), jnp.bfloat16),
            jax.ShapeDtypeStruct((rows, 2 * HD), jnp.bfloat16),
        ),
        in_specs=[SMEM] * 6 + [VMEM] * (3 + pieces),
        out_specs=(VMEM, VMEM),
        scratch_shapes=[
            pltpu.VMEM((4, LANES, HD), jnp.bfloat16),
            pltpu.VMEM((4, LANES, HD), jnp.bfloat16),
            pltpu.VMEM((rows, 2 * HD), jnp.bfloat16),
            pltpu.VMEM((3, BLOCK, LANES), jnp.float32),
            pltpu.VMEM((rows, 2 * HD), jnp.float32),
            pltpu.VMEM((4, HD, LANES), jnp.float32),
            pltpu.VMEM((4, 8, LANES), jnp.float32),
            pltpu.VMEM((4, 8, LANES), jnp.float32),
            pltpu.VMEM((4, 1, LANES), jnp.float32),
        ],
        compiler_params=pltpu.CompilerParams(vmem_limit_bytes=32 * 1024 * 1024),
        name="attention_grads",
    )(*lists, own, got, delta, *kv_parts)


def looked_up(table, index):
    return jnp.sum(jnp.where(index[..., None] == jnp.arange(table.shape[0]), table, 0), axis=-1)


def work_lists(block_order, block_mask, z, yh, c, nz):
    slot = jnp.arange(4 * 2 * nz, dtype=jnp.int32)
    core = c ^ ((slot // 2) % 2)
    chip = ((z - slot // 8) % nz) * 2 + (yh ^ ((slot // 4) % 2))
    key_block = looked_up(block_order, 2 * (2 * chip + core) + slot % 2)
    mine = slot[:4]
    query_block = looked_up(block_order, 2 * (2 * (2 * z + yh) + (c ^ (mine // 2))) + mine % 2)
    table = jnp.arange(block_mask.shape[0], dtype=jnp.int32)
    query_hot = query_block[:, None] == table
    key_hot = key_block[:, None] == table
    mask_rows = jnp.sum(jnp.where(query_hot[:, :, None], block_mask[None], 0), axis=1)
    live = jnp.sum(jnp.where(key_hot[None], mask_rows[:, None, :], 0), axis=-1) > 0
    place = jnp.sum(jnp.where(live[:, None, :] & (slot[None, :] < slot[:, None]), 1, 0), axis=-1)
    count = jnp.sum(live.astype(jnp.int32), axis=1)
    chosen = live[:, None, :] & (place[:, None, :] == slot[None, :, None])
    diagonal = key_block[None, :] == query_block[:, None]

    def packed(values):
        return jnp.sum(jnp.where(chosen, values, 0), axis=-1)

    slots = packed(jnp.broadcast_to(slot * BLOCK, chosen.shape)).reshape(-1)
    kinds = jnp.where(slot[None, :] < count[:, None], packed(diagonal[:, None, :].astype(jnp.int32)), 2).reshape(-1)
    slots = jnp.concatenate([slots, jnp.zeros((STEP,), jnp.int32)])
    kinds = jnp.concatenate([kinds, jnp.full((STEP,), 2, jnp.int32)])
    turns = (count + STEP - 1) // STEP
    upto = jnp.sum(jnp.where(mine[None, :] <= mine[:, None], turns[None, :], 0), axis=1)
    item = jnp.arange(4 * slot.shape[0] // STEP + 1, dtype=jnp.int32)
    query = jnp.sum((item[:, None] >= upto[None, :]).astype(jnp.int32), axis=1)
    before = jnp.sum(jnp.where(query[:, None] == mine[None, :] + 1, upto[None, :], 0), axis=1)
    start = jnp.where(query < 4, query * slot.shape[0] + STEP * (item - before), 4 * slot.shape[0])
    return slots, kinds, jnp.minimum(query, 3), start, ((upto[3] + 1) // 2)[None], chip[::4] * 256


def query_part_kernel(z_ref, dq_ref, *refs):
    pieces, (part_ref, kv_ref, weight, sems) = refs[:-4], refs[-4:]
    z = z_ref[0]
    rows = 112
    copies = []
    for kind, parts in enumerate(PLACES):
        ref = pieces[kind]
        for i, (quarter, back) in enumerate(parts):
            shard = lax.rem(z + 8 - back, 8) * 4 + z_ref[1 + quarter]
            copies.append(
                pltpu.make_async_copy(
                    ref.at[pl.ds(i * rows, rows), :],
                    weight.at[pl.ds(pl.multiple_of(shard * rows, 16), rows), :],
                    sems.at[len(copies)],
                )
            )
    for copy in copies:
        copy.start()
    for copy in copies:
        copy.wait()
    wide = dq_ref.shape[1]
    dq = dq_ref[...]
    step = 512

    def columns(i, unused):
        cols = pl.ds(pl.multiple_of(i * step, step), step)
        part_ref[:, cols] = dot_nt(dq, weight[cols, 0:wide])
        kv_ref[cols, :] = weight[cols, wide:]
        return unused

    lax.fori_loop(0, part_ref.shape[1] // step, columns, 0)


ORDER = (0, 1, 7, 2, 6, 3, 5, 4)
PLACES = tuple(
    [[(0, back)] for back in ORDER]
    + [[(1, back) for back in ORDER[:4]], [(1, back) for back in ORDER[4:]]]
    + [[(2, back) for back in ORDER[:4]], [(2, back) for back in ORDER[4:]]]
    + [[(3, back) for back in ORDER[:4]]]
    + [[(3, back) for back in ORDER[4:6]], [(3, back) for back in ORDER[6:]]]
)


def query_part(where, dq, pieces):
    total = 4 * 8 * 112
    wide = dq.shape[1]
    return pl.pallas_call(
        query_part_kernel,
        out_shape=(
            jax.ShapeDtypeStruct((dq.shape[0], total), jnp.float32),
            jax.ShapeDtypeStruct((total, 2 * HD), jnp.bfloat16),
        ),
        in_specs=[SMEM, VMEM] + [ANY] * len(pieces),
        out_specs=(VMEM, VMEM),
        scratch_shapes=[
            pltpu.VMEM((total, wide + 2 * HD), jnp.bfloat16),
            pltpu.SemaphoreType.DMA((sum(len(p) for p in PLACES),)),
        ],
        compiler_params=pltpu.CompilerParams(vmem_limit_bytes=24 * 1024 * 1024),
        name="query_part",
    )(where, dq, *[in_hbm(piece) for piece in pieces])


def partial_kernel(rows_ref, spread_ref, kv_ref, part_ref, keep_ref, send_ref, whole, dkv_ref):
    chip = dkv_ref.shape[0]
    tok = chip // 2
    step = 512
    height = 32

    def total(i, unused):
        first = pl.multiple_of(i * height, height)
        dkv_sum = jnp.zeros((height, dkv_ref.shape[1]), jnp.float32)
        for source in range(spread_ref.shape[0] // chip):
            dkv_sum += spread_ref[pl.ds(source * chip + first, height), :].astype(jnp.float32)
        dkv_ref[pl.ds(first, height), :] = dkv_sum.astype(jnp.bfloat16)
        return unused

    lax.fori_loop(0, chip // height, total, 0)
    dkv = dkv_ref[...]

    def columns(i, unused):
        cols = pl.ds(pl.multiple_of(i * step, step), step)
        whole[...] = part_ref[:, cols] + dot_nt(dkv, kv_ref[cols, :])
        keep_ref[0:tok, cols] = whole[0:tok, :].astype(jnp.bfloat16)
        send_ref[0:tok, cols] = whole[tok:, :].astype(jnp.bfloat16)
        need = pl.ds(pl.multiple_of(tok + rows_ref[0], BLOCK), BLOCK)
        sent = pl.ds(pl.multiple_of(rows_ref[1], BLOCK), BLOCK)
        keep_ref[tok:, cols] = whole[need, :].astype(jnp.bfloat16)
        send_ref[tok:, cols] = whole[sent, :].astype(jnp.bfloat16)
        return unused

    lax.fori_loop(0, part_ref.shape[1] // step, columns, 0)


def partial_sums(rows, spread, kv_weight, part):
    out = 2 * BLOCK + BLOCK
    return pl.pallas_call(
        partial_kernel,
        out_shape=(
            jax.ShapeDtypeStruct((out, part.shape[1]), jnp.bfloat16),
            jax.ShapeDtypeStruct((out, part.shape[1]), jnp.bfloat16),
        ),
        in_specs=[SMEM, VMEM, VMEM, VMEM],
        out_specs=(VMEM, VMEM),
        scratch_shapes=[
            pltpu.VMEM((part.shape[0], 512), jnp.float32),
            pltpu.VMEM((part.shape[0], spread.shape[1]), jnp.bfloat16),
        ],
        compiler_params=pltpu.CompilerParams(vmem_limit_bytes=24 * 1024 * 1024),
        name="partial_sums",
    )(rows, spread, kv_weight, part)


def final_kernel(
    rows_ref, keep_ref, got_ref, in_own, swapped_ref, gain_ref, feature_ref, post_ref, projector_hbm,
    token_ref, encoder_ref, projector, frame, post, sem,
):
    load = pltpu.make_async_copy(projector_hbm, projector, sem)
    load.start()
    tok = in_own.shape[0]
    height = 16

    def token_rows(first, inputs):
        norm_grad = keep_ref[pl.ds(first, height), :].astype(jnp.float32) + got_ref[pl.ds(first, height), :].astype(jnp.float32)
        norm_grad = norm_grad.astype(jnp.bfloat16).astype(jnp.float32)
        inputs = inputs.astype(jnp.float32)
        inverse = lax.rsqrt(jnp.mean(inputs * inputs, axis=1, keepdims=True) + EPSILON)
        scaled = norm_grad * gain_ref[...]
        lean = inverse * inverse * inverse * jnp.mean(scaled * inputs, axis=1, keepdims=True)
        return (inverse * scaled - inputs * lean).astype(jnp.bfloat16)

    def own(i, unused):
        first = pl.multiple_of(i * height, height)
        token_ref[pl.ds(first, height), :] = token_rows(first, in_own[pl.ds(first, height), :])
        return unused

    def got(i, unused):
        first = pl.multiple_of(i * height, height)
        frame[pl.ds(pl.multiple_of(rows_ref[4] + first, height), height), :] = token_rows(
            tok + first,
            jnp.concatenate(
                [swapped_ref[pl.ds(tok + first, height), :], swapped_ref[pl.ds(tok + BLOCK + first, height), :]],
                axis=1,
            ),
        )
        return unused

    lax.fori_loop(0, tok // height, own, 0)
    lax.fori_loop(0, BLOCK // height, got, 0)
    frame[pl.ds(pl.multiple_of(rows_ref[3], BLOCK), BLOCK), :] = token_ref[
        pl.ds(pl.multiple_of(rows_ref[2], BLOCK), BLOCK), :
    ]
    features = feature_ref[...].astype(jnp.float32)
    centered = features - jnp.mean(features, axis=1, keepdims=True)
    deviation = lax.rsqrt(jnp.mean(centered * centered, axis=1, keepdims=True) + EPSILON)
    normed = centered * deviation
    load.wait()
    step = 384

    def columns(i, unused):
        cols = pl.ds(pl.multiple_of(i * step, 128), step)
        post[:, cols] = dot_nt(frame[...], projector[cols, :])
        return unused

    lax.fori_loop(0, post.shape[1] // step, columns, 0)
    weighted = post[...] * post_ref[...]
    encoder_ref[...] = (
        deviation
        * (
            weighted
            - jnp.mean(weighted, axis=1, keepdims=True)
            - normed * jnp.mean(weighted * normed, axis=1, keepdims=True)
        )
    ).astype(jnp.bfloat16)


def finished(rows, keep, got, in_own, in_got, gain, features, post_gain, projector):
    return pl.pallas_call(
        final_kernel,
        out_shape=(
            jax.ShapeDtypeStruct(in_own.shape, jnp.bfloat16),
            jax.ShapeDtypeStruct(features.shape, jnp.bfloat16),
        ),
        in_specs=[SMEM] + [VMEM] * 7 + [ANY],
        out_specs=(VMEM, VMEM),
        scratch_shapes=[
            pltpu.VMEM(projector.shape, jnp.bfloat16),
            pltpu.VMEM((2 * BLOCK, in_own.shape[1]), jnp.bfloat16),
            pltpu.VMEM((2 * BLOCK, projector.shape[0]), jnp.float32),
            pltpu.SemaphoreType.DMA,
        ],
        compiler_params=pltpu.CompilerParams(vmem_limit_bytes=32 * 1024 * 1024),
        name="finished",
    )(rows, keep, got, in_own, in_got, gain, features, post_gain, in_hbm(projector))


def swap_core(value):
    return lax.ppermute(value, "c", [(0, 1), (1, 0)])


def in_hbm(value):
    return pltpu.with_memory_space_constraint(value, pltpu.HBM)


def delta_rows(delta):
    return jnp.transpose(delta.reshape(2, BLOCK, GROUP), (0, 2, 1)).reshape(2, 1, LANES)


def program(
    queries,
    keys,
    values,
    out_grad,
    row_delta,
    layer_input,
    norm_gain,
    qkv_weight,
    block_order,
    block_mask,
    frame_owner,
    vision_features,
    post_gain,
    projector,
):
    nz, nx = lax.axis_size("z"), lax.axis_size("x")
    z, yh, c, x, yl = (lax.axis_index(name) for name in ("z", "yh", "c", "x", "yl"))
    wide = GROUP * HD

    def group_of(array, which, width):
        return lax.dynamic_slice_in_dim(array, which * width, width, 1)

    def kv_of(which):
        return jnp.concatenate([group_of(keys, which, HD), group_of(values, which, HD)], axis=1)

    def columns_of(which):
        return jnp.concatenate(
            [
                group_of(qkv_weight[:, : HQ * HD], which, wide),
                group_of(qkv_weight[:, HQ * HD :], which, HD),
                group_of(qkv_weight[:, HQ * HD :], KVH + which, HD),
            ],
            axis=1,
        )

    forward = [(i, (i + 1) % nz) for i in range(nz)]
    backward = [(i, (i - 1) % nz) for i in range(nz)]

    kv_chip = jnp.concatenate([kv_of(c), swap_core(kv_of(1 - c))], axis=0)
    kv_row = lax.ppermute(kv_chip, "yh", [(0, 1), (1, 0)])
    (qkv_weight, queries, out_grad, row_delta), _ = lax.optimization_barrier(
        ((qkv_weight, queries, out_grad, row_delta), kv_chip)
    )
    kv_pair = jnp.concatenate([kv_chip, kv_row], axis=0)

    def index(yh_, c_, x_, yl_):
        return ((yh_ * 2 + c_) * nx + x_) * 2 + yl_

    mine, theirs = columns_of(c), columns_of(1 - c)
    pairs_a, pairs_b = [], []
    for x_ in range(nx):
        for yl_ in range(2):
            home = x_ & 1
            pairs_a.append((index(home, yl_, x_, yl_), index(home, 1 - yl_, x_, yl_)))
            source = index(home, yl_, x_, 1 - yl_)
            pairs_a.append((source, index(1 - home, yl_, x_, yl_)))
            pairs_b.append((source, index(1 - home, 1 - yl_, x_, yl_)))
    plane = ("yh", "c", "x", "yl")
    weight_a = lax.ppermute(jnp.where(c == yl, theirs, mine), plane, pairs_a)
    weight_b = lax.ppermute(theirs, plane, pairs_b)
    quarter = jnp.where(c == yl, jnp.where(yh == x & 1, mine, weight_a), jnp.where(yh == x & 1, weight_a, weight_b))

    kv_parts = {0: kv_pair}
    weights = {0: quarter}
    kv_up = kv_down = kv_pair
    weight_up = weight_down = quarter
    for k in range(1, nz // 2 + 1):
        kv_parts[k] = kv_up = lax.ppermute(kv_up, "z", forward)
        if k < nz // 2:
            kv_parts[nz - k] = kv_down = lax.ppermute(kv_down, "z", backward)
        if k < 3:
            weights[k] = weight_up = lax.ppermute(weight_up, "z", forward)
            weights[nz - k] = weight_down = lax.ppermute(weight_down, "z", backward)
    weights[3] = lax.ppermute(weight_up, "z", forward)
    weights[nz - 3] = lax.ppermute(weight_down, "z", backward)
    weights[4] = lax.ppermute(weight_up, "z", [(i, (i + 2) % nz) for i in range(nz)])
    block_mask, _ = lax.optimization_barrier((block_mask, kv_parts[1]))

    def shift_x(value, by):
        return lax.ppermute(value, "x", [(i, (i + by) % nx) for i in range(nx)])

    def shift_y(value, by):
        return lax.ppermute(value, ("yh", "yl"), [(i, (i + by) % 4) for i in range(4)])

    near = jnp.concatenate([weights[k] for k in ORDER[:4]], axis=0)
    far = jnp.concatenate([weights[k] for k in ORDER[4:]], axis=0)
    x_near, x_far = shift_x(near, 1), shift_x(far, -1)
    y_near, y_far = shift_y(near, 1), shift_y(far, -1)
    corner_near = shift_x(y_near, 1)

    my_index = (z * 2 + yh) * 2 + c
    frame_table = jnp.arange(frame_owner.shape[0], dtype=jnp.int32)
    my_frame = jnp.sum(jnp.where(frame_owner == my_index, frame_table, 0))
    my_block = looked_up(block_order, 2 * my_index)
    other_block = looked_up(block_order, 2 * (my_index ^ 1))
    keep_first = my_block // 2 == my_frame
    need_first = other_block // 2 == my_frame
    kept_block = jnp.where(keep_first, my_block, 2 * block_order.shape[0] // 2 - 1 - my_block)
    half = jnp.int32(BLOCK)
    kept_row = jnp.where(keep_first, 0, half)
    sent_row = half - kept_row
    need_row = jnp.where(need_first, 0, half)
    lead_row = jnp.where(kept_block % 2 == 0, 0, half)
    frame_rows = jnp.stack([need_row, sent_row, kept_row, lead_row, half - lead_row]).astype(jnp.int32)
    half_in = lax.dynamic_slice_in_dim(layer_input, sent_row, BLOCK, 0)
    middle = half_in.shape[1] // 2

    def tokens_of(which):
        return jnp.concatenate([group_of(queries, which, wide), group_of(out_grad, which, wide)], axis=1)

    own = tokens_of(c)
    got = swap_core(jnp.concatenate([tokens_of(1 - c), half_in[:, :middle], half_in[:, middle:]], axis=0))
    delta_got = swap_core(delta_rows(group_of(row_delta, 1 - c, GROUP)))
    delta = jnp.concatenate([delta_rows(group_of(row_delta, c, GROUP)), delta_got], axis=0)

    lists = work_lists(block_order, block_mask, z, yh, c, nz)
    dq, dkv = attention(lists, own, got, delta, [kv_parts[k] for k in range(nz)])

    spread = lax.all_to_all(dkv, ("z", "yh"), 0, 0, tiled=True)

    two = near.shape[0] // 2
    diagonals = [corner_near, shift_x(y_far[:two], -1), shift_y(x_far[two:], -1)]
    quarters = [(x & 1) * 2 + yl, (1 - (x & 1)) * 2 + yl, (x & 1) * 2 + 1 - yl, (1 - (x & 1)) * 2 + 1 - yl]
    where = jnp.stack([z] + quarters).astype(jnp.int32)
    part, kv_weight = query_part(
        where, dq, [weights[k] for k in ORDER] + [x_near, x_far, y_near, y_far] + diagonals
    )
    keep, send = partial_sums(frame_rows, spread, kv_weight, part)
    token_grad, encoder_grad = finished(
        frame_rows,
        keep,
        swap_core(send),
        layer_input,
        got,
        norm_gain[None],
        vision_features[0],
        post_gain[None],
        projector,
    )
    return (token_grad, encoder_grad[None])


def solution(mesh):
    grid = Mesh(mesh.devices.reshape(8, 2, 2, 4, 2), ("z", "yh", "c", "x", "yl"))
    both = ("x", "yl", "z", "yh", "c")
    placed = (
        P(both, None),
        P(both, None),
        P(both, None),
        P(both, None),
        P(both, None),
        P(both, None),
        P(),
        P(("z", "yh", "c"), None),
        P(("x", "yl")),
        P(("x", "yl"), None),
        P(("x", "yl")),
        P(both, None, None),
        P(),
        P(),
    )
    return jax.shard_map(
        program,
        mesh=grid,
        in_specs=placed,
        out_specs=(P(both, None), P(both, None, None)),
        check_vma=False,
    )
```

```python
import jax
import jax.numpy as jnp
from jax import lax
from jax.experimental import pallas as pl
from jax.experimental.pallas import tpu as pltpu
from jax.sharding import Mesh, PartitionSpec as P

HQ = 14
KVH = 2
HD = 128
GROUP = HQ // KVH
EPSILON = 1e-06
NEGATIVE = -1e30
BLOCK = 64
LANES = GROUP * BLOCK
STEP = 4


def dot_nt(a, b):
    return lax.dot_general(a, b, (((1,), (1,)), ((), ())), preferred_element_type=jnp.float32)


def dot_nn(a, b):
    return lax.dot_general(a, b, (((1,), (0,)), ((), ())), preferred_element_type=jnp.float32)


def dot_tn(a, b):
    return lax.dot_general(a, b, (((0,), (0,)), ((), ())), preferred_element_type=jnp.float32)


def attention_kernel(pieces, *refs):
    slot_ref, kind_ref, query_ref, start_ref, turns_ref, place_ref, own_ref, got_ref, delta_ref = refs[:9]
    kv_parts = refs[9 : 9 + pieces]
    dq_ref, dkv_ref = refs[9 + pieces : 11 + pieces]
    qs, gs, kv, bias, acc, dqt, tops, sums, lses = refs[11 + pieces :]
    wide = GROUP * HD
    scaling = HD ** (-0.5)
    to_log2 = scaling * 1.4426950408889634
    height = kv_parts[0].shape[0]
    rows = height * pieces
    for i, part in enumerate(kv_parts):
        kv[i * height : (i + 1) * height, :] = part[...]
    for a in range(4):
        ref = own_ref if a < 2 else got_ref
        first = (a % 2) * BLOCK
        for h in range(GROUP):
            into, cols = slice(h * BLOCK, (h + 1) * BLOCK), h * HD
            qs[a, into, :] = ref[first : first + BLOCK, cols : cols + HD]
            gs[a, into, :] = ref[first : first + BLOCK, wide + cols : wide + cols + HD]
    key_row = lax.broadcasted_iota(jnp.int32, (BLOCK, LANES), 0)
    query_row = lax.broadcasted_iota(jnp.int32, (BLOCK, LANES), 1) % BLOCK
    bias[0] = jnp.zeros((BLOCK, LANES), jnp.float32)
    bias[1] = jnp.where(key_row <= query_row, 0.0, NEGATIVE)
    bias[2] = jnp.full((BLOCK, LANES), NEGATIVE, jnp.float32)
    acc[...] = jnp.zeros(acc.shape, jnp.float32)
    dqt[...] = jnp.zeros(dqt.shape, jnp.float32)
    tops[...] = jnp.full(tops.shape, NEGATIVE, jnp.float32)
    sums[...] = jnp.zeros(sums.shape, jnp.float32)

    def slots_of(item):
        first = start_ref[item]
        return [pl.multiple_of(slot_ref[first + i], BLOCK) for i in range(STEP)]

    def gathered(slots, first):
        return jnp.concatenate([kv[pl.ds(row, BLOCK), first : first + HD] for row in slots], axis=0)

    def scores(item, a, keys):
        first = start_ref[item]
        mask = jnp.concatenate([bias[kind_ref[first + i]] for i in range(STEP)], axis=0)
        return dot_nt(keys, qs[a]) * to_log2 + mask

    def total(turn, unused):
        for item in (2 * turn, 2 * turn + 1):
            a = query_ref[item]
            score = scores(item, a, gathered(slots_of(item), 0)).reshape(STEP * BLOCK // 8, 8, LANES)
            top = tops[a]
            top_next = jnp.maximum(top, jnp.max(score, axis=0))
            sums[a] = sums[a] * jnp.exp2(top - top_next) + jnp.sum(jnp.exp2(score - top_next), axis=0)
            tops[a] = top_next
        return unused

    lax.fori_loop(0, turns_ref[0], total, 0)
    for a in range(4):
        top = tops[a]
        peak = jnp.max(top, axis=0, keepdims=True)
        whole = jnp.sum(sums[a] * jnp.exp2(top - peak), axis=0, keepdims=True)
        lses[a] = peak + jnp.log2(whole)

    def grads(turn, unused):
        for item in (2 * turn, 2 * turn + 1):
            a = query_ref[item]
            slots = slots_of(item)
            keys = gathered(slots, 0)
            values = gathered(slots, HD)
            prob = jnp.exp2(scores(item, a, keys) - lses[a])
            prob_grad = dot_nt(values, gs[a])
            score_grad = (prob * (prob_grad - delta_ref[a])).astype(jnp.bfloat16)
            value_add = dot_nn(prob.astype(jnp.bfloat16), gs[a])
            key_add = dot_nn(score_grad, qs[a])
            dqt[a] += dot_tn(keys, score_grad)
            for i, row in enumerate(slots):
                acc[pl.ds(row, BLOCK), 0:HD] += key_add[i * BLOCK : (i + 1) * BLOCK, :]
                acc[pl.ds(row, BLOCK), HD : 2 * HD] += value_add[i * BLOCK : (i + 1) * BLOCK, :]
        return unused

    lax.fori_loop(0, turns_ref[0], grads, 0)
    for a in range(4):
        dq = (dqt[a].T * scaling).astype(jnp.bfloat16)
        for h in range(GROUP):
            dq_ref[a * BLOCK : (a + 1) * BLOCK, h * HD : (h + 1) * HD] = dq[h * BLOCK : (h + 1) * BLOCK, :]
    scale = jnp.where(lax.broadcasted_iota(jnp.int32, (1, 2 * HD), 1) < HD, scaling, 1.0)
    chip = 4 * BLOCK

    def write(i, unused):
        source = pl.ds(pl.multiple_of(i * chip, chip), chip)
        target = pl.ds(pl.multiple_of(place_ref[i], chip), chip)
        dkv_ref[target, :] = (acc[source, :] * scale).astype(jnp.bfloat16)
        return unused

    lax.fori_loop(0, rows // chip, write, 0)


SMEM = pl.BlockSpec(memory_space=pltpu.SMEM)
VMEM = pl.BlockSpec(memory_space=pltpu.VMEM)
ANY = pl.BlockSpec(memory_space=pl.ANY)


def attention(lists, own, got, delta, kv_parts):
    pieces = len(kv_parts)
    rows = pieces * kv_parts[0].shape[0]
    return pl.pallas_call(
        lambda *refs: attention_kernel(pieces, *refs),
        out_shape=(
            jax.ShapeDtypeStruct((4 * BLOCK, GROUP * HD), jnp.bfloat16),
            jax.ShapeDtypeStruct((rows, 2 * HD), jnp.bfloat16),
        ),
        in_specs=[SMEM] * 6 + [VMEM] * (3 + pieces),
        out_specs=(VMEM, VMEM),
        scratch_shapes=[
            pltpu.VMEM((4, LANES, HD), jnp.bfloat16),
            pltpu.VMEM((4, LANES, HD), jnp.bfloat16),
            pltpu.VMEM((rows, 2 * HD), jnp.bfloat16),
            pltpu.VMEM((3, BLOCK, LANES), jnp.float32),
            pltpu.VMEM((rows, 2 * HD), jnp.float32),
            pltpu.VMEM((4, HD, LANES), jnp.float32),
            pltpu.VMEM((4, 8, LANES), jnp.float32),
            pltpu.VMEM((4, 8, LANES), jnp.float32),
            pltpu.VMEM((4, 1, LANES), jnp.float32),
        ],
        compiler_params=pltpu.CompilerParams(vmem_limit_bytes=32 * 1024 * 1024),
        name="attention_grads",
    )(*lists, own, got, delta, *kv_parts)


def looked_up(table, index):
    return jnp.sum(jnp.where(index[..., None] == jnp.arange(table.shape[0]), table, 0), axis=-1)


def work_lists(block_order, block_mask, z, yh, c, nz):
    slot = jnp.arange(4 * 2 * nz, dtype=jnp.int32)
    core = c ^ ((slot // 2) % 2)
    chip = ((z - slot // 8) % nz) * 2 + (yh ^ ((slot // 4) % 2))
    key_block = looked_up(block_order, 2 * (2 * chip + core) + slot % 2)
    mine = slot[:4]
    query_block = looked_up(block_order, 2 * (2 * (2 * z + yh) + (c ^ (mine // 2))) + mine % 2)
    table = jnp.arange(block_mask.shape[0], dtype=jnp.int32)
    query_hot = query_block[:, None] == table
    key_hot = key_block[:, None] == table
    mask_rows = jnp.sum(jnp.where(query_hot[:, :, None], block_mask[None], 0), axis=1)
    live = jnp.sum(jnp.where(key_hot[None], mask_rows[:, None, :], 0), axis=-1) > 0
    place = jnp.sum(jnp.where(live[:, None, :] & (slot[None, :] < slot[:, None]), 1, 0), axis=-1)
    count = jnp.sum(live.astype(jnp.int32), axis=1)
    chosen = live[:, None, :] & (place[:, None, :] == slot[None, :, None])
    diagonal = key_block[None, :] == query_block[:, None]

    def packed(values):
        return jnp.sum(jnp.where(chosen, values, 0), axis=-1)

    slots = packed(jnp.broadcast_to(slot * BLOCK, chosen.shape)).reshape(-1)
    kinds = jnp.where(slot[None, :] < count[:, None], packed(diagonal[:, None, :].astype(jnp.int32)), 2).reshape(-1)
    slots = jnp.concatenate([slots, jnp.zeros((STEP,), jnp.int32)])
    kinds = jnp.concatenate([kinds, jnp.full((STEP,), 2, jnp.int32)])
    turns = (count + STEP - 1) // STEP
    upto = jnp.sum(jnp.where(mine[None, :] <= mine[:, None], turns[None, :], 0), axis=1)
    item = jnp.arange(4 * slot.shape[0] // STEP + 1, dtype=jnp.int32)
    query = jnp.sum((item[:, None] >= upto[None, :]).astype(jnp.int32), axis=1)
    before = jnp.sum(jnp.where(query[:, None] == mine[None, :] + 1, upto[None, :], 0), axis=1)
    start = jnp.where(query < 4, query * slot.shape[0] + STEP * (item - before), 4 * slot.shape[0])
    return slots, kinds, jnp.minimum(query, 3), start, ((upto[3] + 1) // 2)[None], chip[::4] * 256


def query_part_kernel(z_ref, dq_ref, *refs):
    pieces, (part_ref, kv_ref, weight, sems) = refs[:-4], refs[-4:]
    z = z_ref[0]
    rows = 112
    copies = []
    for kind, parts in enumerate(PLACES):
        ref = pieces[kind]
        for i, (quarter, back) in enumerate(parts):
            shard = lax.rem(z + 8 - back, 8) * 4 + z_ref[1 + quarter]
            copies.append(
                pltpu.make_async_copy(
                    ref.at[pl.ds(i * rows, rows), :],
                    weight.at[pl.ds(pl.multiple_of(shard * rows, 16), rows), :],
                    sems.at[len(copies)],
                )
            )
    for copy in copies:
        copy.start()
    for copy in copies:
        copy.wait()
    wide = dq_ref.shape[1]
    dq = dq_ref[...]
    step = 512

    def columns(i, unused):
        cols = pl.ds(pl.multiple_of(i * step, step), step)
        part_ref[:, cols] = dot_nt(dq, weight[cols, 0:wide])
        kv_ref[cols, :] = weight[cols, wide:]
        return unused

    lax.fori_loop(0, part_ref.shape[1] // step, columns, 0)


ORDER = (0, 1, 7, 2, 6, 3, 5, 4)
NEAR, FAR = ORDER[:5], ORDER[5:]
PLACES = tuple(
    [[(0, back)] for back in ORDER]
    + [[(kind, back) for back in side] for kind in (1, 2, 3) for side in (NEAR, FAR)]
)


def query_part(where, dq, pieces):
    total = 4 * 8 * 112
    wide = dq.shape[1]
    return pl.pallas_call(
        query_part_kernel,
        out_shape=(
            jax.ShapeDtypeStruct((dq.shape[0], total), jnp.float32),
            jax.ShapeDtypeStruct((total, 2 * HD), jnp.bfloat16),
        ),
        in_specs=[SMEM, VMEM] + [ANY] * len(pieces),
        out_specs=(VMEM, VMEM),
        scratch_shapes=[
            pltpu.VMEM((total, wide + 2 * HD), jnp.bfloat16),
            pltpu.SemaphoreType.DMA((sum(len(p) for p in PLACES),)),
        ],
        compiler_params=pltpu.CompilerParams(vmem_limit_bytes=24 * 1024 * 1024),
        name="query_part",
    )(where, dq, *[in_hbm(piece) for piece in pieces])


def partial_kernel(rows_ref, spread_ref, kv_ref, part_ref, keep_ref, send_ref, whole, dkv_ref):
    chip = dkv_ref.shape[0]
    tok = chip // 2
    step = 512
    height = 32

    def total(i, unused):
        first = pl.multiple_of(i * height, height)
        dkv_sum = jnp.zeros((height, dkv_ref.shape[1]), jnp.float32)
        for source in range(spread_ref.shape[0] // chip):
            dkv_sum += spread_ref[pl.ds(source * chip + first, height), :].astype(jnp.float32)
        dkv_ref[pl.ds(first, height), :] = dkv_sum.astype(jnp.bfloat16)
        return unused

    lax.fori_loop(0, chip // height, total, 0)
    dkv = dkv_ref[...]

    def columns(i, unused):
        cols = pl.ds(pl.multiple_of(i * step, step), step)
        whole[...] = part_ref[:, cols] + dot_nt(dkv, kv_ref[cols, :])
        keep_ref[0:tok, cols] = whole[0:tok, :].astype(jnp.bfloat16)
        send_ref[0:tok, cols] = whole[tok:, :].astype(jnp.bfloat16)
        need = pl.ds(pl.multiple_of(tok + rows_ref[0], BLOCK), BLOCK)
        sent = pl.ds(pl.multiple_of(rows_ref[1], BLOCK), BLOCK)
        keep_ref[tok:, cols] = whole[need, :].astype(jnp.bfloat16)
        send_ref[tok:, cols] = whole[sent, :].astype(jnp.bfloat16)
        return unused

    lax.fori_loop(0, part_ref.shape[1] // step, columns, 0)


def partial_sums(rows, spread, kv_weight, part):
    out = 2 * BLOCK + BLOCK
    return pl.pallas_call(
        partial_kernel,
        out_shape=(
            jax.ShapeDtypeStruct((out, part.shape[1]), jnp.bfloat16),
            jax.ShapeDtypeStruct((out, part.shape[1]), jnp.bfloat16),
        ),
        in_specs=[SMEM, VMEM, VMEM, VMEM],
        out_specs=(VMEM, VMEM),
        scratch_shapes=[
            pltpu.VMEM((part.shape[0], 512), jnp.float32),
            pltpu.VMEM((part.shape[0], spread.shape[1]), jnp.bfloat16),
        ],
        compiler_params=pltpu.CompilerParams(vmem_limit_bytes=24 * 1024 * 1024),
        name="partial_sums",
    )(rows, spread, in_hbm(kv_weight), in_hbm(part))


def final_kernel(
    rows_ref, keep_ref, got_ref, in_own, swapped_ref, gain_ref, feature_ref, post_ref, projector_hbm,
    token_ref, encoder_ref, projector, frame, post, sem,
):
    load = pltpu.make_async_copy(projector_hbm, projector, sem)
    load.start()
    tok = in_own.shape[0]
    height = 16

    def token_rows(first, inputs):
        norm_grad = keep_ref[pl.ds(first, height), :].astype(jnp.float32) + got_ref[pl.ds(first, height), :].astype(jnp.float32)
        norm_grad = norm_grad.astype(jnp.bfloat16).astype(jnp.float32)
        inputs = inputs.astype(jnp.float32)
        inverse = lax.rsqrt(jnp.mean(inputs * inputs, axis=1, keepdims=True) + EPSILON)
        scaled = norm_grad * gain_ref[...]
        lean = inverse * inverse * inverse * jnp.mean(scaled * inputs, axis=1, keepdims=True)
        return (inverse * scaled - inputs * lean).astype(jnp.bfloat16)

    def own(i, unused):
        first = pl.multiple_of(i * height, height)
        token_ref[pl.ds(first, height), :] = token_rows(first, in_own[pl.ds(first, height), :])
        return unused

    def got(i, unused):
        first = pl.multiple_of(i * height, height)
        frame[pl.ds(pl.multiple_of(rows_ref[4] + first, height), height), :] = token_rows(
            tok + first,
            jnp.concatenate(
                [swapped_ref[pl.ds(tok + first, height), :], swapped_ref[pl.ds(tok + BLOCK + first, height), :]],
                axis=1,
            ),
        )
        return unused

    lax.fori_loop(0, tok // height, own, 0)
    lax.fori_loop(0, BLOCK // height, got, 0)
    frame[pl.ds(pl.multiple_of(rows_ref[3], BLOCK), BLOCK), :] = token_ref[
        pl.ds(pl.multiple_of(rows_ref[2], BLOCK), BLOCK), :
    ]
    features = feature_ref[...].astype(jnp.float32)
    centered = features - jnp.mean(features, axis=1, keepdims=True)
    deviation = lax.rsqrt(jnp.mean(centered * centered, axis=1, keepdims=True) + EPSILON)
    normed = centered * deviation
    load.wait()
    step = 384

    def columns(i, unused):
        cols = pl.ds(pl.multiple_of(i * step, 128), step)
        post[:, cols] = dot_nt(frame[...], projector[cols, :])
        return unused

    lax.fori_loop(0, post.shape[1] // step, columns, 0)
    weighted = post[...] * post_ref[...]
    encoder_ref[...] = (
        deviation
        * (
            weighted
            - jnp.mean(weighted, axis=1, keepdims=True)
            - normed * jnp.mean(weighted * normed, axis=1, keepdims=True)
        )
    ).astype(jnp.bfloat16)


def finished(rows, keep, got, in_own, in_got, gain, features, post_gain, projector):
    return pl.pallas_call(
        final_kernel,
        out_shape=(
            jax.ShapeDtypeStruct(in_own.shape, jnp.bfloat16),
            jax.ShapeDtypeStruct(features.shape, jnp.bfloat16),
        ),
        in_specs=[SMEM] + [VMEM] * 7 + [ANY],
        out_specs=(VMEM, VMEM),
        scratch_shapes=[
            pltpu.VMEM(projector.shape, jnp.bfloat16),
            pltpu.VMEM((2 * BLOCK, in_own.shape[1]), jnp.bfloat16),
            pltpu.VMEM((2 * BLOCK, projector.shape[0]), jnp.float32),
            pltpu.SemaphoreType.DMA,
        ],
        compiler_params=pltpu.CompilerParams(vmem_limit_bytes=32 * 1024 * 1024),
        name="finished",
    )(rows, keep, got, in_own, in_got, gain, features, post_gain, in_hbm(projector))


def swap_core(value):
    return lax.ppermute(value, "c", [(0, 1), (1, 0)])


def in_hbm(value):
    return pltpu.with_memory_space_constraint(value, pltpu.HBM)


def delta_rows(delta):
    return jnp.transpose(delta.reshape(2, BLOCK, GROUP), (0, 2, 1)).reshape(2, 1, LANES)


def program(
    queries,
    keys,
    values,
    out_grad,
    row_delta,
    layer_input,
    norm_gain,
    qkv_weight,
    block_order,
    block_mask,
    frame_owner,
    vision_features,
    post_gain,
    projector,
):
    nz, nx = lax.axis_size("z"), lax.axis_size("x")
    z, yh, c, x, yl = (lax.axis_index(name) for name in ("z", "yh", "c", "x", "yl"))
    wide = GROUP * HD

    def group_of(array, which, width):
        return lax.dynamic_slice_in_dim(array, which * width, width, 1)

    def kv_of(which):
        return jnp.concatenate([group_of(keys, which, HD), group_of(values, which, HD)], axis=1)

    def columns_of(which):
        return jnp.concatenate(
            [
                group_of(qkv_weight[:, : HQ * HD], which, wide),
                group_of(qkv_weight[:, HQ * HD :], which, HD),
                group_of(qkv_weight[:, HQ * HD :], KVH + which, HD),
            ],
            axis=1,
        )

    forward = [(i, (i + 1) % nz) for i in range(nz)]
    backward = [(i, (i - 1) % nz) for i in range(nz)]

    kv_chip = jnp.concatenate([kv_of(c), swap_core(kv_of(1 - c))], axis=0)
    kv_row = lax.ppermute(kv_chip, "yh", [(0, 1), (1, 0)])
    (qkv_weight, queries, out_grad, row_delta), _ = lax.optimization_barrier(
        ((qkv_weight, queries, out_grad, row_delta), kv_chip)
    )
    kv_pair = jnp.concatenate([kv_chip, kv_row], axis=0)

    def index(yh_, c_, x_, yl_):
        return ((yh_ * 2 + c_) * nx + x_) * 2 + yl_

    mine, theirs = columns_of(c), columns_of(1 - c)
    pairs_a, pairs_b = [], []
    for x_ in range(nx):
        for yl_ in range(2):
            home = x_ & 1
            pairs_a.append((index(home, yl_, x_, yl_), index(home, 1 - yl_, x_, yl_)))
            source = index(home, yl_, x_, 1 - yl_)
            pairs_a.append((source, index(1 - home, yl_, x_, yl_)))
            pairs_b.append((source, index(1 - home, 1 - yl_, x_, yl_)))
    plane = ("yh", "c", "x", "yl")
    weight_a = lax.ppermute(jnp.where(c == yl, theirs, mine), plane, pairs_a)
    weight_b = lax.ppermute(theirs, plane, pairs_b)
    quarter = jnp.where(c == yl, jnp.where(yh == x & 1, mine, weight_a), jnp.where(yh == x & 1, weight_a, weight_b))

    kv_parts = {0: kv_pair}
    weights = {0: quarter}
    kv_up = kv_down = kv_pair
    weight_up = weight_down = quarter
    for k in range(1, nz // 2 + 1):
        kv_parts[k] = kv_up = lax.ppermute(kv_up, "z", forward)
        if k < nz // 2:
            kv_parts[nz - k] = kv_down = lax.ppermute(kv_down, "z", backward)
        if k < 3:
            weights[k] = weight_up = lax.ppermute(weight_up, "z", forward)
            weights[nz - k] = weight_down = lax.ppermute(weight_down, "z", backward)
    weights[3] = lax.ppermute(weight_up, "z", forward)
    weights[nz - 3] = lax.ppermute(weight_down, "z", backward)
    weights[4] = lax.ppermute(weight_up, "z", [(i, (i + 2) % nz) for i in range(nz)])
    (block_order, block_mask, frame_owner), _ = lax.optimization_barrier(
        ((block_order, block_mask, frame_owner), kv_parts[1])
    )

    def shift_x(value, by):
        return lax.ppermute(value, "x", [(i, (i + by) % nx) for i in range(nx)])

    def shift_y(value, by):
        return lax.ppermute(value, ("yh", "yl"), [(i, (i + by) % 4) for i in range(4)])

    near = jnp.concatenate([weights[k] for k in NEAR], axis=0)
    x_near, y_near = shift_x(near, 1), shift_y(near, 1)
    corner_near = shift_x(y_near, 1)

    my_index = (z * 2 + yh) * 2 + c
    frame_table = jnp.arange(frame_owner.shape[0], dtype=jnp.int32)
    my_frame = jnp.sum(jnp.where(frame_owner == my_index, frame_table, 0))
    my_block = looked_up(block_order, 2 * my_index)
    other_block = looked_up(block_order, 2 * (my_index ^ 1))
    keep_first = my_block // 2 == my_frame
    need_first = other_block // 2 == my_frame
    kept_block = jnp.where(keep_first, my_block, 2 * block_order.shape[0] // 2 - 1 - my_block)
    half = jnp.int32(BLOCK)
    kept_row = jnp.where(keep_first, 0, half)
    sent_row = half - kept_row
    need_row = jnp.where(need_first, 0, half)
    lead_row = jnp.where(kept_block % 2 == 0, 0, half)
    frame_rows = jnp.stack([need_row, sent_row, kept_row, lead_row, half - lead_row]).astype(jnp.int32)
    half_in = lax.dynamic_slice_in_dim(layer_input, sent_row, BLOCK, 0)
    middle = half_in.shape[1] // 2

    def tokens_of(which):
        return jnp.concatenate([group_of(queries, which, wide), group_of(out_grad, which, wide)], axis=1)

    own = tokens_of(c)
    got = swap_core(jnp.concatenate([tokens_of(1 - c), half_in[:, :middle], half_in[:, middle:]], axis=0))
    delta_got = swap_core(delta_rows(group_of(row_delta, 1 - c, GROUP)))
    delta = jnp.concatenate([delta_rows(group_of(row_delta, c, GROUP)), delta_got], axis=0)

    lists = work_lists(block_order, block_mask, z, yh, c, nz)
    dq, dkv = attention(lists, own, got, delta, [kv_parts[k] for k in range(nz)])

    spread = lax.all_to_all(dkv, ("z", "yh"), 0, 0, tiled=True)

    dq, late = lax.optimization_barrier((dq, [weights[k] for k in FAR]))
    for k, piece in zip(FAR, late, strict=True):
        weights[k] = piece
    far = jnp.concatenate(late, axis=0)
    x_far, y_far = shift_x(far, -1), shift_y(far, -1)
    corner_far = shift_x(y_far, -1)
    quarters = [(x & 1) * 2 + yl, (1 - (x & 1)) * 2 + yl, (x & 1) * 2 + 1 - yl, (1 - (x & 1)) * 2 + 1 - yl]
    where = jnp.stack([z] + quarters).astype(jnp.int32)
    part, kv_weight = query_part(
        where, dq, [weights[k] for k in ORDER] + [x_near, x_far, y_near, y_far, corner_near, corner_far]
    )
    keep, send = partial_sums(frame_rows, spread, kv_weight, part)
    token_grad, encoder_grad = finished(
        frame_rows,
        keep,
        swap_core(send),
        layer_input,
        got,
        norm_gain[None],
        vision_features[0],
        post_gain[None],
        projector,
    )
    return (token_grad, encoder_grad[None])


def solution(mesh):
    grid = Mesh(mesh.devices.reshape(8, 2, 2, 4, 2), ("z", "yh", "c", "x", "yl"))
    both = ("x", "yl", "z", "yh", "c")
    placed = (
        P(both, None),
        P(both, None),
        P(both, None),
        P(both, None),
        P(both, None),
        P(both, None),
        P(),
        P(("z", "yh", "c"), None),
        P(("x", "yl")),
        P(("x", "yl"), None),
        P(("x", "yl")),
        P(both, None, None),
        P(),
        P(),
    )
    return jax.shard_map(
        program,
        mesh=grid,
        in_specs=placed,
        out_specs=(P(both, None), P(both, None, None)),
        check_vma=False,
    )
```

```python
import jax
import jax.numpy as jnp
from jax import lax
from jax.experimental import pallas as pl
from jax.experimental.pallas import tpu as pltpu
from jax.sharding import Mesh, PartitionSpec as P

HQ = 14
KVH = 2
HD = 128
GROUP = HQ // KVH
EPSILON = 1e-06
NEGATIVE = -1e30
BLOCK = 64
LANES = GROUP * BLOCK
STEP = 4


def dot_nt(a, b):
    return lax.dot_general(a, b, (((1,), (1,)), ((), ())), preferred_element_type=jnp.float32)


def dot_nn(a, b):
    return lax.dot_general(a, b, (((1,), (0,)), ((), ())), preferred_element_type=jnp.float32)


def dot_tn(a, b):
    return lax.dot_general(a, b, (((0,), (0,)), ((), ())), preferred_element_type=jnp.float32)


def attention_kernel(pieces, *refs):
    slot_ref, kind_ref, query_ref, start_ref, turns_ref, place_ref, own_ref, got_ref, delta_ref = refs[:9]
    kv_parts = refs[9 : 9 + pieces]
    dq_ref, dkv_ref = refs[9 + pieces : 11 + pieces]
    qs, gs, kv, bias, acc, dqt, tops, sums, lses = refs[11 + pieces :]
    wide = GROUP * HD
    scaling = HD ** (-0.5)
    to_log2 = scaling * 1.4426950408889634
    height = kv_parts[0].shape[0]
    rows = height * pieces
    for i, part in enumerate(kv_parts):
        kv[i * height : (i + 1) * height, :] = part[...]
    for a in range(4):
        ref = own_ref if a < 2 else got_ref
        first = (a % 2) * BLOCK
        for h in range(GROUP):
            into, cols = slice(h * BLOCK, (h + 1) * BLOCK), h * HD
            qs[a, into, :] = ref[first : first + BLOCK, cols : cols + HD]
            gs[a, into, :] = ref[first : first + BLOCK, wide + cols : wide + cols + HD]
    key_row = lax.broadcasted_iota(jnp.int32, (BLOCK, LANES), 0)
    query_row = lax.broadcasted_iota(jnp.int32, (BLOCK, LANES), 1) % BLOCK
    bias[0] = jnp.zeros((BLOCK, LANES), jnp.float32)
    bias[1] = jnp.where(key_row <= query_row, 0.0, NEGATIVE)
    bias[2] = jnp.full((BLOCK, LANES), NEGATIVE, jnp.float32)
    acc[...] = jnp.zeros(acc.shape, jnp.float32)
    dqt[...] = jnp.zeros(dqt.shape, jnp.float32)
    tops[...] = jnp.full(tops.shape, NEGATIVE, jnp.float32)
    sums[...] = jnp.zeros(sums.shape, jnp.float32)

    def slots_of(item):
        first = start_ref[item]
        return [pl.multiple_of(slot_ref[first + i], BLOCK) for i in range(STEP)]

    def gathered(slots, first):
        return jnp.concatenate([kv[pl.ds(row, BLOCK), first : first + HD] for row in slots], axis=0)

    def scores(item, a, keys):
        first = start_ref[item]
        mask = jnp.concatenate([bias[kind_ref[first + i]] for i in range(STEP)], axis=0)
        return dot_nt(keys, qs[a]) * to_log2 + mask

    def total(turn, unused):
        for item in (2 * turn, 2 * turn + 1):
            a = query_ref[item]
            score = scores(item, a, gathered(slots_of(item), 0)).reshape(STEP * BLOCK // 8, 8, LANES)
            top = tops[a]
            top_next = jnp.maximum(top, jnp.max(score, axis=0))
            sums[a] = sums[a] * jnp.exp2(top - top_next) + jnp.sum(jnp.exp2(score - top_next), axis=0)
            tops[a] = top_next
        return unused

    lax.fori_loop(0, turns_ref[0], total, 0)
    for a in range(4):
        top = tops[a]
        peak = jnp.max(top, axis=0, keepdims=True)
        whole = jnp.sum(sums[a] * jnp.exp2(top - peak), axis=0, keepdims=True)
        lses[a] = peak + jnp.log2(whole)

    def grads(turn, unused):
        for item in (2 * turn, 2 * turn + 1):
            a = query_ref[item]
            slots = slots_of(item)
            keys = gathered(slots, 0)
            values = gathered(slots, HD)
            prob = jnp.exp2(scores(item, a, keys) - lses[a])
            prob_grad = dot_nt(values, gs[a])
            score_grad = (prob * (prob_grad - delta_ref[a])).astype(jnp.bfloat16)
            value_add = dot_nn(prob.astype(jnp.bfloat16), gs[a])
            key_add = dot_nn(score_grad, qs[a])
            dqt[a] += dot_tn(keys, score_grad)
            for i, row in enumerate(slots):
                acc[pl.ds(row, BLOCK), 0:HD] += key_add[i * BLOCK : (i + 1) * BLOCK, :]
                acc[pl.ds(row, BLOCK), HD : 2 * HD] += value_add[i * BLOCK : (i + 1) * BLOCK, :]
        return unused

    lax.fori_loop(0, turns_ref[0], grads, 0)
    for a in range(4):
        dq = (dqt[a].T * scaling).astype(jnp.bfloat16)
        for h in range(GROUP):
            dq_ref[a * BLOCK : (a + 1) * BLOCK, h * HD : (h + 1) * HD] = dq[h * BLOCK : (h + 1) * BLOCK, :]
    scale = jnp.where(lax.broadcasted_iota(jnp.int32, (1, 2 * HD), 1) < HD, scaling, 1.0)
    chip = 4 * BLOCK

    def write(i, unused):
        source = pl.ds(pl.multiple_of(i * chip, chip), chip)
        target = pl.ds(pl.multiple_of(place_ref[i], chip), chip)
        dkv_ref[target, :] = (acc[source, :] * scale).astype(jnp.bfloat16)
        return unused

    lax.fori_loop(0, rows // chip, write, 0)


SMEM = pl.BlockSpec(memory_space=pltpu.SMEM)
VMEM = pl.BlockSpec(memory_space=pltpu.VMEM)
ANY = pl.BlockSpec(memory_space=pl.ANY)


def attention(lists, own, got, delta, kv_parts):
    pieces = len(kv_parts)
    rows = pieces * kv_parts[0].shape[0]
    return pl.pallas_call(
        lambda *refs: attention_kernel(pieces, *refs),
        out_shape=(
            jax.ShapeDtypeStruct((4 * BLOCK, GROUP * HD), jnp.bfloat16),
            jax.ShapeDtypeStruct((rows, 2 * HD), jnp.bfloat16),
        ),
        in_specs=[SMEM] * 6 + [VMEM] * (3 + pieces),
        out_specs=(VMEM, VMEM),
        scratch_shapes=[
            pltpu.VMEM((4, LANES, HD), jnp.bfloat16),
            pltpu.VMEM((4, LANES, HD), jnp.bfloat16),
            pltpu.VMEM((rows, 2 * HD), jnp.bfloat16),
            pltpu.VMEM((3, BLOCK, LANES), jnp.float32),
            pltpu.VMEM((rows, 2 * HD), jnp.float32),
            pltpu.VMEM((4, HD, LANES), jnp.float32),
            pltpu.VMEM((4, 8, LANES), jnp.float32),
            pltpu.VMEM((4, 8, LANES), jnp.float32),
            pltpu.VMEM((4, 1, LANES), jnp.float32),
        ],
        compiler_params=pltpu.CompilerParams(vmem_limit_bytes=32 * 1024 * 1024),
        name="attention_grads",
    )(*lists, own, got, delta, *kv_parts)


def tables_kernel(
    where_ref, order_ref, mask_ref, owner_ref,
    slot_ref, kind_ref, query_ref, start_ref, turns_ref, place_ref, rows_ref, block_ref,
):
    z, yh, c = where_ref[0], where_ref[1], where_ref[2]
    count = block_ref.shape[0]
    nz = count // 8

    def chip_of(slot):
        return lax.rem(z + nz - (slot >> 3), nz) * 2 + (yh ^ ((slot >> 2) & 1))

    def block(slot, unused):
        core = c ^ ((slot >> 1) & 1)
        block_ref[slot] = order_ref[2 * (2 * chip_of(slot) + core) + (slot & 1)]
        return unused

    lax.fori_loop(0, count, block, 0)

    def place(chip, unused):
        place_ref[chip] = chip_of(4 * chip) * (4 * BLOCK)
        return unused

    lax.fori_loop(0, count // 4, place, 0)
    items = jnp.int32(0)
    for a in range(4):
        query = block_ref[a]

        def listed(slot, found, a=a, query=query):
            slot_ref[a * count + found] = slot * BLOCK
            kind_ref[a * count + found] = jnp.where(slot == a, 1, 0)
            return found + jnp.where(mask_ref[query, block_ref[slot]] > 0, 1, 0)

        found = lax.fori_loop(0, count, listed, jnp.int32(0))
        for i in range(STEP):
            slot_ref[a * count + found + i] = 0
            kind_ref[a * count + found + i] = 2
        turns = (found + STEP - 1) // STEP

        def item(i, unused, a=a, items=items):
            query_ref[items + i] = a
            start_ref[items + i] = a * count + STEP * i
            return unused

        lax.fori_loop(0, turns, item, 0)
        items = items + turns
    for i in range(STEP):
        slot_ref[4 * count + i] = 0
        kind_ref[4 * count + i] = 2
    query_ref[items] = 3
    start_ref[items] = 4 * count
    turns_ref[0] = (items + 1) >> 1
    me = (z * 2 + yh) * 2 + c

    def frame(f, mine):
        return jnp.where(owner_ref[f] == me, f, mine)

    mine = lax.fori_loop(0, owner_ref.shape[0], frame, jnp.int32(0))
    first, second = order_ref[2 * me], order_ref[2 * me + 1]
    keep_first = (first >> 1) == mine
    kept_row = jnp.where(keep_first, 0, BLOCK)
    lead_row = jnp.where((jnp.where(keep_first, first, second) & 1) == 0, 0, BLOCK)
    rows_ref[0] = jnp.where((order_ref[2 * (me ^ 1)] >> 1) == mine, 0, BLOCK)
    rows_ref[1] = BLOCK - kept_row
    rows_ref[2] = kept_row
    rows_ref[3] = lead_row
    rows_ref[4] = BLOCK - lead_row


def work_tables(where, block_order, block_mask, frame_owner):
    count = block_order.shape[0]
    sizes = [4 * count + STEP, 4 * count + STEP, count + 1, count + 1, 1, count // 4, 5]
    return pl.pallas_call(
        tables_kernel,
        out_shape=tuple(jax.ShapeDtypeStruct((size,), jnp.int32) for size in sizes),
        in_specs=[SMEM] * 4,
        out_specs=(SMEM,) * len(sizes),
        scratch_shapes=[pltpu.SMEM((count,), jnp.int32)],
        name="work_tables",
    )(where, block_order, block_mask, frame_owner)


def stack_kernel(*refs):
    pieces, (out_ref, sems) = refs[:-2], refs[-2:]
    rows = pieces[0].shape[0]
    copies = [
        pltpu.make_async_copy(piece, out_ref.at[pl.ds(i * rows, rows), :], sems.at[i])
        for i, piece in enumerate(pieces)
    ]
    for copy in copies:
        copy.start()
    for copy in copies:
        copy.wait()


def stacked(pieces):
    rows, width = pieces[0].shape
    return pl.pallas_call(
        stack_kernel,
        out_shape=jax.ShapeDtypeStruct((len(pieces) * rows, width), pieces[0].dtype),
        in_specs=[ANY] * len(pieces),
        out_specs=ANY,
        scratch_shapes=[pltpu.SemaphoreType.DMA((len(pieces),))],
        compiler_params=pltpu.CompilerParams(vmem_limit_bytes=1024 * 1024),
    )(*[in_hbm(piece) for piece in pieces])


def query_part_kernel(z_ref, dq_ref, *refs):
    pieces, (part_ref, kv_ref, weight, sems) = refs[:-4], refs[-4:]
    z = z_ref[0]
    rows = 112
    copies = []
    for kind, parts in enumerate(PLACES):
        ref = pieces[kind]
        for i, (quarter, back) in enumerate(parts):
            shard = lax.rem(z + 8 - back, 8) * 4 + z_ref[1 + quarter]
            copies.append(
                pltpu.make_async_copy(
                    ref.at[pl.ds(i * rows, rows), :],
                    weight.at[pl.ds(pl.multiple_of(shard * rows, 16), rows), :],
                    sems.at[len(copies)],
                )
            )
    for copy in copies:
        copy.start()
    for copy in copies:
        copy.wait()
    wide = dq_ref.shape[1]
    dq = dq_ref[...]
    step = 512

    def columns(i, unused):
        cols = pl.ds(pl.multiple_of(i * step, step), step)
        part_ref[:, cols] = dot_nt(dq, weight[cols, 0:wide])
        kv_ref[cols, :] = weight[cols, wide:]
        return unused

    lax.fori_loop(0, part_ref.shape[1] // step, columns, 0)


ORDER = (0, 1, 7, 2, 6, 3, 5, 4)
NEAR, FAR = ORDER[:5], ORDER[5:]
PLACES = tuple(
    [[(0, back)] for back in ORDER]
    + [[(kind, back) for back in side] for kind in (1, 2, 3) for side in (NEAR, FAR)]
)


def query_part(where, dq, pieces):
    total = 4 * 8 * 112
    wide = dq.shape[1]
    return pl.pallas_call(
        query_part_kernel,
        out_shape=(
            jax.ShapeDtypeStruct((dq.shape[0], total), jnp.float32),
            jax.ShapeDtypeStruct((total, 2 * HD), jnp.bfloat16),
        ),
        in_specs=[SMEM, VMEM] + [ANY] * len(pieces),
        out_specs=(VMEM, VMEM),
        scratch_shapes=[
            pltpu.VMEM((total, wide + 2 * HD), jnp.bfloat16),
            pltpu.SemaphoreType.DMA((sum(len(p) for p in PLACES),)),
        ],
        compiler_params=pltpu.CompilerParams(vmem_limit_bytes=24 * 1024 * 1024),
        name="query_part",
    )(where, dq, *[in_hbm(piece) for piece in pieces])


def partial_kernel(rows_ref, spread_ref, kv_ref, part_ref, keep_ref, send_ref, whole, dkv_ref):
    chip = dkv_ref.shape[0]
    tok = chip // 2
    height = 32

    def total(i, unused):
        first = pl.multiple_of(i * height, height)
        dkv_sum = jnp.zeros((height, dkv_ref.shape[1]), jnp.float32)
        for source in range(spread_ref.shape[0] // chip):
            dkv_sum += spread_ref[pl.ds(source * chip + first, height), :].astype(jnp.float32)
        dkv_ref[pl.ds(first, height), :] = dkv_sum.astype(jnp.bfloat16)
        return unused

    @pl.when(pl.program_id(0) == 0)
    def _():
        lax.fori_loop(0, chip // height, total, 0)

    whole[...] = part_ref[...] + dot_nt(dkv_ref[...], kv_ref[...])
    keep_ref[0:tok, :] = whole[0:tok, :].astype(jnp.bfloat16)
    send_ref[0:tok, :] = whole[tok:, :].astype(jnp.bfloat16)
    need = pl.ds(pl.multiple_of(tok + rows_ref[0], BLOCK), BLOCK)
    sent = pl.ds(pl.multiple_of(rows_ref[1], BLOCK), BLOCK)
    keep_ref[tok:, :] = whole[need, :].astype(jnp.bfloat16)
    send_ref[tok:, :] = whole[sent, :].astype(jnp.bfloat16)


def partial_sums(rows, spread, kv_weight, part):
    out = 2 * BLOCK + BLOCK
    step = 512
    height, width = part.shape
    return pl.pallas_call(
        partial_kernel,
        grid=(width // step,),
        out_shape=(
            jax.ShapeDtypeStruct((out, width), jnp.bfloat16),
            jax.ShapeDtypeStruct((out, width), jnp.bfloat16),
        ),
        in_specs=[
            SMEM,
            pl.BlockSpec(spread.shape, lambda i: (0, 0)),
            pl.BlockSpec((step, kv_weight.shape[1]), lambda i: (i, 0)),
            pl.BlockSpec((height, step), lambda i: (0, i)),
        ],
        out_specs=(pl.BlockSpec((out, step), lambda i: (0, i)), pl.BlockSpec((out, step), lambda i: (0, i))),
        scratch_shapes=[
            pltpu.VMEM((height, step), jnp.float32),
            pltpu.VMEM((height, spread.shape[1]), jnp.bfloat16),
        ],
        compiler_params=pltpu.CompilerParams(
            dimension_semantics=("arbitrary",), vmem_limit_bytes=24 * 1024 * 1024
        ),
        name="partial_sums",
    )(rows, spread, in_hbm(kv_weight), in_hbm(part))


def final_kernel(
    rows_ref, keep_ref, got_ref, in_own, swapped_ref, gain_ref, feature_ref, post_ref, projector_hbm,
    token_ref, encoder_ref, projector, frame, post, sem,
):
    load = pltpu.make_async_copy(projector_hbm, projector, sem)
    load.start()
    tok = in_own.shape[0]
    height = 16

    def token_rows(first, inputs):
        norm_grad = keep_ref[pl.ds(first, height), :].astype(jnp.float32) + got_ref[pl.ds(first, height), :].astype(jnp.float32)
        norm_grad = norm_grad.astype(jnp.bfloat16).astype(jnp.float32)
        inputs = inputs.astype(jnp.float32)
        inverse = lax.rsqrt(jnp.mean(inputs * inputs, axis=1, keepdims=True) + EPSILON)
        scaled = norm_grad * gain_ref[...]
        lean = inverse * inverse * inverse * jnp.mean(scaled * inputs, axis=1, keepdims=True)
        return (inverse * scaled - inputs * lean).astype(jnp.bfloat16)

    def own(i, unused):
        first = pl.multiple_of(i * height, height)
        token_ref[pl.ds(first, height), :] = token_rows(first, in_own[pl.ds(first, height), :])
        return unused

    def got(i, unused):
        first = pl.multiple_of(i * height, height)
        frame[pl.ds(pl.multiple_of(rows_ref[4] + first, height), height), :] = token_rows(
            tok + first,
            jnp.concatenate(
                [swapped_ref[pl.ds(tok + first, height), :], swapped_ref[pl.ds(tok + BLOCK + first, height), :]],
                axis=1,
            ),
        )
        return unused

    lax.fori_loop(0, tok // height, own, 0)
    lax.fori_loop(0, BLOCK // height, got, 0)
    frame[pl.ds(pl.multiple_of(rows_ref[3], BLOCK), BLOCK), :] = token_ref[
        pl.ds(pl.multiple_of(rows_ref[2], BLOCK), BLOCK), :
    ]
    features = feature_ref[...].astype(jnp.float32)
    centered = features - jnp.mean(features, axis=1, keepdims=True)
    deviation = lax.rsqrt(jnp.mean(centered * centered, axis=1, keepdims=True) + EPSILON)
    normed = centered * deviation
    load.wait()
    step = 384

    def columns(i, unused):
        cols = pl.ds(pl.multiple_of(i * step, 128), step)
        post[:, cols] = dot_nt(frame[...], projector[cols, :])
        return unused

    lax.fori_loop(0, post.shape[1] // step, columns, 0)
    weighted = post[...] * post_ref[...]
    encoder_ref[...] = (
        deviation
        * (
            weighted
            - jnp.mean(weighted, axis=1, keepdims=True)
            - normed * jnp.mean(weighted * normed, axis=1, keepdims=True)
        )
    ).astype(jnp.bfloat16)


def finished(rows, keep, got, in_own, in_got, gain, features, post_gain, projector):
    return pl.pallas_call(
        final_kernel,
        out_shape=(
            jax.ShapeDtypeStruct(in_own.shape, jnp.bfloat16),
            jax.ShapeDtypeStruct(features.shape, jnp.bfloat16),
        ),
        in_specs=[SMEM] + [VMEM] * 7 + [ANY],
        out_specs=(VMEM, VMEM),
        scratch_shapes=[
            pltpu.VMEM(projector.shape, jnp.bfloat16),
            pltpu.VMEM((2 * BLOCK, in_own.shape[1]), jnp.bfloat16),
            pltpu.VMEM((2 * BLOCK, projector.shape[0]), jnp.float32),
            pltpu.SemaphoreType.DMA,
        ],
        compiler_params=pltpu.CompilerParams(vmem_limit_bytes=32 * 1024 * 1024),
        name="finished",
    )(rows, keep, got, in_own, in_got, gain, features, post_gain, in_hbm(projector))


def swap_core(value):
    return lax.ppermute(value, "c", [(0, 1), (1, 0)])


def in_hbm(value):
    return pltpu.with_memory_space_constraint(value, pltpu.HBM)


def delta_rows(delta):
    return jnp.transpose(delta.reshape(2, BLOCK, GROUP), (0, 2, 1)).reshape(2, 1, LANES)


def program(
    queries,
    keys,
    values,
    out_grad,
    row_delta,
    layer_input,
    norm_gain,
    qkv_weight,
    block_order,
    block_mask,
    frame_owner,
    vision_features,
    post_gain,
    projector,
):
    nz, nx = lax.axis_size("z"), lax.axis_size("x")
    z, yh, c, x, yl = (lax.axis_index(name) for name in ("z", "yh", "c", "x", "yl"))
    wide = GROUP * HD

    def group_of(array, which, width):
        return lax.dynamic_slice_in_dim(array, which * width, width, 1)

    def kv_of(which):
        return jnp.concatenate([group_of(keys, which, HD), group_of(values, which, HD)], axis=1)

    def columns_of(which):
        return jnp.concatenate(
            [
                group_of(qkv_weight[:, : HQ * HD], which, wide),
                group_of(qkv_weight[:, HQ * HD :], which, HD),
                group_of(qkv_weight[:, HQ * HD :], KVH + which, HD),
            ],
            axis=1,
        )

    forward = [(i, (i + 1) % nz) for i in range(nz)]
    backward = [(i, (i - 1) % nz) for i in range(nz)]

    kv_chip = jnp.concatenate([kv_of(c), swap_core(kv_of(1 - c))], axis=0)
    kv_row = lax.ppermute(kv_chip, "yh", [(0, 1), (1, 0)])
    (qkv_weight, queries, out_grad, row_delta), _ = lax.optimization_barrier(
        ((qkv_weight, queries, out_grad, row_delta), kv_chip)
    )

    def index(yh_, c_, x_, yl_):
        return ((yh_ * 2 + c_) * nx + x_) * 2 + yl_

    mine, theirs = columns_of(c), columns_of(1 - c)
    pairs_a, pairs_b = [], []
    for x_ in range(nx):
        for yl_ in range(2):
            home = x_ & 1
            pairs_a.append((index(home, yl_, x_, yl_), index(home, 1 - yl_, x_, yl_)))
            source = index(home, yl_, x_, 1 - yl_)
            pairs_a.append((source, index(1 - home, yl_, x_, yl_)))
            pairs_b.append((source, index(1 - home, 1 - yl_, x_, yl_)))
    plane = ("yh", "c", "x", "yl")
    weight_a = lax.ppermute(jnp.where(c == yl, theirs, mine), plane, pairs_a)
    weight_b = lax.ppermute(theirs, plane, pairs_b)
    quarter = jnp.where(c == yl, jnp.where(yh == x & 1, mine, weight_a), jnp.where(yh == x & 1, weight_a, weight_b))

    kv_parts = {(0, 0): kv_chip, (0, 1): kv_row}
    ups, downs = [kv_chip, kv_row], [kv_chip, kv_row]
    weights = {0: quarter}
    weight_up = weight_down = quarter
    for k in range(1, nz // 2 + 1):
        for y in range(2):
            kv_parts[k, y] = ups[y] = lax.ppermute(ups[y], "z", forward)
            if k < nz // 2:
                kv_parts[nz - k, y] = downs[y] = lax.ppermute(downs[y], "z", backward)
        if k < 3:
            weights[k] = weight_up = lax.ppermute(weight_up, "z", forward)
            weights[nz - k] = weight_down = lax.ppermute(weight_down, "z", backward)
    weights[3] = lax.ppermute(weight_up, "z", forward)
    weights[nz - 3] = lax.ppermute(weight_down, "z", backward)
    weights[4] = lax.ppermute(weight_up, "z", [(i, (i + 2) % nz) for i in range(nz)])

    def shift_x(value, by):
        return lax.ppermute(value, "x", [(i, (i + by) % nx) for i in range(nx)])

    def shift_y(value, by):
        return lax.ppermute(value, ("yh", "yl"), [(i, (i + by) % 4) for i in range(4)])

    near = stacked([weights[k] for k in NEAR])
    x_near, y_near = shift_x(near, 1), shift_y(near, 1)
    corner_near = shift_x(y_near, 1)

    *lists, frame_rows = work_tables(
        jnp.stack([z, yh, c]).astype(jnp.int32), block_order, block_mask, frame_owner
    )
    half_in = lax.dynamic_slice_in_dim(layer_input, frame_rows[1], BLOCK, 0)
    middle = half_in.shape[1] // 2

    def tokens_of(which):
        return jnp.concatenate([group_of(queries, which, wide), group_of(out_grad, which, wide)], axis=1)

    own = tokens_of(c)
    got = swap_core(jnp.concatenate([tokens_of(1 - c), half_in[:, :middle], half_in[:, middle:]], axis=0))
    delta_got = swap_core(delta_rows(group_of(row_delta, 1 - c, GROUP)))
    delta = jnp.concatenate([delta_rows(group_of(row_delta, c, GROUP)), delta_got], axis=0)

    dq, dkv = attention(lists, own, got, delta, [kv_parts[k, y] for k in range(nz) for y in range(2)])

    spread = lax.all_to_all(dkv, ("z", "yh"), 0, 0, tiled=True)

    dq, late = lax.optimization_barrier((dq, [weights[k] for k in FAR]))
    for k, piece in zip(FAR, late, strict=True):
        weights[k] = piece
    far = stacked(late)
    x_far, y_far = shift_x(far, -1), shift_y(far, -1)
    corner_far = shift_x(y_far, -1)
    quarters = [(x & 1) * 2 + yl, (1 - (x & 1)) * 2 + yl, (x & 1) * 2 + 1 - yl, (1 - (x & 1)) * 2 + 1 - yl]
    where = jnp.stack([z] + quarters).astype(jnp.int32)
    part, kv_weight = query_part(
        where, dq, [weights[k] for k in ORDER] + [x_near, x_far, y_near, y_far, corner_near, corner_far]
    )
    keep, send = partial_sums(frame_rows, spread, kv_weight, part)
    token_grad, encoder_grad = finished(
        frame_rows,
        keep,
        swap_core(send),
        layer_input,
        got,
        norm_gain[None],
        vision_features[0],
        post_gain[None],
        projector,
    )
    return (token_grad, encoder_grad[None])


def solution(mesh):
    grid = Mesh(mesh.devices.reshape(8, 2, 2, 4, 2), ("z", "yh", "c", "x", "yl"))
    both = ("x", "yl", "z", "yh", "c")
    placed = (
        P(both, None),
        P(both, None),
        P(both, None),
        P(both, None),
        P(both, None),
        P(both, None),
        P(),
        P(("z", "yh", "c"), None),
        P(("x", "yl")),
        P(("x", "yl"), None),
        P(("x", "yl")),
        P(both, None, None),
        P(),
        P(),
    )
    return jax.shard_map(
        program,
        mesh=grid,
        in_specs=placed,
        out_specs=(P(both, None), P(both, None, None)),
        check_vma=False,
    )
```

```python
import jax
import jax.numpy as jnp
from jax import lax
from jax.experimental import pallas as pl
from jax.experimental.pallas import tpu as pltpu
from jax.sharding import Mesh, PartitionSpec as P

HQ = 14
KVH = 2
HD = 128
GROUP = HQ // KVH
EPSILON = 1e-06
NEGATIVE = -1e30
BLOCK = 64
LANES = GROUP * BLOCK
STEP = 4


def dot_nt(a, b):
    return lax.dot_general(a, b, (((1,), (1,)), ((), ())), preferred_element_type=jnp.float32)


def dot_nn(a, b):
    return lax.dot_general(a, b, (((1,), (0,)), ((), ())), preferred_element_type=jnp.float32)


def dot_tn(a, b):
    return lax.dot_general(a, b, (((0,), (0,)), ((), ())), preferred_element_type=jnp.float32)


def attention_kernel(pieces, *refs):
    slot_ref, kind_ref, query_ref, start_ref, turns_ref, place_ref, own_ref, got_ref, delta_ref = refs[:9]
    kv_parts = refs[9 : 9 + pieces]
    dq_ref, dkv_ref = refs[9 + pieces : 11 + pieces]
    qs, gs, kv, bias, acc, dqt, tops, sums, lses = refs[11 + pieces :]
    wide = GROUP * HD
    scaling = HD ** (-0.5)
    to_log2 = scaling * 1.4426950408889634
    height = kv_parts[0].shape[0]
    rows = height * pieces
    for i, part in enumerate(kv_parts):
        kv[i * height : (i + 1) * height, :] = part[...]
    for a in range(4):
        ref = own_ref if a < 2 else got_ref
        first = (a % 2) * BLOCK
        for h in range(GROUP):
            into, cols = slice(h * BLOCK, (h + 1) * BLOCK), h * HD
            qs[a, into, :] = ref[first : first + BLOCK, cols : cols + HD]
            gs[a, into, :] = ref[first : first + BLOCK, wide + cols : wide + cols + HD]
    key_row = lax.broadcasted_iota(jnp.int32, (BLOCK, LANES), 0)
    query_row = lax.broadcasted_iota(jnp.int32, (BLOCK, LANES), 1) % BLOCK
    bias[0] = jnp.zeros((BLOCK, LANES), jnp.float32)
    bias[1] = jnp.where(key_row <= query_row, 0.0, NEGATIVE)
    bias[2] = jnp.full((BLOCK, LANES), NEGATIVE, jnp.float32)
    acc[...] = jnp.zeros(acc.shape, jnp.float32)
    dqt[...] = jnp.zeros(dqt.shape, jnp.float32)
    tops[...] = jnp.full(tops.shape, NEGATIVE, jnp.float32)
    sums[...] = jnp.zeros(sums.shape, jnp.float32)

    def slots_of(item):
        first = start_ref[item]
        return [pl.multiple_of(slot_ref[first + i], BLOCK) for i in range(STEP)]

    def gathered(slots, first):
        return jnp.concatenate([kv[pl.ds(row, BLOCK), first : first + HD] for row in slots], axis=0)

    def scores(item, a, keys):
        first = start_ref[item]
        mask = jnp.concatenate([bias[kind_ref[first + i]] for i in range(STEP)], axis=0)
        return dot_nt(keys, qs[a]) * to_log2 + mask

    def total(turn, unused):
        for item in (2 * turn, 2 * turn + 1):
            a = query_ref[item]
            score = scores(item, a, gathered(slots_of(item), 0)).reshape(STEP * BLOCK // 8, 8, LANES)
            top = tops[a]
            top_next = jnp.maximum(top, jnp.max(score, axis=0))
            sums[a] = sums[a] * jnp.exp2(top - top_next) + jnp.sum(jnp.exp2(score - top_next), axis=0)
            tops[a] = top_next
        return unused

    lax.fori_loop(0, turns_ref[0], total, 0)
    for a in range(4):
        top = tops[a]
        peak = jnp.max(top, axis=0, keepdims=True)
        whole = jnp.sum(sums[a] * jnp.exp2(top - peak), axis=0, keepdims=True)
        lses[a] = peak + jnp.log2(whole)

    def grads(turn, unused):
        for item in (2 * turn, 2 * turn + 1):
            a = query_ref[item]
            slots = slots_of(item)
            keys = gathered(slots, 0)
            values = gathered(slots, HD)
            prob = jnp.exp2(scores(item, a, keys) - lses[a])
            prob_grad = dot_nt(values, gs[a])
            score_grad = (prob * (prob_grad - delta_ref[a])).astype(jnp.bfloat16)
            value_add = dot_nn(prob.astype(jnp.bfloat16), gs[a])
            key_add = dot_nn(score_grad, qs[a])
            dqt[a] += dot_tn(keys, score_grad)
            for i, row in enumerate(slots):
                acc[pl.ds(row, BLOCK), 0:HD] += key_add[i * BLOCK : (i + 1) * BLOCK, :]
                acc[pl.ds(row, BLOCK), HD : 2 * HD] += value_add[i * BLOCK : (i + 1) * BLOCK, :]
        return unused

    lax.fori_loop(0, turns_ref[0], grads, 0)
    for a in range(4):
        dq = (dqt[a].T * scaling).astype(jnp.bfloat16)
        for h in range(GROUP):
            dq_ref[a * BLOCK : (a + 1) * BLOCK, h * HD : (h + 1) * HD] = dq[h * BLOCK : (h + 1) * BLOCK, :]
    scale = jnp.where(lax.broadcasted_iota(jnp.int32, (1, 2 * HD), 1) < HD, scaling, 1.0)
    chip = 4 * BLOCK

    def write(i, unused):
        source = pl.ds(pl.multiple_of(i * chip, chip), chip)
        target = pl.ds(pl.multiple_of(place_ref[i], chip), chip)
        dkv_ref[target, :] = (acc[source, :] * scale).astype(jnp.bfloat16)
        return unused

    lax.fori_loop(0, rows // chip, write, 0)


SMEM = pl.BlockSpec(memory_space=pltpu.SMEM)
VMEM = pl.BlockSpec(memory_space=pltpu.VMEM)
ANY = pl.BlockSpec(memory_space=pl.ANY)


def attention(lists, own, got, delta, kv_parts):
    pieces = len(kv_parts)
    rows = pieces * kv_parts[0].shape[0]
    return pl.pallas_call(
        lambda *refs: attention_kernel(pieces, *refs),
        out_shape=(
            jax.ShapeDtypeStruct((4 * BLOCK, GROUP * HD), jnp.bfloat16),
            jax.ShapeDtypeStruct((rows, 2 * HD), jnp.bfloat16),
        ),
        in_specs=[SMEM] * 6 + [VMEM] * (3 + pieces),
        out_specs=(VMEM, VMEM),
        scratch_shapes=[
            pltpu.VMEM((4, LANES, HD), jnp.bfloat16),
            pltpu.VMEM((4, LANES, HD), jnp.bfloat16),
            pltpu.VMEM((rows, 2 * HD), jnp.bfloat16),
            pltpu.VMEM((3, BLOCK, LANES), jnp.float32),
            pltpu.VMEM((rows, 2 * HD), jnp.float32),
            pltpu.VMEM((4, HD, LANES), jnp.float32),
            pltpu.VMEM((4, 8, LANES), jnp.float32),
            pltpu.VMEM((4, 8, LANES), jnp.float32),
            pltpu.VMEM((4, 1, LANES), jnp.float32),
        ],
        compiler_params=pltpu.CompilerParams(vmem_limit_bytes=32 * 1024 * 1024),
        name="attention_grads",
    )(*lists, own, got, delta, *kv_parts)


def tables_kernel(
    where_ref, order_ref, mask_ref, owner_ref,
    slot_ref, kind_ref, query_ref, start_ref, turns_ref, place_ref, rows_ref, block_ref,
):
    z, yh, c = where_ref[0], where_ref[1], where_ref[2]
    count = block_ref.shape[0]
    nz = count // 8

    def chip_of(slot):
        return lax.rem(z + nz - (slot >> 3), nz) * 2 + (yh ^ ((slot >> 2) & 1))

    def block(slot, unused):
        core = c ^ ((slot >> 1) & 1)
        block_ref[slot] = order_ref[2 * (2 * chip_of(slot) + core) + (slot & 1)]
        return unused

    lax.fori_loop(0, count, block, 0)

    def place(chip, unused):
        place_ref[chip] = chip_of(4 * chip) * (4 * BLOCK)
        return unused

    lax.fori_loop(0, count // 4, place, 0)
    stride = count + STEP
    queries = [block_ref[a] for a in range(4)]

    def listed(slot, found):
        block = block_ref[slot]
        after = []
        for a in range(4):
            place = a * stride + found[a]
            slot_ref[place] = slot * BLOCK
            kind_ref[place] = jnp.where(slot == a, 1, 0)
            after.append(found[a] + jnp.where(mask_ref[queries[a], block] > 0, 1, 0))
        return tuple(after)

    found = lax.fori_loop(0, count, listed, (jnp.int32(0),) * 4)
    items = jnp.int32(0)
    for a in range(4):
        for i in range(STEP):
            slot_ref[a * stride + found[a] + i] = 0
            kind_ref[a * stride + found[a] + i] = 2
        turns = (found[a] + STEP - 1) // STEP

        def item(i, unused, a=a, items=items):
            query_ref[items + i] = a
            start_ref[items + i] = a * stride + STEP * i
            return unused

        lax.fori_loop(0, turns, item, 0)
        items = items + turns
    for i in range(STEP):
        slot_ref[4 * stride + i] = 0
        kind_ref[4 * stride + i] = 2
    query_ref[items] = 3
    start_ref[items] = 4 * stride
    turns_ref[0] = (items + 1) >> 1
    me = (z * 2 + yh) * 2 + c

    def frame(f, mine):
        return jnp.where(owner_ref[f] == me, f, mine)

    mine = lax.fori_loop(0, owner_ref.shape[0], frame, jnp.int32(0))
    first, second = order_ref[2 * me], order_ref[2 * me + 1]
    keep_first = (first >> 1) == mine
    kept_row = jnp.where(keep_first, 0, BLOCK)
    lead_row = jnp.where((jnp.where(keep_first, first, second) & 1) == 0, 0, BLOCK)
    rows_ref[0] = jnp.where((order_ref[2 * (me ^ 1)] >> 1) == mine, 0, BLOCK)
    rows_ref[1] = BLOCK - kept_row
    rows_ref[2] = kept_row
    rows_ref[3] = lead_row
    rows_ref[4] = BLOCK - lead_row


def work_tables(where, block_order, block_mask, frame_owner):
    count = block_order.shape[0]
    sizes = [4 * count + 5 * STEP, 4 * count + 5 * STEP, count + 1, count + 1, 1, count // 4, 5]
    return pl.pallas_call(
        tables_kernel,
        out_shape=tuple(jax.ShapeDtypeStruct((size,), jnp.int32) for size in sizes),
        in_specs=[SMEM] * 4,
        out_specs=(SMEM,) * len(sizes),
        scratch_shapes=[pltpu.SMEM((count,), jnp.int32)],
        name="work_tables",
    )(where, block_order, block_mask, frame_owner)


def stack_kernel(*refs):
    pieces, out_ref = refs[:-1], refs[-1]
    rows = pieces[0].shape[0]
    for i, piece in enumerate(pieces):
        out_ref[i * rows : (i + 1) * rows, :] = piece[...]


def stacked(pieces):
    rows, width = pieces[0].shape
    return pl.pallas_call(
        stack_kernel,
        out_shape=jax.ShapeDtypeStruct((len(pieces) * rows, width), pieces[0].dtype),
        in_specs=[VMEM] * len(pieces),
        out_specs=VMEM,
        compiler_params=pltpu.CompilerParams(vmem_limit_bytes=8 * 1024 * 1024),
    )(*pieces)


def query_part_kernel(z_ref, dq_ref, *refs):
    pieces, (part_ref, kv_ref, weight, sems) = refs[:-4], refs[-4:]
    z = z_ref[0]
    rows = 112
    copies = []
    for kind, parts in enumerate(PLACES):
        ref = pieces[kind]
        for i, (quarter, back) in enumerate(parts):
            shard = lax.rem(z + 8 - back, 8) * 4 + z_ref[1 + quarter]
            copies.append(
                pltpu.make_async_copy(
                    ref.at[pl.ds(i * rows, rows), :],
                    weight.at[pl.ds(pl.multiple_of(shard * rows, 16), rows), :],
                    sems.at[len(copies)],
                )
            )
    for copy in copies:
        copy.start()
    for copy in copies:
        copy.wait()
    wide = dq_ref.shape[1]
    dq = dq_ref[...]
    step = 512

    def columns(i, unused):
        cols = pl.ds(pl.multiple_of(i * step, step), step)
        part_ref[:, cols] = dot_nt(dq, weight[cols, 0:wide])
        kv_ref[cols, :] = weight[cols, wide:]
        return unused

    lax.fori_loop(0, part_ref.shape[1] // step, columns, 0)


ORDER = (0, 1, 7, 2, 6, 3, 5, 4)
NEAR, FAR = ORDER[:5], ORDER[5:]
PLACES = tuple(
    [[(0, back)] for back in ORDER]
    + [[(kind, back) for back in side] for kind in (1, 2, 3) for side in (NEAR, FAR)]
)


def query_part(where, dq, pieces):
    total = 4 * 8 * 112
    wide = dq.shape[1]
    return pl.pallas_call(
        query_part_kernel,
        out_shape=(
            jax.ShapeDtypeStruct((dq.shape[0], total), jnp.float32),
            jax.ShapeDtypeStruct((total, 2 * HD), jnp.bfloat16),
        ),
        in_specs=[SMEM, VMEM] + [ANY] * len(pieces),
        out_specs=(VMEM, VMEM),
        scratch_shapes=[
            pltpu.VMEM((total, wide + 2 * HD), jnp.bfloat16),
            pltpu.SemaphoreType.DMA((sum(len(p) for p in PLACES),)),
        ],
        compiler_params=pltpu.CompilerParams(vmem_limit_bytes=24 * 1024 * 1024),
        name="query_part",
    )(where, dq, *[in_hbm(piece) for piece in pieces])


def partial_kernel(rows_ref, spread_ref, kv_ref, part_ref, keep_ref, send_ref, whole, dkv_ref):
    chip = dkv_ref.shape[0]
    tok = chip // 2
    step = 512
    height = 32

    def total(i, unused):
        first = pl.multiple_of(i * height, height)
        dkv_sum = jnp.zeros((height, dkv_ref.shape[1]), jnp.float32)
        for source in range(spread_ref.shape[0] // chip):
            dkv_sum += spread_ref[pl.ds(source * chip + first, height), :].astype(jnp.float32)
        dkv_ref[pl.ds(first, height), :] = dkv_sum.astype(jnp.bfloat16)
        return unused

    lax.fori_loop(0, chip // height, total, 0)
    dkv = dkv_ref[...]

    def columns(i, unused):
        cols = pl.ds(pl.multiple_of(i * step, step), step)
        whole[...] = part_ref[:, cols] + dot_nt(dkv, kv_ref[cols, :])
        keep_ref[0:tok, cols] = whole[0:tok, :].astype(jnp.bfloat16)
        send_ref[0:tok, cols] = whole[tok:, :].astype(jnp.bfloat16)
        need = pl.ds(pl.multiple_of(tok + rows_ref[0], BLOCK), BLOCK)
        sent = pl.ds(pl.multiple_of(rows_ref[1], BLOCK), BLOCK)
        keep_ref[tok:, cols] = whole[need, :].astype(jnp.bfloat16)
        send_ref[tok:, cols] = whole[sent, :].astype(jnp.bfloat16)
        return unused

    lax.fori_loop(0, part_ref.shape[1] // step, columns, 0)


def partial_sums(rows, spread, kv_weight, part):
    out = 2 * BLOCK + BLOCK
    return pl.pallas_call(
        partial_kernel,
        out_shape=(
            jax.ShapeDtypeStruct((out, part.shape[1]), jnp.bfloat16),
            jax.ShapeDtypeStruct((out, part.shape[1]), jnp.bfloat16),
        ),
        in_specs=[SMEM, VMEM, VMEM, VMEM],
        out_specs=(VMEM, VMEM),
        scratch_shapes=[
            pltpu.VMEM((part.shape[0], 512), jnp.float32),
            pltpu.VMEM((part.shape[0], spread.shape[1]), jnp.bfloat16),
        ],
        compiler_params=pltpu.CompilerParams(vmem_limit_bytes=24 * 1024 * 1024),
        name="partial_sums",
    )(rows, spread, in_hbm(kv_weight), in_hbm(part))


def final_kernel(
    rows_ref, keep_ref, got_ref, in_own, swapped_ref, gain_ref, feature_ref, post_ref, projector_hbm,
    token_ref, encoder_ref, projector, frame, post, sem,
):
    load = pltpu.make_async_copy(projector_hbm, projector, sem)
    load.start()
    tok = in_own.shape[0]
    height = 16

    def token_rows(first, inputs):
        norm_grad = keep_ref[pl.ds(first, height), :].astype(jnp.float32) + got_ref[pl.ds(first, height), :].astype(jnp.float32)
        norm_grad = norm_grad.astype(jnp.bfloat16).astype(jnp.float32)
        inputs = inputs.astype(jnp.float32)
        inverse = lax.rsqrt(jnp.mean(inputs * inputs, axis=1, keepdims=True) + EPSILON)
        scaled = norm_grad * gain_ref[...]
        lean = inverse * inverse * inverse * jnp.mean(scaled * inputs, axis=1, keepdims=True)
        return (inverse * scaled - inputs * lean).astype(jnp.bfloat16)

    def own(i, unused):
        first = pl.multiple_of(i * height, height)
        token_ref[pl.ds(first, height), :] = token_rows(first, in_own[pl.ds(first, height), :])
        return unused

    def got(i, unused):
        first = pl.multiple_of(i * height, height)
        frame[pl.ds(pl.multiple_of(rows_ref[4] + first, height), height), :] = token_rows(
            tok + first,
            jnp.concatenate(
                [swapped_ref[pl.ds(tok + first, height), :], swapped_ref[pl.ds(tok + BLOCK + first, height), :]],
                axis=1,
            ),
        )
        return unused

    lax.fori_loop(0, tok // height, own, 0)
    lax.fori_loop(0, BLOCK // height, got, 0)
    frame[pl.ds(pl.multiple_of(rows_ref[3], BLOCK), BLOCK), :] = token_ref[
        pl.ds(pl.multiple_of(rows_ref[2], BLOCK), BLOCK), :
    ]
    features = feature_ref[...].astype(jnp.float32)
    centered = features - jnp.mean(features, axis=1, keepdims=True)
    deviation = lax.rsqrt(jnp.mean(centered * centered, axis=1, keepdims=True) + EPSILON)
    normed = centered * deviation
    load.wait()
    step = 384

    def columns(i, unused):
        cols = pl.ds(pl.multiple_of(i * step, 128), step)
        post[:, cols] = dot_nt(frame[...], projector[cols, :])
        return unused

    lax.fori_loop(0, post.shape[1] // step, columns, 0)
    weighted = post[...] * post_ref[...]
    encoder_ref[...] = (
        deviation
        * (
            weighted
            - jnp.mean(weighted, axis=1, keepdims=True)
            - normed * jnp.mean(weighted * normed, axis=1, keepdims=True)
        )
    ).astype(jnp.bfloat16)


def finished(rows, keep, got, in_own, in_got, gain, features, post_gain, projector):
    return pl.pallas_call(
        final_kernel,
        out_shape=(
            jax.ShapeDtypeStruct(in_own.shape, jnp.bfloat16),
            jax.ShapeDtypeStruct(features.shape, jnp.bfloat16),
        ),
        in_specs=[SMEM] + [VMEM] * 7 + [ANY],
        out_specs=(VMEM, VMEM),
        scratch_shapes=[
            pltpu.VMEM(projector.shape, jnp.bfloat16),
            pltpu.VMEM((2 * BLOCK, in_own.shape[1]), jnp.bfloat16),
            pltpu.VMEM((2 * BLOCK, projector.shape[0]), jnp.float32),
            pltpu.SemaphoreType.DMA,
        ],
        compiler_params=pltpu.CompilerParams(vmem_limit_bytes=32 * 1024 * 1024),
        name="finished",
    )(rows, keep, got, in_own, in_got, gain, features, post_gain, in_hbm(projector))


def swap_core(value):
    return lax.ppermute(value, "c", [(0, 1), (1, 0)])


def in_hbm(value):
    return pltpu.with_memory_space_constraint(value, pltpu.HBM)


def delta_rows(delta):
    return jnp.transpose(delta.reshape(2, BLOCK, GROUP), (0, 2, 1)).reshape(2, 1, LANES)


def program(
    queries,
    keys,
    values,
    out_grad,
    row_delta,
    layer_input,
    norm_gain,
    qkv_weight,
    block_order,
    block_mask,
    frame_owner,
    vision_features,
    post_gain,
    projector,
):
    nz, nx = lax.axis_size("z"), lax.axis_size("x")
    z, yh, c, x, yl = (lax.axis_index(name) for name in ("z", "yh", "c", "x", "yl"))
    wide = GROUP * HD

    def group_of(array, which, width):
        return lax.dynamic_slice_in_dim(array, which * width, width, 1)

    def kv_of(which):
        return jnp.concatenate([group_of(keys, which, HD), group_of(values, which, HD)], axis=1)

    def columns_of(which):
        return jnp.concatenate(
            [
                group_of(qkv_weight[:, : HQ * HD], which, wide),
                group_of(qkv_weight[:, HQ * HD :], which, HD),
                group_of(qkv_weight[:, HQ * HD :], KVH + which, HD),
            ],
            axis=1,
        )

    forward = [(i, (i + 1) % nz) for i in range(nz)]
    backward = [(i, (i - 1) % nz) for i in range(nz)]

    kv_chip = jnp.concatenate([kv_of(c), swap_core(kv_of(1 - c))], axis=0)
    kv_row = lax.ppermute(kv_chip, "yh", [(0, 1), (1, 0)])
    (qkv_weight, queries, out_grad, row_delta), _ = lax.optimization_barrier(
        ((qkv_weight, queries, out_grad, row_delta), kv_chip)
    )
    kv_pair = jnp.concatenate([kv_chip, kv_row], axis=0)

    def index(yh_, c_, x_, yl_):
        return ((yh_ * 2 + c_) * nx + x_) * 2 + yl_

    mine, theirs = columns_of(c), columns_of(1 - c)
    pairs_a, pairs_b = [], []
    for x_ in range(nx):
        for yl_ in range(2):
            home = x_ & 1
            pairs_a.append((index(home, yl_, x_, yl_), index(home, 1 - yl_, x_, yl_)))
            source = index(home, yl_, x_, 1 - yl_)
            pairs_a.append((source, index(1 - home, yl_, x_, yl_)))
            pairs_b.append((source, index(1 - home, 1 - yl_, x_, yl_)))
    plane = ("yh", "c", "x", "yl")
    weight_a = lax.ppermute(jnp.where(c == yl, theirs, mine), plane, pairs_a)
    weight_b = lax.ppermute(theirs, plane, pairs_b)
    quarter = jnp.where(c == yl, jnp.where(yh == x & 1, mine, weight_a), jnp.where(yh == x & 1, weight_a, weight_b))

    kv_parts = {0: kv_pair}
    weights = {0: quarter}
    kv_up = kv_down = kv_pair
    weight_up = weight_down = quarter
    for k in range(1, nz // 2 + 1):
        kv_parts[k] = kv_up = lax.ppermute(kv_up, "z", forward)
        if k < nz // 2:
            kv_parts[nz - k] = kv_down = lax.ppermute(kv_down, "z", backward)
        if k < 3:
            weights[k] = weight_up = lax.ppermute(weight_up, "z", forward)
            weights[nz - k] = weight_down = lax.ppermute(weight_down, "z", backward)
    weights[3] = lax.ppermute(weight_up, "z", forward)
    weights[nz - 3] = lax.ppermute(weight_down, "z", backward)
    weights[4] = lax.ppermute(weight_up, "z", [(i, (i + 2) % nz) for i in range(nz)])

    def shift_x(value, by):
        return lax.ppermute(value, "x", [(i, (i + by) % nx) for i in range(nx)])

    def shift_y(value, by):
        return lax.ppermute(value, ("yh", "yl"), [(i, (i + by) % 4) for i in range(4)])

    near = stacked([weights[k] for k in NEAR])
    x_near, y_near = shift_x(near, 1), shift_y(near, 1)
    corner_near = shift_x(y_near, 1)

    *lists, frame_rows = work_tables(
        jnp.stack([z, yh, c]).astype(jnp.int32), block_order, block_mask, frame_owner
    )
    half_in = lax.dynamic_slice_in_dim(layer_input, frame_rows[1], BLOCK, 0)
    middle = half_in.shape[1] // 2

    def tokens_of(which):
        return jnp.concatenate([group_of(queries, which, wide), group_of(out_grad, which, wide)], axis=1)

    own = tokens_of(c)
    got = swap_core(
        jnp.concatenate([tokens_of(1 - c), half_in[:, :middle], half_in[:, middle:]], axis=0),
    )
    delta_got = swap_core(delta_rows(group_of(row_delta, 1 - c, GROUP)))
    delta = jnp.concatenate([delta_rows(group_of(row_delta, c, GROUP)), delta_got], axis=0)

    dq, dkv = attention(lists, own, got, delta, [kv_parts[k] for k in range(nz)])

    spread = lax.all_to_all(dkv, ("z", "yh"), 0, 0, tiled=True)

    dq, late = lax.optimization_barrier((dq, [weights[k] for k in FAR]))
    for k, piece in zip(FAR, late, strict=True):
        weights[k] = piece
    far = stacked(late)
    x_far, y_far = shift_x(far, -1), shift_y(far, -1)
    corner_far = shift_x(y_far, -1)
    quarters = [(x & 1) * 2 + yl, (1 - (x & 1)) * 2 + yl, (x & 1) * 2 + 1 - yl, (1 - (x & 1)) * 2 + 1 - yl]
    where = jnp.stack([z] + quarters).astype(jnp.int32)
    part, kv_weight = query_part(
        where, dq, [weights[k] for k in ORDER] + [x_near, x_far, y_near, y_far, corner_near, corner_far]
    )
    keep, send = partial_sums(frame_rows, spread, kv_weight, part)
    token_grad, encoder_grad = finished(
        frame_rows,
        keep,
        swap_core(send),
        layer_input,
        got,
        norm_gain[None],
        vision_features[0],
        post_gain[None],
        projector,
    )
    return (token_grad, encoder_grad[None])


def solution(mesh):
    grid = Mesh(mesh.devices.reshape(8, 2, 2, 4, 2), ("z", "yh", "c", "x", "yl"))
    both = ("x", "yl", "z", "yh", "c")
    placed = (
        P(both, None),
        P(both, None),
        P(both, None),
        P(both, None),
        P(both, None),
        P(both, None),
        P(),
        P(("z", "yh", "c"), None),
        P(("x", "yl")),
        P(("x", "yl"), None),
        P(("x", "yl")),
        P(both, None, None),
        P(),
        P(),
    )
    return jax.shard_map(
        program,
        mesh=grid,
        in_specs=placed,
        out_specs=(P(both, None), P(both, None, None)),
        check_vma=False,
    )
```

```python
import jax
import jax.numpy as jnp
from jax import lax
from jax.experimental import pallas as pl
from jax.experimental.pallas import tpu as pltpu
from jax.sharding import Mesh, PartitionSpec as P

HQ = 14
KVH = 2
HD = 128
GROUP = HQ // KVH
EPSILON = 1e-06
NEGATIVE = -1e30
BLOCK = 64
LANES = GROUP * BLOCK
STEP = 4


def dot_nt(a, b):
    return lax.dot_general(a, b, (((1,), (1,)), ((), ())), preferred_element_type=jnp.float32)


def dot_nn(a, b):
    return lax.dot_general(a, b, (((1,), (0,)), ((), ())), preferred_element_type=jnp.float32)


def dot_tn(a, b):
    return lax.dot_general(a, b, (((0,), (0,)), ((), ())), preferred_element_type=jnp.float32)


def attention_kernel(pieces, *refs):
    slot_ref, kind_ref, query_ref, start_ref, turns_ref, place_ref, where_ref = refs[:7]
    q_own, q_got, g_own, g_got, delta_ref = refs[7:12]
    kv_parts = refs[12 : 12 + pieces]
    dq_ref, dkv_ref = refs[12 + pieces : 14 + pieces]
    qs, gs, kv, bias, acc, dqt, tops, sums, lses = refs[14 + pieces :]
    wide = GROUP * HD
    scaling = HD ** (-0.5)
    to_log2 = scaling * 1.4426950408889634
    height = kv_parts[0].shape[0]
    rows = height * pieces
    for i, part in enumerate(kv_parts):
        kv[i * height : (i + 1) * height, :] = part[...]
    for a in range(4):
        q_ref, g_ref = (q_own, g_own) if a < 2 else (q_got, g_got)
        first = (a % 2) * BLOCK
        for h in range(GROUP):
            into = slice(h * BLOCK, (h + 1) * BLOCK)
            cols = pl.ds(pl.multiple_of(where_ref[2] * wide + h * HD, HD), HD)
            qs[a, into, :] = q_ref[first : first + BLOCK, cols]
            gs[a, into, :] = g_ref[first : first + BLOCK, cols]
    key_row = lax.broadcasted_iota(jnp.int32, (BLOCK, LANES), 0)
    query_row = lax.broadcasted_iota(jnp.int32, (BLOCK, LANES), 1) % BLOCK
    bias[0] = jnp.zeros((BLOCK, LANES), jnp.float32)
    bias[1] = jnp.where(key_row <= query_row, 0.0, NEGATIVE)
    bias[2] = jnp.full((BLOCK, LANES), NEGATIVE, jnp.float32)
    acc[...] = jnp.zeros(acc.shape, jnp.float32)
    dqt[...] = jnp.zeros(dqt.shape, jnp.float32)
    tops[...] = jnp.full(tops.shape, NEGATIVE, jnp.float32)
    sums[...] = jnp.zeros(sums.shape, jnp.float32)

    def slots_of(item):
        first = start_ref[item]
        return [pl.multiple_of(slot_ref[first + i], BLOCK) for i in range(STEP)]

    def gathered(slots, first):
        return jnp.concatenate([kv[pl.ds(row, BLOCK), first : first + HD] for row in slots], axis=0)

    def scores(item, a, keys):
        first = start_ref[item]
        mask = jnp.concatenate([bias[kind_ref[first + i]] for i in range(STEP)], axis=0)
        return dot_nt(keys, qs[a]) * to_log2 + mask

    def total(turn, unused):
        for item in (2 * turn, 2 * turn + 1):
            a = query_ref[item]
            score = scores(item, a, gathered(slots_of(item), 0)).reshape(STEP * BLOCK // 8, 8, LANES)
            top = tops[a]
            top_next = jnp.maximum(top, jnp.max(score, axis=0))
            sums[a] = sums[a] * jnp.exp2(top - top_next) + jnp.sum(jnp.exp2(score - top_next), axis=0)
            tops[a] = top_next
        return unused

    lax.fori_loop(0, turns_ref[0], total, 0)
    for a in range(4):
        top = tops[a]
        peak = jnp.max(top, axis=0, keepdims=True)
        whole = jnp.sum(sums[a] * jnp.exp2(top - peak), axis=0, keepdims=True)
        lses[a] = peak + jnp.log2(whole)

    def grads(turn, unused):
        for item in (2 * turn, 2 * turn + 1):
            a = query_ref[item]
            slots = slots_of(item)
            keys = gathered(slots, 0)
            values = gathered(slots, HD)
            prob = jnp.exp2(scores(item, a, keys) - lses[a])
            prob_grad = dot_nt(values, gs[a])
            score_grad = (prob * (prob_grad - delta_ref[a])).astype(jnp.bfloat16)
            value_add = dot_nn(prob.astype(jnp.bfloat16), gs[a])
            key_add = dot_nn(score_grad, qs[a])
            dqt[a] += dot_tn(keys, score_grad)
            for i, row in enumerate(slots):
                acc[pl.ds(row, BLOCK), 0:HD] += key_add[i * BLOCK : (i + 1) * BLOCK, :]
                acc[pl.ds(row, BLOCK), HD : 2 * HD] += value_add[i * BLOCK : (i + 1) * BLOCK, :]
        return unused

    lax.fori_loop(0, turns_ref[0], grads, 0)
    for a in range(4):
        dq = (dqt[a].T * scaling).astype(jnp.bfloat16)
        for h in range(GROUP):
            dq_ref[a * BLOCK : (a + 1) * BLOCK, h * HD : (h + 1) * HD] = dq[h * BLOCK : (h + 1) * BLOCK, :]
    scale = jnp.where(lax.broadcasted_iota(jnp.int32, (1, 2 * HD), 1) < HD, scaling, 1.0)
    chip = 4 * BLOCK

    def write(i, unused):
        source = pl.ds(pl.multiple_of(i * chip, chip), chip)
        target = pl.ds(pl.multiple_of(place_ref[i], chip), chip)
        dkv_ref[target, :] = (acc[source, :] * scale).astype(jnp.bfloat16)
        return unused

    lax.fori_loop(0, rows // chip, write, 0)


SMEM = pl.BlockSpec(memory_space=pltpu.SMEM)
VMEM = pl.BlockSpec(memory_space=pltpu.VMEM)
ANY = pl.BlockSpec(memory_space=pl.ANY)


def attention(lists, where, tokens, delta, kv_parts):
    pieces = len(kv_parts)
    rows = pieces * kv_parts[0].shape[0]
    return pl.pallas_call(
        lambda *refs: attention_kernel(pieces, *refs),
        out_shape=(
            jax.ShapeDtypeStruct((4 * BLOCK, GROUP * HD), jnp.bfloat16),
            jax.ShapeDtypeStruct((rows, 2 * HD), jnp.bfloat16),
        ),
        in_specs=[SMEM] * 7 + [VMEM] * (5 + pieces),
        out_specs=(VMEM, VMEM),
        scratch_shapes=[
            pltpu.VMEM((4, LANES, HD), jnp.bfloat16),
            pltpu.VMEM((4, LANES, HD), jnp.bfloat16),
            pltpu.VMEM((rows, 2 * HD), jnp.bfloat16),
            pltpu.VMEM((3, BLOCK, LANES), jnp.float32),
            pltpu.VMEM((rows, 2 * HD), jnp.float32),
            pltpu.VMEM((4, HD, LANES), jnp.float32),
            pltpu.VMEM((4, 8, LANES), jnp.float32),
            pltpu.VMEM((4, 8, LANES), jnp.float32),
            pltpu.VMEM((4, 1, LANES), jnp.float32),
        ],
        compiler_params=pltpu.CompilerParams(vmem_limit_bytes=32 * 1024 * 1024),
        name="attention_grads",
    )(*lists, where, *tokens, delta, *[in_hbm(part) for part in kv_parts])


def tables_kernel(
    where_ref, order_ref, mask_ref, owner_ref,
    slot_ref, kind_ref, query_ref, start_ref, turns_ref, place_ref, rows_ref, block_ref,
):
    z, yh, c = where_ref[0], where_ref[1], where_ref[2]
    count = block_ref.shape[0]
    nz = count // 8

    def chip_of(slot):
        return lax.rem(z + nz - (slot >> 3), nz) * 2 + (yh ^ ((slot >> 2) & 1))

    def block(slot, unused):
        core = c ^ ((slot >> 1) & 1)
        block_ref[slot] = order_ref[2 * (2 * chip_of(slot) + core) + (slot & 1)]
        return unused

    lax.fori_loop(0, count, block, 0)

    def place(chip, unused):
        place_ref[chip] = chip_of(4 * chip) * (4 * BLOCK)
        return unused

    lax.fori_loop(0, count // 4, place, 0)
    stride = count + STEP
    queries = [block_ref[a] for a in range(4)]

    def listed(slot, found):
        block = block_ref[slot]
        after = []
        for a in range(4):
            place = a * stride + found[a]
            slot_ref[place] = slot * BLOCK
            kind_ref[place] = jnp.where(slot == a, 1, 0)
            after.append(found[a] + jnp.where(mask_ref[queries[a], block] > 0, 1, 0))
        return tuple(after)

    found = lax.fori_loop(0, count, listed, (jnp.int32(0),) * 4)
    items = jnp.int32(0)
    for a in range(4):
        for i in range(STEP):
            slot_ref[a * stride + found[a] + i] = 0
            kind_ref[a * stride + found[a] + i] = 2
        turns = (found[a] + STEP - 1) // STEP

        def item(i, unused, a=a, items=items):
            query_ref[items + i] = a
            start_ref[items + i] = a * stride + STEP * i
            return unused

        lax.fori_loop(0, turns, item, 0)
        items = items + turns
    for i in range(STEP):
        slot_ref[4 * stride + i] = 0
        kind_ref[4 * stride + i] = 2
    query_ref[items] = 3
    start_ref[items] = 4 * stride
    turns_ref[0] = (items + 1) >> 1
    me = (z * 2 + yh) * 2 + c

    def frame(f, mine):
        return jnp.where(owner_ref[f] == me, f, mine)

    mine = lax.fori_loop(0, owner_ref.shape[0], frame, jnp.int32(0))
    first, second = order_ref[2 * me], order_ref[2 * me + 1]
    keep_first = (first >> 1) == mine
    kept_row = jnp.where(keep_first, 0, BLOCK)
    lead_row = jnp.where((jnp.where(keep_first, first, second) & 1) == 0, 0, BLOCK)
    rows_ref[0] = jnp.where((order_ref[2 * (me ^ 1)] >> 1) == mine, 0, BLOCK)
    rows_ref[1] = BLOCK - kept_row
    rows_ref[2] = kept_row
    rows_ref[3] = lead_row
    rows_ref[4] = BLOCK - lead_row


def work_tables(where, block_order, block_mask, frame_owner):
    count = block_order.shape[0]
    sizes = [4 * count + 5 * STEP, 4 * count + 5 * STEP, count + 1, count + 1, 1, count // 4, 5]
    return pl.pallas_call(
        tables_kernel,
        out_shape=tuple(jax.ShapeDtypeStruct((size,), jnp.int32) for size in sizes),
        in_specs=[SMEM] * 4,
        out_specs=(SMEM,) * len(sizes),
        scratch_shapes=[pltpu.SMEM((count,), jnp.int32)],
        name="work_tables",
    )(where, block_order, block_mask, frame_owner)


def stack_kernel(*refs):
    pieces, out_ref = refs[:-1], refs[-1]
    rows = pieces[0].shape[0]
    for i, piece in enumerate(pieces):
        out_ref[i * rows : (i + 1) * rows, :] = piece[...]


def stacked(pieces):
    rows, width = pieces[0].shape
    return pl.pallas_call(
        stack_kernel,
        out_shape=jax.ShapeDtypeStruct((len(pieces) * rows, width), pieces[0].dtype),
        in_specs=[VMEM] * len(pieces),
        out_specs=VMEM,
        compiler_params=pltpu.CompilerParams(vmem_limit_bytes=8 * 1024 * 1024),
    )(*pieces)


def query_part_kernel(z_ref, dq_ref, *refs):
    pieces, (part_ref, kv_ref, weight, sems) = refs[:-4], refs[-4:]
    z = z_ref[0]
    rows = 112
    copies = []
    for kind, parts in enumerate(PLACES):
        ref = pieces[kind]
        for i, (quarter, back) in enumerate(parts):
            shard = lax.rem(z + 8 - back, 8) * 4 + z_ref[1 + quarter]
            copies.append(
                pltpu.make_async_copy(
                    ref.at[pl.ds(i * rows, rows), :],
                    weight.at[pl.ds(pl.multiple_of(shard * rows, 16), rows), :],
                    sems.at[len(copies)],
                )
            )
    for copy in copies:
        copy.start()
    for copy in copies:
        copy.wait()
    wide = dq_ref.shape[1]
    dq = dq_ref[...]
    step = 512

    def columns(i, unused):
        cols = pl.ds(pl.multiple_of(i * step, step), step)
        part_ref[:, cols] = dot_nt(dq, weight[cols, 0:wide]).astype(jnp.bfloat16)
        kv_ref[cols, :] = weight[cols, wide:]
        return unused

    lax.fori_loop(0, part_ref.shape[1] // step, columns, 0)


ORDER = (0, 1, 7, 2, 6, 3, 5, 4)
NEAR, FAR = ORDER[:5], ORDER[5:]
PLACES = tuple(
    [[(0, back)] for back in ORDER]
    + [[(kind, back) for back in side] for kind in (1, 2, 3) for side in (NEAR, FAR)]
)


def query_part(where, dq, pieces):
    total = 4 * 8 * 112
    wide = dq.shape[1]
    return pl.pallas_call(
        query_part_kernel,
        out_shape=(
            jax.ShapeDtypeStruct((dq.shape[0], total), jnp.bfloat16),
            jax.ShapeDtypeStruct((total, 2 * HD), jnp.bfloat16),
        ),
        in_specs=[SMEM, VMEM] + [ANY] * len(pieces),
        out_specs=(VMEM, VMEM),
        scratch_shapes=[
            pltpu.VMEM((total, wide + 2 * HD), jnp.bfloat16),
            pltpu.SemaphoreType.DMA((sum(len(p) for p in PLACES),)),
        ],
        compiler_params=pltpu.CompilerParams(vmem_limit_bytes=24 * 1024 * 1024),
        name="query_part",
    )(where, dq, *[in_hbm(piece) for piece in pieces])


def partial_kernel(rows_ref, spread_ref, kv_ref, part_ref, keep_ref, send_ref, whole, dkv_ref):
    chip = dkv_ref.shape[0]
    tok = chip // 2
    step = 512
    height = 32

    def total(i, unused):
        first = pl.multiple_of(i * height, height)
        dkv_sum = jnp.zeros((height, dkv_ref.shape[1]), jnp.float32)
        for source in range(spread_ref.shape[0] // chip):
            dkv_sum += spread_ref[pl.ds(source * chip + first, height), :].astype(jnp.float32)
        dkv_ref[pl.ds(first, height), :] = dkv_sum.astype(jnp.bfloat16)
        return unused

    lax.fori_loop(0, chip // height, total, 0)
    dkv = dkv_ref[...]

    def columns(i, unused):
        cols = pl.ds(pl.multiple_of(i * step, step), step)
        whole[...] = part_ref[:, cols].astype(jnp.float32) + dot_nt(dkv, kv_ref[cols, :])
        keep_ref[0:tok, cols] = whole[0:tok, :].astype(jnp.bfloat16)
        send_ref[0:tok, cols] = whole[tok:, :].astype(jnp.bfloat16)
        need = pl.ds(pl.multiple_of(tok + rows_ref[0], BLOCK), BLOCK)
        sent = pl.ds(pl.multiple_of(rows_ref[1], BLOCK), BLOCK)
        keep_ref[tok:, cols] = whole[need, :].astype(jnp.bfloat16)
        send_ref[tok:, cols] = whole[sent, :].astype(jnp.bfloat16)
        return unused

    lax.fori_loop(0, part_ref.shape[1] // step, columns, 0)


def partial_sums(rows, spread, kv_weight, part):
    out = 2 * BLOCK + BLOCK
    return pl.pallas_call(
        partial_kernel,
        out_shape=(
            jax.ShapeDtypeStruct((out, part.shape[1]), jnp.bfloat16),
            jax.ShapeDtypeStruct((out, part.shape[1]), jnp.bfloat16),
        ),
        in_specs=[SMEM, VMEM, VMEM, VMEM],
        out_specs=(VMEM, VMEM),
        scratch_shapes=[
            pltpu.VMEM((part.shape[0], 512), jnp.float32),
            pltpu.VMEM((part.shape[0], spread.shape[1]), jnp.bfloat16),
        ],
        compiler_params=pltpu.CompilerParams(vmem_limit_bytes=24 * 1024 * 1024),
        name="partial_sums",
    )(rows, spread, in_hbm(kv_weight), in_hbm(part))


def final_kernel(
    rows_ref, keep_ref, got_ref, in_own, swapped_ref, gain_ref, feature_ref, post_ref, projector_hbm,
    token_ref, encoder_ref, projector, frame, post, sem,
):
    load = pltpu.make_async_copy(projector_hbm, projector, sem)
    load.start()
    tok = in_own.shape[0]
    height = 16

    def token_rows(first, inputs):
        norm_grad = keep_ref[pl.ds(first, height), :].astype(jnp.float32) + got_ref[pl.ds(first, height), :].astype(jnp.float32)
        norm_grad = norm_grad.astype(jnp.bfloat16).astype(jnp.float32)
        inputs = inputs.astype(jnp.float32)
        inverse = lax.rsqrt(jnp.mean(inputs * inputs, axis=1, keepdims=True) + EPSILON)
        scaled = norm_grad * gain_ref[...]
        lean = inverse * inverse * inverse * jnp.mean(scaled * inputs, axis=1, keepdims=True)
        return (inverse * scaled - inputs * lean).astype(jnp.bfloat16)

    def own(i, unused):
        first = pl.multiple_of(i * height, height)
        token_ref[pl.ds(first, height), :] = token_rows(first, in_own[pl.ds(first, height), :])
        return unused

    def got(i, unused):
        first = pl.multiple_of(i * height, height)
        frame[pl.ds(pl.multiple_of(rows_ref[4] + first, height), height), :] = token_rows(
            tok + first,
            swapped_ref[pl.ds(pl.multiple_of(rows_ref[0] + first, height), height), :],
        )
        return unused

    lax.fori_loop(0, tok // height, own, 0)
    lax.fori_loop(0, BLOCK // height, got, 0)
    frame[pl.ds(pl.multiple_of(rows_ref[3], BLOCK), BLOCK), :] = token_ref[
        pl.ds(pl.multiple_of(rows_ref[2], BLOCK), BLOCK), :
    ]
    features = feature_ref[...].astype(jnp.float32)
    centered = features - jnp.mean(features, axis=1, keepdims=True)
    deviation = lax.rsqrt(jnp.mean(centered * centered, axis=1, keepdims=True) + EPSILON)
    normed = centered * deviation
    load.wait()
    step = 384

    def columns(i, unused):
        cols = pl.ds(pl.multiple_of(i * step, 128), step)
        post[:, cols] = dot_nt(projector[cols, :], frame[...]).T
        return unused

    lax.fori_loop(0, post.shape[1] // step, columns, 0)
    weighted = post[...] * post_ref[...]
    encoder_ref[...] = (
        deviation
        * (
            weighted
            - jnp.mean(weighted, axis=1, keepdims=True)
            - normed * jnp.mean(weighted * normed, axis=1, keepdims=True)
        )
    ).astype(jnp.bfloat16)


def finished(rows, keep, got, in_own, in_got, gain, features, post_gain, projector):
    return pl.pallas_call(
        final_kernel,
        out_shape=(
            jax.ShapeDtypeStruct(in_own.shape, jnp.bfloat16),
            jax.ShapeDtypeStruct(features.shape, jnp.bfloat16),
        ),
        in_specs=[SMEM] + [VMEM] * 7 + [ANY],
        out_specs=(VMEM, VMEM),
        scratch_shapes=[
            pltpu.VMEM(projector.shape, jnp.bfloat16),
            pltpu.VMEM((2 * BLOCK, in_own.shape[1]), jnp.bfloat16),
            pltpu.VMEM((2 * BLOCK, projector.shape[0]), jnp.float32),
            pltpu.SemaphoreType.DMA,
        ],
        compiler_params=pltpu.CompilerParams(vmem_limit_bytes=32 * 1024 * 1024),
        name="finished",
    )(rows, keep, got, in_own, in_got, gain, features, post_gain, in_hbm(projector))


def swap_core(value):
    return lax.ppermute(value, "c", [(0, 1), (1, 0)])


def in_hbm(value):
    return pltpu.with_memory_space_constraint(value, pltpu.HBM)


def delta_rows(delta):
    return jnp.transpose(delta.reshape(2, BLOCK, GROUP), (0, 2, 1)).reshape(2, 1, LANES)


def program(
    queries,
    keys,
    values,
    out_grad,
    row_delta,
    layer_input,
    norm_gain,
    qkv_weight,
    block_order,
    block_mask,
    frame_owner,
    vision_features,
    post_gain,
    projector,
):
    nz, nx = lax.axis_size("z"), lax.axis_size("x")
    z, yh, c, x, yl = (lax.axis_index(name) for name in ("z", "yh", "c", "x", "yl"))
    wide = GROUP * HD

    def group_of(array, which, width):
        return lax.dynamic_slice_in_dim(array, which * width, width, 1)

    def kv_of(which):
        return jnp.concatenate([group_of(keys, which, HD), group_of(values, which, HD)], axis=1)

    def columns_of(which):
        return jnp.concatenate(
            [
                group_of(qkv_weight[:, : HQ * HD], which, wide),
                group_of(qkv_weight[:, HQ * HD :], which, HD),
                group_of(qkv_weight[:, HQ * HD :], KVH + which, HD),
            ],
            axis=1,
        )

    forward = [(i, (i + 1) % nz) for i in range(nz)]
    backward = [(i, (i - 1) % nz) for i in range(nz)]

    kv_chip = jnp.concatenate([kv_of(c), swap_core(kv_of(1 - c))], axis=0)
    kv_row = lax.ppermute(kv_chip, "yh", [(0, 1), (1, 0)])
    (qkv_weight, row_delta), _ = lax.optimization_barrier(((qkv_weight, row_delta), kv_chip))
    kv_pair = jnp.concatenate([kv_chip, kv_row], axis=0)

    def index(yh_, c_, x_, yl_):
        return ((yh_ * 2 + c_) * nx + x_) * 2 + yl_

    mine, theirs = columns_of(c), columns_of(1 - c)
    pairs_a, pairs_b = [], []
    for x_ in range(nx):
        for yl_ in range(2):
            home = x_ & 1
            pairs_a.append((index(home, yl_, x_, yl_), index(home, 1 - yl_, x_, yl_)))
            source = index(home, yl_, x_, 1 - yl_)
            pairs_a.append((source, index(1 - home, yl_, x_, yl_)))
            pairs_b.append((source, index(1 - home, 1 - yl_, x_, yl_)))
    plane = ("yh", "c", "x", "yl")
    weight_a = lax.ppermute(jnp.where(c == yl, theirs, mine), plane, pairs_a)
    weight_b = lax.ppermute(theirs, plane, pairs_b)
    quarter = jnp.where(c == yl, jnp.where(yh == x & 1, mine, weight_a), jnp.where(yh == x & 1, weight_a, weight_b))

    kv_parts = {0: kv_pair}
    weights = {0: quarter}
    kv_up = kv_down = kv_pair
    weight_up = weight_down = quarter
    for k in range(1, nz // 2 + 1):
        kv_parts[k] = kv_up = lax.ppermute(kv_up, "z", forward)
        if k < nz // 2:
            kv_parts[nz - k] = kv_down = lax.ppermute(kv_down, "z", backward)
        if k < 3:
            weights[k] = weight_up = lax.ppermute(weight_up, "z", forward)
            weights[nz - k] = weight_down = lax.ppermute(weight_down, "z", backward)
    weights[3] = lax.ppermute(weight_up, "z", forward)
    weights[nz - 3] = lax.ppermute(weight_down, "z", backward)
    weights[4] = lax.ppermute(weight_up, "z", [(i, (i + 2) % nz) for i in range(nz)])

    def shift_x(value, by):
        return lax.ppermute(value, "x", [(i, (i + by) % nx) for i in range(nx)])

    def shift_y(value, by):
        return lax.ppermute(value, ("yh", "yl"), [(i, (i + by) % 4) for i in range(4)])

    near = stacked([weights[k] for k in NEAR])
    x_near, y_near = shift_x(near, 1), shift_y(near, 1)
    corner_near = shift_x(y_near, 1)

    place = jnp.stack([z, yh, c]).astype(jnp.int32)
    *lists, frame_rows = work_tables(place, block_order, block_mask, frame_owner)
    tokens = (queries, swap_core(queries), out_grad, swap_core(out_grad))
    in_got = swap_core(layer_input)
    delta_got = swap_core(delta_rows(group_of(row_delta, 1 - c, GROUP)))
    delta = jnp.concatenate([delta_rows(group_of(row_delta, c, GROUP)), delta_got], axis=0)
    dq, dkv = attention(lists, place, tokens, delta, [kv_parts[k] for k in range(nz)])

    spread = lax.all_to_all(dkv, ("z", "yh"), 0, 0, tiled=True)

    dq, late = lax.optimization_barrier((dq, [weights[k] for k in FAR]))
    for k, piece in zip(FAR, late, strict=True):
        weights[k] = piece
    far = stacked(late)
    x_far, y_far = shift_x(far, -1), shift_y(far, -1)
    corner_far = shift_x(y_far, -1)
    quarters = [(x & 1) * 2 + yl, (1 - (x & 1)) * 2 + yl, (x & 1) * 2 + 1 - yl, (1 - (x & 1)) * 2 + 1 - yl]
    where = jnp.stack([z] + quarters).astype(jnp.int32)
    part, kv_weight = query_part(
        where, dq, [weights[k] for k in ORDER] + [x_near, x_far, y_near, y_far, corner_near, corner_far]
    )
    keep, send = partial_sums(frame_rows, spread, kv_weight, part)
    token_grad, encoder_grad = finished(
        frame_rows,
        keep,
        swap_core(send),
        layer_input,
        in_got,
        norm_gain[None],
        vision_features[0],
        post_gain[None],
        projector,
    )
    return (token_grad, encoder_grad[None])


def solution(mesh):
    grid = Mesh(mesh.devices.reshape(8, 2, 2, 4, 2), ("z", "yh", "c", "x", "yl"))
    both = ("x", "yl", "z", "yh", "c")
    placed = (
        P(both, None),
        P(both, None),
        P(both, None),
        P(both, None),
        P(both, None),
        P(both, None),
        P(),
        P(("z", "yh", "c"), None),
        P(("x", "yl")),
        P(("x", "yl"), None),
        P(("x", "yl")),
        P(both, None, None),
        P(),
        P(),
    )
    return jax.shard_map(
        program,
        mesh=grid,
        in_specs=placed,
        out_specs=(P(both, None), P(both, None, None)),
        check_vma=False,
    )
```

```python
import jax
import jax.numpy as jnp
from jax import lax
from jax.experimental import pallas as pl
from jax.experimental.pallas import tpu as pltpu
from jax.sharding import Mesh, PartitionSpec as P

HQ = 14
KVH = 2
HD = 128
GROUP = HQ // KVH
EPSILON = 1e-06
NEGATIVE = -1e30
BLOCK = 64
LANES = GROUP * BLOCK
STEP = 4


def dot_nt(a, b):
    return lax.dot_general(a, b, (((1,), (1,)), ((), ())), preferred_element_type=jnp.float32)


def dot_nn(a, b):
    return lax.dot_general(a, b, (((1,), (0,)), ((), ())), preferred_element_type=jnp.float32)


def dot_tn(a, b):
    return lax.dot_general(a, b, (((0,), (0,)), ((), ())), preferred_element_type=jnp.float32)


def attention_kernel(pieces, *refs):
    slot_ref, kind_ref, query_ref, start_ref, turns_ref, place_ref, where_ref = refs[:7]
    q_own, q_got, g_own, g_got, delta_ref = refs[7:12]
    kv_parts = refs[12 : 12 + pieces]
    dq_ref, dkv_ref = refs[12 + pieces : 14 + pieces]
    qs, gs, kv, bias, acc, dqt, tops, sums, lses, tok, sems = refs[14 + pieces :]
    wide = GROUP * HD
    scaling = HD ** (-0.5)
    to_log2 = scaling * 1.4426950408889634
    height = kv_parts[0].shape[0]
    rows = height * pieces
    base = pl.multiple_of(where_ref[2] * wide, HD)
    copies = [
        pltpu.make_async_copy(ref.at[:, pl.ds(base, wide)], tok.at[i], sems.at[i])
        for i, ref in enumerate((q_own, q_got, g_own, g_got))
    ]
    copies += [
        pltpu.make_async_copy(part, kv.at[pl.ds(i * height, height), :], sems.at[4 + i])
        for i, part in enumerate(kv_parts)
    ]
    for copy in copies:
        copy.start()
    key_row = lax.broadcasted_iota(jnp.int32, (BLOCK, LANES), 0)
    query_row = lax.broadcasted_iota(jnp.int32, (BLOCK, LANES), 1) % BLOCK
    bias[0] = jnp.zeros((BLOCK, LANES), jnp.float32)
    bias[1] = jnp.where(key_row <= query_row, 0.0, NEGATIVE)
    bias[2] = jnp.full((BLOCK, LANES), NEGATIVE, jnp.float32)
    acc[...] = jnp.zeros(acc.shape, jnp.float32)
    dqt[...] = jnp.zeros(dqt.shape, jnp.float32)
    tops[...] = jnp.full(tops.shape, NEGATIVE, jnp.float32)
    sums[...] = jnp.zeros(sums.shape, jnp.float32)
    for copy in copies:
        copy.wait()
    for a in range(4):
        first = (a % 2) * BLOCK
        for h in range(GROUP):
            into, cols = slice(h * BLOCK, (h + 1) * BLOCK), slice(h * HD, (h + 1) * HD)
            qs[a, into, :] = tok[a // 2, first : first + BLOCK, cols]
            gs[a, into, :] = tok[2 + a // 2, first : first + BLOCK, cols]

    def slots_of(item):
        first = start_ref[item]
        return [pl.multiple_of(slot_ref[first + i], BLOCK) for i in range(STEP)]

    def gathered(slots, first):
        return jnp.concatenate([kv[pl.ds(row, BLOCK), first : first + HD] for row in slots], axis=0)

    def scores(item, a, keys):
        first = start_ref[item]
        mask = jnp.concatenate([bias[kind_ref[first + i]] for i in range(STEP)], axis=0)
        return dot_nt(keys, qs[a]) * to_log2 + mask

    def total(turn, unused):
        for item in (2 * turn, 2 * turn + 1):
            a = query_ref[item]
            score = scores(item, a, gathered(slots_of(item), 0)).reshape(STEP * BLOCK // 8, 8, LANES)
            top = tops[a]
            top_next = jnp.maximum(top, jnp.max(score, axis=0))
            sums[a] = sums[a] * jnp.exp2(top - top_next) + jnp.sum(jnp.exp2(score - top_next), axis=0)
            tops[a] = top_next
        return unused

    lax.fori_loop(0, turns_ref[0], total, 0)
    for a in range(4):
        top = tops[a]
        peak = jnp.max(top, axis=0, keepdims=True)
        whole = jnp.sum(sums[a] * jnp.exp2(top - peak), axis=0, keepdims=True)
        lses[a] = peak + jnp.log2(whole)

    def grads(turn, unused):
        for item in (2 * turn, 2 * turn + 1):
            a = query_ref[item]
            slots = slots_of(item)
            keys = gathered(slots, 0)
            values = gathered(slots, HD)
            prob = jnp.exp2(scores(item, a, keys) - lses[a])
            prob_grad = dot_nt(values, gs[a])
            score_grad = (prob * (prob_grad - delta_ref[a])).astype(jnp.bfloat16)
            value_add = dot_nn(prob.astype(jnp.bfloat16), gs[a])
            key_add = dot_nn(score_grad, qs[a])
            dqt[a] += dot_tn(keys, score_grad)
            for i, row in enumerate(slots):
                acc[pl.ds(row, BLOCK), 0:HD] += key_add[i * BLOCK : (i + 1) * BLOCK, :]
                acc[pl.ds(row, BLOCK), HD : 2 * HD] += value_add[i * BLOCK : (i + 1) * BLOCK, :]
        return unused

    lax.fori_loop(0, turns_ref[0], grads, 0)
    for a in range(4):
        dq = (dqt[a].T * scaling).astype(jnp.bfloat16)
        for h in range(GROUP):
            dq_ref[a * BLOCK : (a + 1) * BLOCK, h * HD : (h + 1) * HD] = dq[h * BLOCK : (h + 1) * BLOCK, :]
    scale = jnp.where(lax.broadcasted_iota(jnp.int32, (1, 2 * HD), 1) < HD, scaling, 1.0)
    chip = 4 * BLOCK

    def write(i, unused):
        source = pl.ds(pl.multiple_of(i * chip, chip), chip)
        target = pl.ds(pl.multiple_of(place_ref[i], chip), chip)
        dkv_ref[target, :] = (acc[source, :] * scale).astype(jnp.bfloat16)
        return unused

    lax.fori_loop(0, rows // chip, write, 0)


SMEM = pl.BlockSpec(memory_space=pltpu.SMEM)
VMEM = pl.BlockSpec(memory_space=pltpu.VMEM)
ANY = pl.BlockSpec(memory_space=pl.ANY)


def attention(lists, where, tokens, delta, kv_parts):
    pieces = len(kv_parts)
    rows = pieces * kv_parts[0].shape[0]
    return pl.pallas_call(
        lambda *refs: attention_kernel(pieces, *refs),
        out_shape=(
            jax.ShapeDtypeStruct((4 * BLOCK, GROUP * HD), jnp.bfloat16),
            jax.ShapeDtypeStruct((rows, 2 * HD), jnp.bfloat16),
        ),
        in_specs=[SMEM] * 7 + [ANY] * 4 + [VMEM] + [ANY] * pieces,
        out_specs=(VMEM, VMEM),
        scratch_shapes=[
            pltpu.VMEM((4, LANES, HD), jnp.bfloat16),
            pltpu.VMEM((4, LANES, HD), jnp.bfloat16),
            pltpu.VMEM((rows, 2 * HD), jnp.bfloat16),
            pltpu.VMEM((3, BLOCK, LANES), jnp.float32),
            pltpu.VMEM((rows, 2 * HD), jnp.float32),
            pltpu.VMEM((4, HD, LANES), jnp.float32),
            pltpu.VMEM((4, 8, LANES), jnp.float32),
            pltpu.VMEM((4, 8, LANES), jnp.float32),
            pltpu.VMEM((4, 1, LANES), jnp.float32),
            pltpu.VMEM((4, 2 * BLOCK, GROUP * HD), jnp.bfloat16),
            pltpu.SemaphoreType.DMA((4 + pieces,)),
        ],
        compiler_params=pltpu.CompilerParams(vmem_limit_bytes=32 * 1024 * 1024),
        name="attention_grads",
    )(*[in_hbm(t) for t in lists], in_hbm(where), *[in_hbm(t) for t in tokens], delta, *[in_hbm(part) for part in kv_parts])


def tables_kernel(
    where_ref, order_ref, mask_ref, owner_ref,
    slot_ref, kind_ref, query_ref, start_ref, turns_ref, place_ref, rows_ref, block_ref,
):
    z, yh, c = where_ref[0], where_ref[1], where_ref[2]
    count = block_ref.shape[0]
    nz = count // 8

    def chip_of(slot):
        return lax.rem(z + nz - (slot >> 3), nz) * 2 + (yh ^ ((slot >> 2) & 1))

    def block(slot, unused):
        core = c ^ ((slot >> 1) & 1)
        block_ref[slot] = order_ref[2 * (2 * chip_of(slot) + core) + (slot & 1)]
        return unused

    lax.fori_loop(0, count, block, 0, unroll=8)

    def place(chip, unused):
        place_ref[chip] = chip_of(4 * chip) * (4 * BLOCK)
        return unused

    lax.fori_loop(0, count // 4, place, 0, unroll=8)
    stride = count + STEP
    queries = [block_ref[a] for a in range(4)]

    def listed(slot, found):
        block = block_ref[slot]
        after = []
        for a in range(4):
            place = a * stride + found[a]
            slot_ref[place] = slot * BLOCK
            kind_ref[place] = jnp.where(slot == a, 1, 0)
            after.append(found[a] + jnp.where(mask_ref[queries[a], block] > 0, 1, 0))
        return tuple(after)

    found = lax.fori_loop(0, count, listed, (jnp.int32(0),) * 4, unroll=4)
    items = jnp.int32(0)
    for a in range(4):
        for i in range(STEP):
            slot_ref[a * stride + found[a] + i] = 0
            kind_ref[a * stride + found[a] + i] = 2
        turns = (found[a] + STEP - 1) // STEP

        def item(i, unused, a=a, items=items):
            query_ref[items + i] = a
            start_ref[items + i] = a * stride + STEP * i
            return unused

        lax.fori_loop(0, turns, item, 0)
        items = items + turns
    for i in range(STEP):
        slot_ref[4 * stride + i] = 0
        kind_ref[4 * stride + i] = 2
    query_ref[items] = 3
    start_ref[items] = 4 * stride
    turns_ref[0] = (items + 1) >> 1
    me = (z * 2 + yh) * 2 + c

    def frame(f, mine):
        return jnp.where(owner_ref[f] == me, f, mine)

    mine = lax.fori_loop(0, owner_ref.shape[0], frame, jnp.int32(0), unroll=8)
    first, second = order_ref[2 * me], order_ref[2 * me + 1]
    keep_first = (first >> 1) == mine
    kept_row = jnp.where(keep_first, 0, BLOCK)
    lead_row = jnp.where((jnp.where(keep_first, first, second) & 1) == 0, 0, BLOCK)
    rows_ref[0] = jnp.where((order_ref[2 * (me ^ 1)] >> 1) == mine, 0, BLOCK)
    rows_ref[1] = BLOCK - kept_row
    rows_ref[2] = kept_row
    rows_ref[3] = lead_row
    rows_ref[4] = BLOCK - lead_row


def work_tables(where, block_order, block_mask, frame_owner):
    count = block_order.shape[0]
    sizes = [4 * count + 5 * STEP, 4 * count + 5 * STEP, count + 1, count + 1, 1, count // 4, 5]
    return pl.pallas_call(
        tables_kernel,
        out_shape=tuple(jax.ShapeDtypeStruct((size,), jnp.int32) for size in sizes),
        in_specs=[SMEM] * 4,
        out_specs=(SMEM,) * len(sizes),
        scratch_shapes=[pltpu.SMEM((count,), jnp.int32)],
        name="work_tables",
    )(where, block_order, block_mask, frame_owner)


def stack_kernel(*refs):
    pieces, out_ref = refs[:-1], refs[-1]
    rows = pieces[0].shape[0]
    for i, piece in enumerate(pieces):
        out_ref[i * rows : (i + 1) * rows, :] = piece[...]


def stacked(pieces):
    rows, width = pieces[0].shape
    return pl.pallas_call(
        stack_kernel,
        out_shape=jax.ShapeDtypeStruct((len(pieces) * rows, width), pieces[0].dtype),
        in_specs=[VMEM] * len(pieces),
        out_specs=VMEM,
        compiler_params=pltpu.CompilerParams(vmem_limit_bytes=8 * 1024 * 1024),
    )(*pieces)


def query_part_kernel(z_ref, dq_ref, *refs):
    pieces, (part_ref, kv_ref, weight, sems) = refs[:-4], refs[-4:]
    z = z_ref[0]
    rows = 112
    copies = []
    for kind, parts in enumerate(PLACES):
        ref = pieces[kind]
        for i, (quarter, back) in enumerate(parts):
            shard = lax.rem(z + 8 - back, 8) * 4 + z_ref[1 + quarter]
            copies.append(
                pltpu.make_async_copy(
                    ref.at[pl.ds(i * rows, rows), :],
                    weight.at[pl.ds(pl.multiple_of(shard * rows, 16), rows), :],
                    sems.at[len(copies)],
                )
            )
    for copy in copies:
        copy.start()
    for copy in copies:
        copy.wait()
    wide = dq_ref.shape[1]
    dq = dq_ref[...]
    step = 512

    def columns(i, unused):
        cols = pl.ds(pl.multiple_of(i * step, step), step)
        part_ref[:, cols] = dot_nt(dq, weight[cols, 0:wide]).astype(jnp.bfloat16)
        kv_ref[cols, :] = weight[cols, wide:]
        return unused

    lax.fori_loop(0, part_ref.shape[1] // step, columns, 0)


ORDER = (0, 1, 7, 2, 6, 3, 5, 4)
NEAR, FAR = ORDER[:5], ORDER[5:]
PLACES = tuple(
    [[(0, back)] for back in ORDER]
    + [[(kind, back) for back in side] for kind in (1, 2, 3) for side in (NEAR, FAR)]
)


def query_part(where, dq, pieces):
    total = 4 * 8 * 112
    wide = dq.shape[1]
    return pl.pallas_call(
        query_part_kernel,
        out_shape=(
            jax.ShapeDtypeStruct((dq.shape[0], total), jnp.bfloat16),
            jax.ShapeDtypeStruct((total, 2 * HD), jnp.bfloat16),
        ),
        in_specs=[SMEM, VMEM] + [ANY] * len(pieces),
        out_specs=(VMEM, VMEM),
        scratch_shapes=[
            pltpu.VMEM((total, wide + 2 * HD), jnp.bfloat16),
            pltpu.SemaphoreType.DMA((sum(len(p) for p in PLACES),)),
        ],
        compiler_params=pltpu.CompilerParams(vmem_limit_bytes=24 * 1024 * 1024),
        name="query_part",
    )(where, in_hbm(dq), *[in_hbm(piece) for piece in pieces])


def partial_kernel(rows_ref, spread_ref, kv_ref, part_ref, keep_ref, send_ref, whole, dkv_ref):
    chip = dkv_ref.shape[0]
    tok = chip // 2
    step = 512
    height = 32

    def total(i, unused):
        first = pl.multiple_of(i * height, height)
        dkv_sum = jnp.zeros((height, dkv_ref.shape[1]), jnp.float32)
        for source in range(spread_ref.shape[0] // chip):
            dkv_sum += spread_ref[pl.ds(source * chip + first, height), :].astype(jnp.float32)
        dkv_ref[pl.ds(first, height), :] = dkv_sum.astype(jnp.bfloat16)
        return unused

    lax.fori_loop(0, chip // height, total, 0)
    dkv = dkv_ref[...]

    def columns(i, unused):
        cols = pl.ds(pl.multiple_of(i * step, step), step)
        whole[...] = part_ref[:, cols].astype(jnp.float32) + dot_nt(dkv, kv_ref[cols, :])
        keep_ref[0:tok, cols] = whole[0:tok, :].astype(jnp.bfloat16)
        send_ref[0:tok, cols] = whole[tok:, :].astype(jnp.bfloat16)
        need = pl.ds(pl.multiple_of(tok + rows_ref[0], BLOCK), BLOCK)
        sent = pl.ds(pl.multiple_of(rows_ref[1], BLOCK), BLOCK)
        keep_ref[tok:, cols] = whole[need, :].astype(jnp.bfloat16)
        send_ref[tok:, cols] = whole[sent, :].astype(jnp.bfloat16)
        return unused

    lax.fori_loop(0, part_ref.shape[1] // step, columns, 0)


def partial_sums(rows, spread, kv_weight, part):
    out = 2 * BLOCK + BLOCK
    return pl.pallas_call(
        partial_kernel,
        out_shape=(
            jax.ShapeDtypeStruct((out, part.shape[1]), jnp.bfloat16),
            jax.ShapeDtypeStruct((out, part.shape[1]), jnp.bfloat16),
        ),
        in_specs=[SMEM, VMEM, VMEM, VMEM],
        out_specs=(VMEM, VMEM),
        scratch_shapes=[
            pltpu.VMEM((part.shape[0], 512), jnp.float32),
            pltpu.VMEM((part.shape[0], spread.shape[1]), jnp.bfloat16),
        ],
        compiler_params=pltpu.CompilerParams(vmem_limit_bytes=24 * 1024 * 1024),
        name="partial_sums",
    )(rows, spread, in_hbm(kv_weight), in_hbm(part))


def final_kernel(
    rows_ref, keep_ref, got_ref, in_own, swapped_ref, gain_ref, feature_ref, post_ref, projector_hbm,
    token_ref, encoder_ref, projector, frame, post, sem,
):
    load = pltpu.make_async_copy(projector_hbm, projector, sem)
    load.start()
    tok = in_own.shape[0]
    height = 16

    def token_rows(first, inputs):
        norm_grad = keep_ref[pl.ds(first, height), :].astype(jnp.float32) + got_ref[pl.ds(first, height), :].astype(jnp.float32)
        norm_grad = norm_grad.astype(jnp.bfloat16).astype(jnp.float32)
        inputs = inputs.astype(jnp.float32)
        inverse = lax.rsqrt(jnp.mean(inputs * inputs, axis=1, keepdims=True) + EPSILON)
        scaled = norm_grad * gain_ref[...]
        lean = inverse * inverse * inverse * jnp.mean(scaled * inputs, axis=1, keepdims=True)
        return (inverse * scaled - inputs * lean).astype(jnp.bfloat16)

    def own(i, unused):
        first = pl.multiple_of(i * height, height)
        token_ref[pl.ds(first, height), :] = token_rows(first, in_own[pl.ds(first, height), :])
        return unused

    def got(i, unused):
        first = pl.multiple_of(i * height, height)
        frame[pl.ds(pl.multiple_of(rows_ref[4] + first, height), height), :] = token_rows(
            tok + first,
            swapped_ref[pl.ds(pl.multiple_of(rows_ref[0] + first, height), height), :],
        )
        return unused

    lax.fori_loop(0, tok // height, own, 0)
    lax.fori_loop(0, BLOCK // height, got, 0)
    frame[pl.ds(pl.multiple_of(rows_ref[3], BLOCK), BLOCK), :] = token_ref[
        pl.ds(pl.multiple_of(rows_ref[2], BLOCK), BLOCK), :
    ]
    features = feature_ref[...].astype(jnp.float32)
    centered = features - jnp.mean(features, axis=1, keepdims=True)
    deviation = lax.rsqrt(jnp.mean(centered * centered, axis=1, keepdims=True) + EPSILON)
    normed = centered * deviation
    load.wait()
    step = 384

    def columns(i, unused):
        cols = pl.ds(pl.multiple_of(i * step, 128), step)
        post[:, cols] = dot_nt(frame[...], projector[cols, :])
        return unused

    lax.fori_loop(0, post.shape[1] // step, columns, 0)
    weighted = post[...] * post_ref[...]
    encoder_ref[...] = (
        deviation
        * (
            weighted
            - jnp.mean(weighted, axis=1, keepdims=True)
            - normed * jnp.mean(weighted * normed, axis=1, keepdims=True)
        )
    ).astype(jnp.bfloat16)


def finished(rows, keep, got, in_own, in_got, gain, features, post_gain, projector):
    return pl.pallas_call(
        final_kernel,
        out_shape=(
            jax.ShapeDtypeStruct(in_own.shape, jnp.bfloat16),
            jax.ShapeDtypeStruct(features.shape, jnp.bfloat16),
        ),
        in_specs=[SMEM] + [VMEM] * 7 + [ANY],
        out_specs=(VMEM, VMEM),
        scratch_shapes=[
            pltpu.VMEM(projector.shape, jnp.bfloat16),
            pltpu.VMEM((2 * BLOCK, in_own.shape[1]), jnp.bfloat16),
            pltpu.VMEM((2 * BLOCK, projector.shape[0]), jnp.float32),
            pltpu.SemaphoreType.DMA,
        ],
        compiler_params=pltpu.CompilerParams(vmem_limit_bytes=32 * 1024 * 1024),
        name="finished",
    )(rows, keep, got, in_own, in_got, gain, features, post_gain, in_hbm(projector))


def swap_core(value):
    return lax.ppermute(value, "c", [(0, 1), (1, 0)])


def in_hbm(value):
    return pltpu.with_memory_space_constraint(value, pltpu.HBM)


def delta_rows(delta):
    return jnp.transpose(delta.reshape(2, BLOCK, GROUP), (0, 2, 1)).reshape(2, 1, LANES)


def program(
    queries,
    keys,
    values,
    out_grad,
    row_delta,
    layer_input,
    norm_gain,
    qkv_weight,
    block_order,
    block_mask,
    frame_owner,
    vision_features,
    post_gain,
    projector,
):
    nz, nx = lax.axis_size("z"), lax.axis_size("x")
    z, yh, c, x, yl = (lax.axis_index(name) for name in ("z", "yh", "c", "x", "yl"))
    wide = GROUP * HD

    def group_of(array, which, width):
        return lax.dynamic_slice_in_dim(array, which * width, width, 1)

    def kv_of(which):
        return jnp.concatenate([group_of(keys, which, HD), group_of(values, which, HD)], axis=1)

    def columns_of(which):
        return jnp.concatenate(
            [
                group_of(qkv_weight[:, : HQ * HD], which, wide),
                group_of(qkv_weight[:, HQ * HD :], which, HD),
                group_of(qkv_weight[:, HQ * HD :], KVH + which, HD),
            ],
            axis=1,
        )

    forward = [(i, (i + 1) % nz) for i in range(nz)]
    backward = [(i, (i - 1) % nz) for i in range(nz)]

    kv_chip = jnp.concatenate([kv_of(c), swap_core(kv_of(1 - c))], axis=0)
    kv_row = lax.ppermute(kv_chip, "yh", [(0, 1), (1, 0)])
    (qkv_weight, row_delta), _ = lax.optimization_barrier(((qkv_weight, row_delta), kv_chip))
    kv_pair = jnp.concatenate([kv_chip, kv_row], axis=0)

    def index(yh_, c_, x_, yl_):
        return ((yh_ * 2 + c_) * nx + x_) * 2 + yl_

    mine, theirs = columns_of(c), columns_of(1 - c)
    pairs_a, pairs_b = [], []
    for x_ in range(nx):
        for yl_ in range(2):
            home = x_ & 1
            pairs_a.append((index(home, yl_, x_, yl_), index(home, 1 - yl_, x_, yl_)))
            source = index(home, yl_, x_, 1 - yl_)
            pairs_a.append((source, index(1 - home, yl_, x_, yl_)))
            pairs_b.append((source, index(1 - home, 1 - yl_, x_, yl_)))
    plane = ("yh", "c", "x", "yl")
    weight_a = lax.ppermute(jnp.where(c == yl, theirs, mine), plane, pairs_a)
    weight_b = lax.ppermute(theirs, plane, pairs_b)
    quarter = jnp.where(c == yl, jnp.where(yh == x & 1, mine, weight_a), jnp.where(yh == x & 1, weight_a, weight_b))

    kv_parts = {0: kv_pair}
    weights = {0: quarter}
    kv_up = kv_down = kv_pair
    weight_up = weight_down = quarter
    for k in range(1, nz // 2 + 1):
        kv_parts[k] = kv_up = lax.ppermute(kv_up, "z", forward)
        if k < nz // 2:
            kv_parts[nz - k] = kv_down = lax.ppermute(kv_down, "z", backward)
        if k < 3:
            weights[k] = weight_up = lax.ppermute(weight_up, "z", forward)
            weights[nz - k] = weight_down = lax.ppermute(weight_down, "z", backward)
    weights[3] = lax.ppermute(weight_up, "z", forward)
    weights[nz - 3] = lax.ppermute(weight_down, "z", backward)
    weights[4] = lax.ppermute(weight_up, "z", [(i, (i + 2) % nz) for i in range(nz)])

    def shift_x(value, by):
        return lax.ppermute(value, "x", [(i, (i + by) % nx) for i in range(nx)])

    def shift_y(value, by):
        return lax.ppermute(value, ("yh", "yl"), [(i, (i + by) % 4) for i in range(4)])

    near = stacked([weights[k] for k in NEAR])
    x_near, y_near = shift_x(near, 1), shift_y(near, 1)
    corner_near = shift_x(y_near, 1)

    place = jnp.stack([z, yh, c]).astype(jnp.int32)
    *lists, frame_rows = work_tables(place, block_order, block_mask, frame_owner)
    tokens = (queries, swap_core(queries), out_grad, swap_core(out_grad))
    in_got = swap_core(layer_input)
    delta_got = swap_core(delta_rows(group_of(row_delta, 1 - c, GROUP)))
    delta = jnp.concatenate([delta_rows(group_of(row_delta, c, GROUP)), delta_got], axis=0)
    dq, dkv = attention(lists, place, tokens, delta, [kv_parts[k] for k in range(nz)])

    spread = lax.all_to_all(dkv, ("z", "yh"), 0, 0, tiled=True)

    dq, late = lax.optimization_barrier((dq, [weights[k] for k in FAR]))
    for k, piece in zip(FAR, late, strict=True):
        weights[k] = piece
    far = stacked(late)
    x_far, y_far = shift_x(far, -1), shift_y(far, -1)
    corner_far = shift_x(y_far, -1)
    quarters = [(x & 1) * 2 + yl, (1 - (x & 1)) * 2 + yl, (x & 1) * 2 + 1 - yl, (1 - (x & 1)) * 2 + 1 - yl]
    where = jnp.stack([z] + quarters).astype(jnp.int32)
    part, kv_weight = query_part(
        where, dq, [weights[k] for k in ORDER] + [x_near, x_far, y_near, y_far, corner_near, corner_far]
    )
    keep, send = partial_sums(frame_rows, spread, kv_weight, part)
    token_grad, encoder_grad = finished(
        frame_rows,
        keep,
        swap_core(send),
        layer_input,
        in_got,
        norm_gain[None],
        vision_features[0],
        post_gain[None],
        projector,
    )
    return (token_grad, encoder_grad[None])


def solution(mesh):
    grid = Mesh(mesh.devices.reshape(8, 2, 2, 4, 2), ("z", "yh", "c", "x", "yl"))
    both = ("x", "yl", "z", "yh", "c")
    placed = (
        P(both, None),
        P(both, None),
        P(both, None),
        P(both, None),
        P(both, None),
        P(both, None),
        P(),
        P(("z", "yh", "c"), None),
        P(("x", "yl")),
        P(("x", "yl"), None),
        P(("x", "yl")),
        P(both, None, None),
        P(),
        P(),
    )
    return jax.shard_map(
        program,
        mesh=grid,
        in_specs=placed,
        out_specs=(P(both, None), P(both, None, None)),
        check_vma=False,
    )
```
